128 devices in a mesh: dp: 1, ep: 128 (over z, y, x, core).
Axes of the slice: x: 4, y: 4, z: 4, core: 2. Of those that a mesh axis runs over, the one named last changes fastest.
Arguments:
- tokens: bfloat16 [32768, 2048], P(('dp', 'ep'))
- routes: int32 [32768, 8], P(('dp', 'ep'))
- w_router: bfloat16 [2048, 128], replicated
- w_one: bfloat16 [128, 2048, 768], P('ep')
- w_three: bfloat16 [128, 2048, 768], P('ep')
- w_two: bfloat16 [128, 768, 2048], P('ep')
Outputs:
- output: bfloat16 [32768, 2048], P(('dp', 'ep'))
All inputs are finite; a program needn't handle non-finite values.
Results may differ from the reference program's by a relative error of at most 0.00819171.
Values are sent between devices in bfloat16 or wider.
A program may use at most 1 GiB of HBM per device.

```python
import jax
import jax.numpy as jnp
from jax import lax

GROUP_SIZE = 128
DEV_TOKENS = 256
D_MODEL = 2048
D_EXPERT = 768
NUM_EXPERTS = 128
TOP_K = 8
CAPACITY = 24


def draw_routes(route_key):
    perm_key, row_key, slot_key = jax.random.split(route_key, 3)
    num_pairs = DEV_TOKENS * TOP_K
    hot_count = NUM_EXPERTS // 8
    rest_pairs = num_pairs - hot_count * CAPACITY
    base_count = rest_pairs // (NUM_EXPERTS - hot_count)
    extra_count = rest_pairs % (NUM_EXPERTS - hot_count)
    rank_ids = jnp.arange(NUM_EXPERTS, dtype=jnp.int32)
    counts = jnp.where(rank_ids < hot_count, CAPACITY, base_count + (rank_ids - hot_count < extra_count).astype(jnp.int32))
    count_ends = jnp.cumsum(counts)
    pair_rank = jnp.searchsorted(count_ends, jnp.arange(num_pairs, dtype=jnp.int32), side='right')
    expert_of_rank = jax.random.permutation(perm_key, NUM_EXPERTS)
    layout = expert_of_rank[pair_rank].reshape(TOP_K, DEV_TOKENS).T

    def device_routes(perm_rows, perm_slots):
        row_order = jax.random.permutation(perm_rows, DEV_TOKENS)
        scores = jax.random.randint(perm_slots, (DEV_TOKENS, TOP_K), 0, 1 << 20) * TOP_K + jnp.arange(TOP_K)
        slot_order = jnp.argsort(scores, axis=1)
        return jnp.take_along_axis(layout[row_order], slot_order, axis=1)

    per_device = jax.vmap(device_routes)(jax.random.split(row_key, GROUP_SIZE), jax.random.split(slot_key, GROUP_SIZE))
    return per_device.reshape(GROUP_SIZE * DEV_TOKENS, TOP_K).astype(jnp.int32)


def setup_inputs(seed: int = 0, part: int = 0) -> dict:
    part_key = jax.random.fold_in(jax.random.key(seed), part)
    token_key, route_key = jax.random.split(part_key)
    shared = jax.random.split(jax.random.key(seed + 1), 4)
    tokens = jax.random.normal(token_key, (GROUP_SIZE * DEV_TOKENS, D_MODEL), jnp.float32)
    w_router = jax.random.normal(shared[0], (D_MODEL, NUM_EXPERTS), jnp.float32) * (1.5 * D_MODEL ** -0.5)
    w_one = jax.random.normal(shared[1], (NUM_EXPERTS, D_MODEL, D_EXPERT), jnp.float32) * D_MODEL ** -0.5
    w_three = jax.random.normal(shared[2], (NUM_EXPERTS, D_MODEL, D_EXPERT), jnp.float32) * D_MODEL ** -0.5
    w_two = jax.random.normal(shared[3], (NUM_EXPERTS, D_EXPERT, D_MODEL), jnp.float32) * D_EXPERT ** -0.5
    return {'tokens': tokens.astype(jnp.bfloat16), 'routes': draw_routes(route_key), 'w_router': w_router.astype(jnp.bfloat16), 'w_one': w_one.astype(jnp.bfloat16), 'w_three': w_three.astype(jnp.bfloat16), 'w_two': w_two.astype(jnp.bfloat16)}


def expert_rows(rows, w_gate, w_up, w_down):
    gate_pre = jnp.dot(rows, w_gate, preferred_element_type=jnp.float32)
    up_pre = jnp.dot(rows, w_up, preferred_element_type=jnp.float32)
    hidden = (jax.nn.silu(gate_pre) * up_pre).astype(jnp.bfloat16)
    return jnp.dot(hidden, w_down, preferred_element_type=jnp.float32).astype(jnp.bfloat16)


def reference(tokens, routes, w_router, w_one, w_three, w_two):
    logits = jnp.dot(tokens, w_router, preferred_element_type=jnp.float32)
    gate_vals = jax.nn.softmax(jnp.take_along_axis(logits, routes, axis=1), axis=-1)
    flat_gates = gate_vals.reshape(-1)
    flat_routes = routes.reshape(-1)
    num_pairs = flat_routes.shape[0]
    sort_order = jnp.argsort(flat_routes, stable=True)
    counts = jax.ops.segment_sum(jnp.ones_like(flat_routes), flat_routes, num_segments=NUM_EXPERTS)
    starts = jnp.cumsum(counts) - counts
    slot_ids = jnp.arange(GROUP_SIZE * CAPACITY, dtype=jnp.int32)

    def one_expert(y_sum, step_in):
        w_gate, w_up, w_down, exp_start, exp_count = step_in
        pair_at = sort_order[jnp.minimum(exp_start + slot_ids, num_pairs - 1)]
        token_at = pair_at // TOP_K
        weight = jnp.where(slot_ids < exp_count, flat_gates[pair_at], 0.0)
        out_rows = expert_rows(tokens[token_at], w_gate, w_up, w_down)
        return y_sum.at[token_at].add(weight[:, None] * out_rows.astype(jnp.float32)), None

    y_sum = lax.scan(one_expert, jnp.zeros(tokens.shape, jnp.float32), (w_one, w_three, w_two, starts, counts))[0]
    return y_sum.astype(jnp.bfloat16)
```

```python
import functools

import jax
import jax.numpy as jnp
from jax import lax
from jax.experimental import pallas as pl
from jax.experimental.pallas import tpu as pltpu
from jax.sharding import PartitionSpec as P

MESH = pl.DeviceIdType.MESH
Z, Y, X = 0, 1, 2
ORDERS = ((Z, Y, X), (X, Z, Y), (Y, X, Z))
SLOTS = 8


def slot_capacity(num_tokens, top_k, num_experts):
    return 8 * ((3 * num_tokens * top_k + 16 * num_experts - 1) // (16 * num_experts))


def torus_side(group_size):
    side = 1
    while 2 * side ** 3 < group_size:
        side += 1
    return side


def column_groups(d_model):
    lanes = d_model // 128
    widths = [128 * (lanes // 3 + (1 if i < lanes % 3 else 0)) for i in range(3)]
    starts = [sum(widths[:i]) for i in range(3)]
    return list(zip(starts, widths))


def moved(me, side, axis, steps, core_steps=0):
    digits = [me // (2 * side * side), (me // (2 * side)) % side, (me // 2) % side]
    digits[axis] = (digits[axis] + steps + side) % side
    return ((digits[Z] * side + digits[Y]) * side + digits[X]) * 2 + (me + core_steps) % 2


def route_plan(tokens, routes, w_router, expert_at):
    num_tokens = tokens.shape[0]
    num_experts = w_router.shape[1]
    logits = jnp.dot(tokens, w_router, preferred_element_type=jnp.float32)
    expert_ids = jnp.arange(num_experts, dtype=jnp.int32)
    hits = routes[:, :, None] == expert_ids[None, None, :]
    picked = jnp.sum(jnp.where(hits, logits[:, None, :], 0.0), axis=2)
    gate_vals = jax.nn.softmax(picked, axis=-1)
    routes_t = routes.T
    gates_t = gate_vals.T
    at = routes_t[:, None, :] == expert_at[None, :, None]
    mask_t = jnp.any(at, axis=0)
    gate_t = jnp.sum(jnp.where(at, gates_t[:, None, :], 0.0), axis=0)
    token_ids = jnp.arange(num_tokens, dtype=jnp.int32)
    before = (token_ids[:, None] < token_ids[None, :]).astype(jnp.bfloat16)
    rank_t = jnp.dot(mask_t.astype(jnp.bfloat16), before, preferred_element_type=jnp.float32)
    return jnp.where(mask_t, rank_t, -1.0), gate_t


def moe_kernel(side, chunks, groups, tokens_hbm, plans_hbm, w_one_hbm, w_three_hbm, w_two_hbm, y_own, y_peers,
               toks, plans, packed, relay, rows, w_one, w_three, w_two, parts,
               load_sem, w_sem, s0_sem, r0_sem, sp_sem, rp_sem, s1_sem, r1_sem, s2_sem, r2_sem, b1_sem, c1_sem, b2_sem, c2_sem, s3_sem, r3_sem, out_sem, free2_sem, free3_sem):
    me = lax.axis_index('ep')
    dp = lax.axis_index('dp')
    num_tokens = tokens_hbm.shape[0]
    plane = 2 * side * side
    ends = 2 * side
    packed_rows = plane * SLOTS

    def remote(src, dst, s_sem, r_sem, axis, steps, core_steps=0):
        return pltpu.make_async_remote_copy(
            src_ref=src, dst_ref=dst, send_sem=s_sem, recv_sem=r_sem,
            device_id=(dp, moved(me, side, axis, steps, core_steps)), device_id_type=MESH)

    def columns(g):
        return pl.ds(*groups[g])

    def relay_from(g, q, b):
        return relay[g].at[q, b] if g == 1 else relay[g].at[q, :, b]

    def relay_others(g, q):
        return relay[g].at[q, pl.ds(1, side - 1)] if g == 1 else relay[g].at[q, :, pl.ds(1, side - 1)]

    def rows_at(g, q, e):
        c, core = e // 2, e % 2
        third = ORDERS[g][2]
        where = {Z: (q, c, slice(None), slice(None), core), Y: (q, slice(None), c, slice(None), core),
                 X: (q, slice(None), slice(None), c, core)}[third]
        return where + (slice(None), columns(g))

    def gather_copies(g, a):
        first = ORDERS[g][0]
        return (remote(tokens_hbm.at[:, columns(g)], toks[g].at[a], s0_sem.at[g], r0_sem.at[g], first, a),
                remote(plans_hbm[g].at[a], plans[g].at[a], sp_sem.at[g], rp_sem.at[g], first, a))

    def gather_all(g):
        first = ORDERS[g][0]
        others = pl.ds(1, side - 1)
        return (remote(toks[g].at[others], toks[g].at[others], s0_sem.at[g], r0_sem.at[g], first, 1),
                remote(plans[g].at[others], plans[g].at[others], sp_sem.at[g], rp_sem.at[g], first, 1))

    def out_second(g, q, b):
        return remote(packed[g].at[q, b], relay_from(g, q, b), s1_sem.at[g, q], r1_sem.at[g, q], ORDERS[g][1], b)

    def out_second_all(g, q):
        return remote(packed[g].at[q, pl.ds(1, side - 1)], relay_others(g, q), s1_sem.at[g, q], r1_sem.at[g, q], ORDERS[g][1], 1)

    def out_third(g, q, e):
        return remote(relay[g].at[q, :, :, e], rows.at[rows_at(g, q, e)], s2_sem.at[g, q], r2_sem.at[g, q], ORDERS[g][2], e // 2, e % 2)

    def third_all(g, q, s_sem, r_sem):
        some = relay[g].at[q, :, :, pl.ds(1, ends - 1)]
        return remote(some, some, s_sem.at[g, q], r_sem.at[g, q], ORDERS[g][2], 1)

    def home_third(g, q, e):
        return remote(rows.at[rows_at(g, q, e)], relay[g].at[q, :, :, e], b1_sem.at[g, q], c1_sem.at[g, q], ORDERS[g][2], -(e // 2), e % 2)

    def home_second(g, q, b):
        return remote(relay_from(g, q, b), packed[g].at[q, b], b2_sem.at[g, q], c2_sem.at[g, q], ORDERS[g][1], -b)

    def home_second_all(g, q):
        return remote(relay_others(g, q), packed[g].at[q, pl.ds(1, side - 1)], b2_sem.at[g, q], c2_sem.at[g, q], ORDERS[g][1], 1)

    def home_first(g, a):
        return remote(parts.at[a, :, columns(g)], y_peers.at[a - 1, :, columns(g)], s3_sem.at[g], r3_sem.at[g], ORDERS[g][0], -a)

    def home_first_all(g):
        return remote(parts.at[pl.ds(1, side - 1), :, columns(g)], y_peers.at[:, :, columns(g)], s3_sem.at[g], r3_sem.at[g], ORDERS[g][0], 1)

    def tell(sem, axis, steps, core_steps=0):
        pl.semaphore_signal(sem, inc=1, device_id=(dp, moved(me, side, axis, steps, core_steps)), device_id_type=MESH)

    loads = []
    for g in range(3):
        loads.append((pltpu.make_async_copy(tokens_hbm.at[:, columns(g)], toks[g].at[0], load_sem.at[2 * g]),
                      pltpu.make_async_copy(plans_hbm[g].at[0], plans[g].at[0], load_sem.at[2 * g + 1])))
    weights = [pltpu.make_async_copy(src, dst, w_sem.at[i]) for i, (src, dst) in enumerate(
        [(w_one_hbm, w_one), (w_three_hbm, w_three), (w_two_hbm, w_two)])]

    for a in range(1, side):
        for g in range(3):
            for copy in gather_copies(g, a)[::-1]:
                copy.start()
    for g in range(3):
        for copy in loads[g]:
            copy.start()
    for copy in weights:
        copy.start()
    parts[...] = jnp.zeros_like(parts)

    def taken(g, q, a):
        slots = plans[g][a, pl.ds(0, plane), :]
        ids = lax.broadcasted_iota(jnp.int32, (plane, SLOTS, num_tokens), 1) + q * SLOTS
        return jnp.broadcast_to(slots[:, None, :], (plane, SLOTS, num_tokens)) == ids.astype(jnp.float32)

    for g in range(3):
        for copy in loads[g]:
            copy.wait()
        for copy in gather_all(g):
            copy.wait_recv()

    def pack(q, carry):
        for g in range(3):
            width = groups[g][1]

            def source(a, c):
                select = jnp.where(taken(g, q, a), 1.0, 0.0).reshape(packed_rows, num_tokens).astype(jnp.bfloat16)
                out = jnp.dot(select, toks[g][a], preferred_element_type=jnp.float32)
                packed[g][q, :, a] = out.reshape(side, ends, SLOTS, width).astype(jnp.bfloat16)
                return c
            lax.fori_loop(0, side, source, 0)
            for b in range(1, side):
                out_second(g, q, b).start()
            relay_from(g, q, 0)[...] = packed[g][q, 0]
        return carry

    lax.fori_loop(0, chunks, pack, 0)

    def forward(q, carry):
        for g in range(3):
            out_second_all(g, q).wait_recv()
            for e in range(1, ends):
                out_third(g, q, e).start()
            rows[rows_at(g, q, 0)] = relay[g][q, :, :, 0]
            out_second_all(g, q).wait_send()
            for b in range(1, side):
                tell(free2_sem.at[g, q], ORDERS[g][1], b)
        return carry

    lax.fori_loop(0, chunks, forward, 0)
    for copy in weights:
        copy.wait()

    def experts(q, carry):
        for g in range(3):
            third_all(g, q, s2_sem, r2_sem).wait_recv()
        for g in range(3):
            third_all(g, q, s2_sem, r2_sem).wait_send()
            for e in range(1, ends):
                tell(free3_sem.at[g, q], ORDERS[g][2], e // 2, e % 2)

        def block(z, c):
            shape = rows.shape[2:]
            u = rows[q, z].astype(jnp.float32).reshape(packed_rows, shape[-1]).astype(jnp.bfloat16)
            gate_pre = jnp.dot(u, w_one[...], preferred_element_type=jnp.float32)
            up_pre = jnp.dot(u, w_three[...], preferred_element_type=jnp.float32)
            hidden = (jax.nn.silu(gate_pre) * up_pre).astype(jnp.bfloat16)
            out = jnp.dot(hidden, w_two[...], preferred_element_type=jnp.float32)
            rows[q, z] = out.reshape(shape).astype(jnp.bfloat16)
            return c
        lax.fori_loop(0, side, block, 0)
        for g in range(3):
            pl.semaphore_wait(free3_sem.at[g, q], ends - 1)
            for e in range(1, ends):
                home_third(g, q, e).start()
            relay[g][q, :, :, 0] = rows[rows_at(g, q, 0)]
        return carry

    lax.fori_loop(0, chunks, experts, 0)

    def backward(q, carry):
        for g in range(3):
            third_all(g, q, b1_sem, c1_sem).wait_recv()
            pl.semaphore_wait(free2_sem.at[g, q], side - 1)
            for b in range(1, side):
                home_second(g, q, b).start()
            packed[g][q, 0] = relay_from(g, q, 0)[...]
        return carry

    lax.fori_loop(0, chunks, backward, 0)

    def combine(q, carry):
        for g in range(3):
            home_second_all(g, q).wait_recv()
            width = groups[g][1]

            def source(a, c):
                gates = plans[g][a, pl.ds(plane, plane), :]
                used = taken(g, q, a)
                o = packed[g][q, :, a].astype(jnp.float32).reshape(packed_rows, width).astype(jnp.bfloat16)
                total = None
                for _ in range(3):
                    part = gates.astype(jnp.bfloat16).astype(jnp.float32)
                    gates = gates - part
                    mix = jnp.where(used, jnp.broadcast_to(part[:, None, :], used.shape), 0.0).reshape(packed_rows, num_tokens).astype(jnp.bfloat16)
                    term = lax.dot_general(mix, o, (((0,), (0,)), ((), ())), preferred_element_type=jnp.float32)
                    total = term if total is None else total + term
                parts[a, :, columns(g)] += total
                return c
            lax.fori_loop(0, side, source, 0)

            @pl.when(q == chunks - 1)
            def _():
                for a in range(1, side):
                    home_first(g, a).start()
        return carry

    lax.fori_loop(0, chunks, combine, 0)
    own = pltpu.make_async_copy(parts.at[0], y_own, out_sem)
    own.start()

    for g in range(3):
        for copy in gather_all(g):
            copy.wait_send()

        def drain(q, c):
            third_all(g, q, b1_sem, c1_sem).wait_send()
            home_second_all(g, q).wait_send()
            return c
        lax.fori_loop(0, chunks, drain, 0)
        home_first_all(g).wait_send()
        home_first_all(g).wait_recv()
    own.wait()


def solution(mesh):
    group_size = mesh.shape['ep']
    side = torus_side(group_size)
    row_spec = P(('dp', 'ep'), None)
    expert_spec = P('ep', None, None)

    def device_step(tokens, routes, w_router, w_one, w_three, w_two):
        num_tokens, d_model = tokens.shape
        top_k = routes.shape[1]
        num_experts = w_router.shape[1]
        d_expert = w_one.shape[2]
        capacity = slot_capacity(num_tokens, top_k, num_experts)
        chunks = capacity // SLOTS
        groups = column_groups(d_model)
        plane = 2 * side * side
        me = lax.axis_index('ep')
        position = jnp.arange(num_experts, dtype=jnp.int32)
        expert_at = moved(me, side, Z, position // plane)
        expert_at = moved(expert_at, side, Y, (position // (2 * side)) % side)
        expert_at = moved(expert_at, side, X, (position // 2) % side, position % 2)
        slot_t, gate_t = route_plan(tokens, routes, w_router, expert_at)
        plan = jnp.stack([slot_t, gate_t]).reshape(2, side, side, side, 2, num_tokens)
        plans = []
        for first, second, third in ORDERS:
            ordered = jnp.transpose(plan, (1 + first, 0, 1 + second, 1 + third, 4, 5))
            plans.append(ordered.reshape(side, 2 * plane, num_tokens))
        hbm = pl.BlockSpec(memory_space=pl.ANY)
        dma = pltpu.SemaphoreType.DMA
        slab = [[pltpu.VMEM((chunks, side, side, 2 * side, SLOTS, width), jnp.bfloat16) for _, width in groups] for _ in range(2)]
        pair = [dma((3, chunks)), dma((3, chunks))]
        y_own, y_peers = pl.pallas_call(
            functools.partial(moe_kernel, side, chunks, groups),
            out_shape=(jax.ShapeDtypeStruct((num_tokens, d_model), jnp.float32),
                       jax.ShapeDtypeStruct((side - 1, num_tokens, d_model), jnp.float32)),
            in_specs=[hbm, (hbm, hbm, hbm), hbm, hbm, hbm],
            out_specs=(hbm, hbm),
            scratch_shapes=[
                [pltpu.VMEM((side, num_tokens, width), jnp.bfloat16) for _, width in groups],
                [pltpu.VMEM((side, 2 * plane, num_tokens), jnp.float32) for _ in groups],
                slab[0], slab[1],
                pltpu.VMEM((chunks, side, side, side, 2, SLOTS, d_model), jnp.bfloat16),
                pltpu.VMEM((d_model, d_expert), jnp.bfloat16),
                pltpu.VMEM((d_model, d_expert), jnp.bfloat16),
                pltpu.VMEM((d_expert, d_model), jnp.bfloat16),
                pltpu.VMEM((side, num_tokens, d_model), jnp.float32),
                dma((6,)), dma((3,)), dma((3,)), dma((3,)), dma((3,)), dma((3,)),
                *pair, *pair, *pair, *pair, dma((3,)), dma((3,)), dma,
                pltpu.SemaphoreType.REGULAR((3, chunks)), pltpu.SemaphoreType.REGULAR((3, chunks)),
            ],
            compiler_params=pltpu.CompilerParams(has_side_effects=True, vmem_limit_bytes=67043328),
            name='moe',
        )(tokens, tuple(plans), w_one[0], w_three[0], w_two[0])
        total = y_own
        for i in range(side - 1):
            total = total + y_peers[i]
        return total.astype(jnp.bfloat16)

    return jax.shard_map(device_step, mesh=mesh, in_specs=(row_spec, row_spec, P(None, None), expert_spec, expert_spec, expert_spec), out_specs=row_spec, check_vma=False)
```

```python
import functools

import jax
import jax.numpy as jnp
from jax import lax
from jax.experimental import pallas as pl
from jax.experimental.pallas import tpu as pltpu
from jax.sharding import PartitionSpec as P

MESH = pl.DeviceIdType.MESH
Z, Y, X = 0, 1, 2
ORDERS = ((Z, Y, X), (X, Z, Y), (Y, X, Z))
SLOTS = 8


def slot_capacity(num_tokens, top_k, num_experts):
    return 8 * ((3 * num_tokens * top_k + 16 * num_experts - 1) // (16 * num_experts))


def torus_side(group_size):
    side = 1
    while 2 * side ** 3 < group_size:
        side += 1
    return side


def column_groups(d_model):
    lanes = d_model // 128
    widths = [128 * (lanes // 3 + (1 if i < lanes % 3 else 0)) for i in range(3)]
    starts = [sum(widths[:i]) for i in range(3)]
    return list(zip(starts, widths))


def moved(me, side, axis, steps, core_steps=0):
    digits = [me // (2 * side * side), (me // (2 * side)) % side, (me // 2) % side]
    digits[axis] = (digits[axis] + steps + side) % side
    return ((digits[Z] * side + digits[Y]) * side + digits[X]) * 2 + (me + core_steps) % 2


def expert_order(me, side, order, num_tokens):
    bits = side.bit_length() - 1
    position = lax.broadcasted_iota(jnp.int32, (2 * side ** 3, num_tokens), 0)
    digits = [me // (2 * side * side), (me // (2 * side)) % side, (me // 2) % side]
    for place, axis in enumerate(order):
        steps = jnp.right_shift(position, 1 + (2 - place) * bits)
        digits[axis] = jnp.bitwise_and(digits[axis] + steps, side - 1)
    core = jnp.bitwise_and(me + position, 1)
    return ((digits[Z] * side + digits[Y]) * side + digits[X]) * 2 + core


def moe_kernel(side, chunks, groups, tokens_hbm, routes_ref, w_router, w_one_hbm, w_three_hbm, w_two_hbm, y_own, y_peers,
               toks, plans, own_plans, packed, relay, rows, w_one, w_three, w_two, parts,
               load_sem, w_sem, s0_sem, r0_sem, sp_sem, rp_sem, s1_sem, r1_sem, s2_sem, r2_sem, b1_sem, c1_sem, b2_sem, c2_sem, s3_sem, r3_sem, out_sem, free2_sem, free3_sem):
    me = lax.axis_index('ep')
    dp = lax.axis_index('dp')
    num_tokens = tokens_hbm.shape[0]
    plane = 2 * side * side
    ends = 2 * side
    packed_rows = plane * SLOTS

    def remote(src, dst, s_sem, r_sem, axis, steps, core_steps=0):
        return pltpu.make_async_remote_copy(
            src_ref=src, dst_ref=dst, send_sem=s_sem, recv_sem=r_sem,
            device_id=(dp, moved(me, side, axis, steps, core_steps)), device_id_type=MESH)

    def columns(g):
        return pl.ds(*groups[g])

    def relay_from(g, q, b):
        return relay[g].at[q, b] if g == 1 else relay[g].at[q, :, b]

    def relay_others(g, q):
        return relay[g].at[q, pl.ds(1, side - 1)] if g == 1 else relay[g].at[q, :, pl.ds(1, side - 1)]

    def rows_at(g, q, e):
        c, core = e // 2, e % 2
        third = ORDERS[g][2]
        where = {Z: (q, c, slice(None), slice(None), core), Y: (q, slice(None), c, slice(None), core),
                 X: (q, slice(None), slice(None), c, core)}[third]
        return where + (slice(None), columns(g))

    def gather_tokens(g, a):
        return remote(tokens_hbm.at[:, columns(g)], toks[g].at[a], s0_sem.at[g], r0_sem.at[g], ORDERS[g][0], a)

    def gather_plans(g, a):
        return remote(own_plans[g].at[a], plans[g].at[a], sp_sem.at[g], rp_sem.at[g], ORDERS[g][0], a)

    def gather_all(g):
        first = ORDERS[g][0]
        others = pl.ds(1, side - 1)
        return (remote(toks[g].at[others], toks[g].at[others], s0_sem.at[g], r0_sem.at[g], first, 1),
                remote(plans[g].at[others], plans[g].at[others], sp_sem.at[g], rp_sem.at[g], first, 1))

    def relay_slab(g, q, a, b):
        return relay[g].at[q, b, a] if g == 1 else relay[g].at[q, a, b]

    def out_second(g, q, a, b):
        return remote(packed[g].at[q, b, a], relay_slab(g, q, a, b), s1_sem.at[g, q], r1_sem.at[g, q], ORDERS[g][1], b)

    def out_second_all(g, q):
        return remote(packed[g].at[q, pl.ds(1, side - 1)], relay_others(g, q), s1_sem.at[g, q], r1_sem.at[g, q], ORDERS[g][1], 1)

    def out_third(g, q, e):
        return remote(relay[g].at[q, :, :, e], rows.at[rows_at(g, q, e)], s2_sem.at[g, q], r2_sem.at[g, q], ORDERS[g][2], e // 2, e % 2)

    def third_all(g, q, s_sem, r_sem):
        some = relay[g].at[q, :, :, pl.ds(1, ends - 1)]
        return remote(some, some, s_sem.at[g, q], r_sem.at[g, q], ORDERS[g][2], 1)

    def home_third(g, q, e):
        return remote(rows.at[rows_at(g, q, e)], relay[g].at[q, :, :, e], b1_sem.at[g, q], c1_sem.at[g, q], ORDERS[g][2], -(e // 2), e % 2)

    def home_second(g, q, b):
        return remote(relay_from(g, q, b), packed[g].at[q, b], b2_sem.at[g, q], c2_sem.at[g, q], ORDERS[g][1], -b)

    def home_second_all(g, q):
        return remote(relay_others(g, q), packed[g].at[q, pl.ds(1, side - 1)], b2_sem.at[g, q], c2_sem.at[g, q], ORDERS[g][1], 1)

    def home_first(g, a):
        return remote(parts.at[a, :, columns(g)], y_peers.at[a - 1, :, columns(g)], s3_sem.at[g], r3_sem.at[g], ORDERS[g][0], -a)

    def home_first_all(g):
        return remote(parts.at[pl.ds(1, side - 1), :, columns(g)], y_peers.at[:, :, columns(g)], s3_sem.at[g], r3_sem.at[g], ORDERS[g][0], 1)

    def tell(sem, axis, steps, core_steps=0):
        pl.semaphore_signal(sem, inc=1, device_id=(dp, moved(me, side, axis, steps, core_steps)), device_id_type=MESH)

    loads = [pltpu.make_async_copy(tokens_hbm.at[:, columns(g)], toks[g].at[0], load_sem.at[g]) for g in range(3)]
    weights = [pltpu.make_async_copy(src, dst, w_sem.at[i]) for i, (src, dst) in enumerate(
        [(w_one_hbm, w_one), (w_three_hbm, w_three), (w_two_hbm, w_two)])]
    for copy in loads:
        copy.start()

    barrier = pltpu.get_barrier_semaphore()
    tell(barrier, X, 0, 1)
    for axis in (Z, Y, X):
        for steps in range(1, side):
            for core_steps in range(2):
                tell(barrier, axis, steps, core_steps)
    pl.semaphore_wait(barrier, 1 + 3 * (side - 1) * 2)

    for a in range(1, side):
        for g in range(3):
            gather_tokens(g, a).start()
    for copy in loads:
        copy.wait()

    num_experts = 2 * side ** 3
    logits = sum(jnp.dot(toks[g][0], w_router[columns(g), :], preferred_element_type=jnp.float32) for g in range(3)).T
    ids = lax.broadcasted_iota(jnp.int32, (num_experts, num_tokens), 0)
    top_k = routes_ref.shape[0]
    picks = [routes_ref[k:k + 1, :] for k in range(top_k)]
    scores = [jnp.sum(jnp.where(pick == ids, logits, 0.0), axis=0, keepdims=True) for pick in picks]
    peak = functools.reduce(jnp.maximum, scores)
    scores = [jnp.exp(score - peak) for score in scores]
    norm = sum(scores)
    gates = [score / norm for score in scores]
    before = (lax.broadcasted_iota(jnp.int32, (num_tokens, num_tokens), 0)
              < lax.broadcasted_iota(jnp.int32, (num_tokens, num_tokens), 1))
    before = jnp.where(before, 1.0, 0.0).astype(jnp.bfloat16)
    for g in range(3):
        expert_at = expert_order(me, side, ORDERS[g], num_tokens)
        mask = jnp.zeros((num_experts, num_tokens), jnp.float32)
        gate = jnp.zeros((num_experts, num_tokens), jnp.float32)
        for k in range(top_k):
            hit = picks[k] == expert_at
            mask = jnp.where(hit, 1.0, mask)
            gate = jnp.where(hit, gates[k], gate)
        slot = jnp.dot(mask.astype(jnp.bfloat16), before, preferred_element_type=jnp.float32)
        slot = jnp.where(mask > 0.0, slot, -1.0)
        plans[g][0, pl.ds(0, plane), :] = slot[:plane]
        plans[g][0, pl.ds(plane, plane), :] = gate[:plane]
        for a in range(1, side):
            own_plans[g][a, pl.ds(0, plane), :] = slot[a * plane:(a + 1) * plane]
            own_plans[g][a, pl.ds(plane, plane), :] = gate[a * plane:(a + 1) * plane]
        for a in range(1, side):
            gather_plans(g, a).start()
    for copy in weights:
        copy.start()

    def taken(g, q, a):
        slots = plans[g][a, pl.ds(0, plane), :]
        ids = lax.broadcasted_iota(jnp.int32, (plane, SLOTS, num_tokens), 1) + q * SLOTS
        return jnp.broadcast_to(slots[:, None, :], (plane, SLOTS, num_tokens)) == ids.astype(jnp.float32)

    def pack(g, q, a):
        select = jnp.where(taken(g, q, a), 1.0, 0.0).reshape(packed_rows, num_tokens).astype(jnp.bfloat16)
        out = jnp.dot(select, toks[g][a], preferred_element_type=jnp.float32)
        out = out.reshape(side, ends, SLOTS, groups[g][1]).astype(jnp.bfloat16)
        packed[g][q, pl.ds(1, side - 1), a] = out[1:]
        for b in range(1, side):
            out_second(g, q, a, b).start()
        relay_slab(g, q, a, 0)[...] = out[0]

    def pack_own(q, carry):
        for g in range(3):
            pack(g, q, 0)
        return carry

    lax.fori_loop(0, chunks, pack_own, 0)
    parts[...] = jnp.zeros_like(parts)
    for g in range(3):
        for copy in gather_all(g):
            copy.wait_recv()

    def outward(i, carry):
        @pl.when(i < chunks)
        def _():
            for g in range(3):
                def source(a, c):
                    pack(g, i, a)
                    return c
                lax.fori_loop(1, side, source, 0)

        @pl.when(i > 0)
        def _():
            forward(i - 1)
        return carry

    def forward(q):
        for g in range(3):
            out_second_all(g, q).wait_recv()
            for e in range(1, ends):
                out_third(g, q, e).start()
            rows[rows_at(g, q, 0)] = relay[g][q, :, :, 0]
            out_second_all(g, q).wait_send()
            for b in range(1, side):
                tell(free2_sem.at[g, q], ORDERS[g][1], b)

    lax.fori_loop(0, chunks + 1, outward, 0)
    for copy in weights:
        copy.wait()

    def experts(q, carry):
        for g in range(3):
            third_all(g, q, s2_sem, r2_sem).wait_recv()
        for g in range(3):
            third_all(g, q, s2_sem, r2_sem).wait_send()
            for e in range(1, ends):
                tell(free3_sem.at[g, q], ORDERS[g][2], e // 2, e % 2)

        def block(z, c):
            shape = rows.shape[2:]
            u = rows[q, z].astype(jnp.float32).reshape(packed_rows, shape[-1]).astype(jnp.bfloat16)
            gate_pre = jnp.dot(u, w_one[...], preferred_element_type=jnp.float32)
            up_pre = jnp.dot(u, w_three[...], preferred_element_type=jnp.float32)
            hidden = (jax.nn.silu(gate_pre) * up_pre).astype(jnp.bfloat16)
            out = jnp.dot(hidden, w_two[...], preferred_element_type=jnp.float32)
            rows[q, z] = out.reshape(shape).astype(jnp.bfloat16)
            return c
        lax.fori_loop(0, side, block, 0)
        for g in range(3):
            pl.semaphore_wait(free3_sem.at[g, q], ends - 1)
            for e in range(1, ends):
                home_third(g, q, e).start()
            relay[g][q, :, :, 0] = rows[rows_at(g, q, 0)]
        return carry

    lax.fori_loop(0, chunks, experts, 0)

    def backward(q):
        for g in range(3):
            third_all(g, q, b1_sem, c1_sem).wait_recv()
            pl.semaphore_wait(free2_sem.at[g, q], side - 1)
            for b in range(1, side):
                home_second(g, q, b).start()
            packed[g][q, 0] = relay_from(g, q, 0)[...]

    def combine(q):
        for g in (1, 2, 0):
            home_second_all(g, q).wait_recv()
            width = groups[g][1]

            def source(i, c):
                a = (i + 1) % side
                gates = plans[g][a, pl.ds(plane, plane), :]
                used = taken(g, q, a)
                o = packed[g][q, :, a].astype(jnp.float32).reshape(packed_rows, width).astype(jnp.bfloat16)
                total = None
                for _ in range(3):
                    part = gates.astype(jnp.bfloat16).astype(jnp.float32)
                    gates = gates - part
                    mix = jnp.where(used, jnp.broadcast_to(part[:, None, :], used.shape), 0.0).reshape(packed_rows, num_tokens).astype(jnp.bfloat16)
                    term = lax.dot_general(mix, o, (((0,), (0,)), ((), ())), preferred_element_type=jnp.float32)
                    total = term if total is None else total + term
                parts[a, :, columns(g)] += total

                @pl.when(jnp.logical_and(q == chunks - 1, a > 0))
                def _():
                    home_first(g, a).start()
                return c
            lax.fori_loop(0, side, source, 0)

    def homeward(i, carry):
        @pl.when(i < chunks)
        def _():
            backward(i)

        @pl.when(i > 0)
        def _():
            combine(i - 1)
        return carry

    lax.fori_loop(0, chunks + 1, homeward, 0)
    own = pltpu.make_async_copy(parts.at[0], y_own, out_sem)
    own.start()

    for g in range(3):
        for copy in gather_all(g):
            copy.wait_send()

        def drain(q, c):
            third_all(g, q, b1_sem, c1_sem).wait_send()
            home_second_all(g, q).wait_send()
            return c
        lax.fori_loop(0, chunks, drain, 0)
        home_first_all(g).wait_send()
        home_first_all(g).wait_recv()
    own.wait()


def solution(mesh):
    group_size = mesh.shape['ep']
    side = torus_side(group_size)
    row_spec = P(('dp', 'ep'), None)
    expert_spec = P('ep', None, None)

    def device_step(tokens, routes, w_router, w_one, w_three, w_two):
        num_tokens, d_model = tokens.shape
        top_k = routes.shape[1]
        num_experts = w_router.shape[1]
        d_expert = w_one.shape[2]
        capacity = slot_capacity(num_tokens, top_k, num_experts)
        chunks = capacity // SLOTS
        groups = column_groups(d_model)
        plane = 2 * side * side
        hbm = pl.BlockSpec(memory_space=pl.ANY)
        vmem = pl.BlockSpec(memory_space=pltpu.VMEM)
        dma = pltpu.SemaphoreType.DMA
        slab = [[pltpu.VMEM((chunks, side, side, 2 * side, SLOTS, width), jnp.bfloat16) for _, width in groups] for _ in range(2)]
        pair = [dma((3, chunks)), dma((3, chunks))]
        y_own, y_peers = pl.pallas_call(
            functools.partial(moe_kernel, side, chunks, groups),
            out_shape=(jax.ShapeDtypeStruct((num_tokens, d_model), jnp.float32),
                       jax.ShapeDtypeStruct((side - 1, num_tokens, d_model), jnp.float32)),
            in_specs=[hbm, vmem, vmem, hbm, hbm, hbm],
            out_specs=(hbm, hbm),
            scratch_shapes=[
                [pltpu.VMEM((side, num_tokens, width), jnp.bfloat16) for _, width in groups],
                [pltpu.VMEM((side, 2 * plane, num_tokens), jnp.float32) for _ in groups],
                [pltpu.VMEM((side, 2 * plane, num_tokens), jnp.float32) for _ in groups],
                slab[0], slab[1],
                pltpu.VMEM((chunks, side, side, side, 2, SLOTS, d_model), jnp.bfloat16),
                pltpu.VMEM((d_model, d_expert), jnp.bfloat16),
                pltpu.VMEM((d_model, d_expert), jnp.bfloat16),
                pltpu.VMEM((d_expert, d_model), jnp.bfloat16),
                pltpu.VMEM((side, num_tokens, d_model), jnp.float32),
                dma((3,)), dma((3,)), dma((3,)), dma((3,)), dma((3,)), dma((3,)),
                *pair, *pair, *pair, *pair, dma((3,)), dma((3,)), dma,
                pltpu.SemaphoreType.REGULAR((3, chunks)), pltpu.SemaphoreType.REGULAR((3, chunks)),
            ],
            compiler_params=pltpu.CompilerParams(collective_id=0, has_side_effects=True, vmem_limit_bytes=67043328),
            name='moe',
        )(tokens, routes.T, w_router, w_one[0], w_three[0], w_two[0])
        total = y_own
        for i in range(side - 1):
            total = total + y_peers[i]
        return total.astype(jnp.bfloat16)

    return jax.shard_map(device_step, mesh=mesh, in_specs=(row_spec, row_spec, P(None, None), expert_spec, expert_spec, expert_spec), out_specs=row_spec, check_vma=False)
```

```python
import functools

import jax
import jax.numpy as jnp
from jax import lax
from jax.experimental import pallas as pl
from jax.experimental.pallas import tpu as pltpu
from jax.sharding import PartitionSpec as P

MESH = pl.DeviceIdType.MESH
Z, Y, X = 0, 1, 2
ORDERS = ((Z, Y, X), (X, Z, Y), (Y, X, Z))
SLOTS = 8


def slot_capacity(num_tokens, top_k, num_experts):
    return 8 * ((3 * num_tokens * top_k + 16 * num_experts - 1) // (16 * num_experts))


def torus_side(group_size):
    side = 1
    while 2 * side ** 3 < group_size:
        side += 1
    return side


def column_groups(d_model):
    lanes = d_model // 128
    widths = [128 * (lanes // 3 + (1 if i < lanes % 3 else 0)) for i in range(3)]
    starts = [sum(widths[:i]) for i in range(3)]
    return list(zip(starts, widths))


def moved(me, side, axis, steps, core_steps=0):
    digits = [me // (2 * side * side), (me // (2 * side)) % side, (me // 2) % side]
    digits[axis] = (digits[axis] + steps + side) % side
    return ((digits[Z] * side + digits[Y]) * side + digits[X]) * 2 + (me + core_steps) % 2


def expert_order(me, side, order, num_tokens):
    bits = side.bit_length() - 1
    position = lax.broadcasted_iota(jnp.int32, (2 * side ** 3, num_tokens), 0)
    digits = [me // (2 * side * side), (me // (2 * side)) % side, (me // 2) % side]
    for place, axis in enumerate(order):
        steps = jnp.right_shift(position, 1 + (2 - place) * bits)
        digits[axis] = jnp.bitwise_and(digits[axis] + steps, side - 1)
    core = jnp.bitwise_and(me + position, 1)
    return ((digits[Z] * side + digits[Y]) * side + digits[X]) * 2 + core


def moe_kernel(side, chunks, groups, tokens_hbm, routes_ref, w_router, w_one_hbm, w_three_hbm, w_two_hbm, y_own, y_peers,
               toks, plans, own_plans, packed, relay, rows, w_one, w_three, w_two, parts, mids,
               load_sem, w_sem, s0_sem, r0_sem, sp_sem, rp_sem, s1_sem, r1_sem, s2_sem, r2_sem, b1_sem, c1_sem, b2_sem, c2_sem, s3_sem, r3_sem, out_sem, free2_sem, free3_sem):
    me = lax.axis_index('ep')
    dp = lax.axis_index('dp')
    num_tokens = tokens_hbm.shape[0]
    plane = 2 * side * side
    ends = 2 * side
    near = (1, side - 1) if side > 2 else (1,)
    far = side > 2
    packed_rows = plane * SLOTS

    def remote(src, dst, s_sem, r_sem, axis, steps, core_steps=0):
        return pltpu.make_async_remote_copy(
            src_ref=src, dst_ref=dst, send_sem=s_sem, recv_sem=r_sem,
            device_id=(dp, moved(me, side, axis, steps, core_steps)), device_id_type=MESH)

    def columns(g):
        return pl.ds(*groups[g])

    def relay_from(g, q, b):
        return relay[g].at[q, b] if g == 1 else relay[g].at[q, :, b]

    def relay_others(g, q):
        return relay[g].at[q, pl.ds(1, side - 1)] if g == 1 else relay[g].at[q, :, pl.ds(1, side - 1)]

    def rows_at(g, q, e):
        c, core = e // 2, e % 2
        third = ORDERS[g][2]
        where = {Z: (q, c, slice(None), slice(None), core), Y: (q, slice(None), c, slice(None), core),
                 X: (q, slice(None), slice(None), c, core)}[third]
        return where + (slice(None), columns(g))

    def half(i):
        return pl.ds(i * (num_tokens // 2), num_tokens // 2)

    def gather_near(g, d, i):
        part = half(i if d == 0 else 1 - i)
        return remote(tokens_hbm.at[part, columns(g)], toks[g].at[near[d], part],
                      s0_sem.at[g, 2 * d + i], r0_sem.at[g, 2 * d + i], ORDERS[g][0], near[d])

    def gather_far(g, d):
        return remote(toks[g].at[near[d], half(d)], toks[g].at[2, half(d)],
                      s0_sem.at[g, 4 + d], r0_sem.at[g, 4 + d], ORDERS[g][0], near[d])

    def gather_plans(g, a):
        return remote(own_plans[g].at[a], plans[g].at[a], sp_sem.at[g], rp_sem.at[g], ORDERS[g][0], a)

    def gather_plans_all(g):
        others = pl.ds(1, side - 1)
        return remote(plans[g].at[others], plans[g].at[others], sp_sem.at[g], rp_sem.at[g], ORDERS[g][0], 1)

    def relay_slab(g, q, a, b):
        return relay[g].at[q, b, a] if g == 1 else relay[g].at[q, a, b]

    def out_second(g, q, a, b):
        return remote(packed[g].at[q, b, a], relay_slab(g, q, a, b), s1_sem.at[g, q], r1_sem.at[g, q], ORDERS[g][1], b)

    def out_second_all(g, q):
        return remote(packed[g].at[q, pl.ds(1, side - 1)], relay_others(g, q), s1_sem.at[g, q], r1_sem.at[g, q], ORDERS[g][1], 1)

    def out_third(g, q, e):
        return remote(relay[g].at[q, :, :, e], rows.at[rows_at(g, q, e)], s2_sem.at[g, q], r2_sem.at[g, q], ORDERS[g][2], e // 2, e % 2)

    def third_all(g, q, s_sem, r_sem):
        some = relay[g].at[q, :, :, pl.ds(1, ends - 1)]
        return remote(some, some, s_sem.at[g, q], r_sem.at[g, q], ORDERS[g][2], 1)

    def home_third(g, q, e):
        return remote(rows.at[rows_at(g, q, e)], relay[g].at[q, :, :, e], b1_sem.at[g, q], c1_sem.at[g, q], ORDERS[g][2], -(e // 2), e % 2)

    def home_second(g, q, b):
        return remote(relay_from(g, q, b), packed[g].at[q, b], b2_sem.at[g, q], c2_sem.at[g, q], ORDERS[g][1], -b)

    def home_second_all(g, q):
        return remote(relay_others(g, q), packed[g].at[q, pl.ds(1, side - 1)], b2_sem.at[g, q], c2_sem.at[g, q], ORDERS[g][1], 1)

    def home_mid(g, d):
        return remote(parts.at[2, half(d), columns(g)], mids.at[d, :, columns(g)],
                      s3_sem.at[g, d], r3_sem.at[g, d], ORDERS[g][0], -near[d])

    def home_near(g, d, i):
        part = half(1 - d if i == 0 else d)
        return remote(parts.at[near[d], part, columns(g)], y_peers.at[d, part, columns(g)],
                      s3_sem.at[g, 2 + 2 * d + i], r3_sem.at[g, 2 + 2 * d + i], ORDERS[g][0], -near[d])

    def tell(sem, axis, steps, core_steps=0):
        pl.semaphore_signal(sem, inc=1, device_id=(dp, moved(me, side, axis, steps, core_steps)), device_id_type=MESH)

    loads = [pltpu.make_async_copy(tokens_hbm.at[:, columns(g)], toks[g].at[0], load_sem.at[g]) for g in range(3)]
    weights = [pltpu.make_async_copy(src, dst, w_sem.at[i]) for i, (src, dst) in enumerate(
        [(w_one_hbm, w_one), (w_three_hbm, w_three), (w_two_hbm, w_two)])]
    for copy in loads:
        copy.start()

    barrier = pltpu.get_barrier_semaphore()
    tell(barrier, X, 0, 1)
    for axis in (Z, Y, X):
        for steps in range(1, side):
            for core_steps in range(2):
                tell(barrier, axis, steps, core_steps)
    with jax.named_scope('barrier'):
        pl.semaphore_wait(barrier, 1 + 3 * (side - 1) * 2)

    for i in range(2):
        for g in range(3):
            for d in range(len(near)):
                gather_near(g, d, i).start()
    with jax.named_scope('own_wait'):
        for copy in loads:
            copy.wait()

    num_experts = 2 * side ** 3
    logits = sum(jnp.dot(toks[g][0], w_router[columns(g), :], preferred_element_type=jnp.float32) for g in range(3)).T
    ids = lax.broadcasted_iota(jnp.int32, (num_experts, num_tokens), 0)
    top_k = routes_ref.shape[0]
    picks = [routes_ref[k:k + 1, :] for k in range(top_k)]
    scores = [jnp.sum(jnp.where(pick == ids, logits, 0.0), axis=0, keepdims=True) for pick in picks]
    peak = functools.reduce(jnp.maximum, scores)
    scores = [jnp.exp(score - peak) for score in scores]
    norm = sum(scores)
    gates = [score / norm for score in scores]
    before = (lax.broadcasted_iota(jnp.int32, (num_tokens, num_tokens), 0)
              < lax.broadcasted_iota(jnp.int32, (num_tokens, num_tokens), 1))
    before = jnp.where(before, 1.0, 0.0).astype(jnp.bfloat16)
    for g in range(3):
        expert_at = expert_order(me, side, ORDERS[g], num_tokens)
        mask = jnp.zeros((num_experts, num_tokens), jnp.float32)
        gate = jnp.zeros((num_experts, num_tokens), jnp.float32)
        for k in range(top_k):
            hit = picks[k] == expert_at
            mask = jnp.where(hit, 1.0, mask)
            gate = jnp.where(hit, gates[k], gate)
        slot = jnp.dot(mask.astype(jnp.bfloat16), before, preferred_element_type=jnp.float32)
        slot = jnp.where(mask > 0.0, slot, -1.0)
        plans[g][0, pl.ds(0, plane), :] = slot[:plane]
        plans[g][0, pl.ds(plane, plane), :] = gate[:plane]
        for a in range(1, side):
            own_plans[g][a, pl.ds(0, plane), :] = slot[a * plane:(a + 1) * plane]
            own_plans[g][a, pl.ds(plane, plane), :] = gate[a * plane:(a + 1) * plane]
        for a in range(1, side):
            gather_plans(g, a).start()
    for copy in weights:
        copy.start()

    def taken(g, q, a):
        slots = plans[g][a, pl.ds(0, plane), :]
        ids = lax.broadcasted_iota(jnp.int32, (plane, SLOTS, num_tokens), 1) + q * SLOTS
        return jnp.broadcast_to(slots[:, None, :], (plane, SLOTS, num_tokens)) == ids.astype(jnp.float32)

    def pack(g, q, a):
        select = jnp.where(taken(g, q, a), 1.0, 0.0).reshape(packed_rows, num_tokens).astype(jnp.bfloat16)
        out = jnp.dot(select, toks[g][a], preferred_element_type=jnp.float32)
        out = out.reshape(side, ends, SLOTS, groups[g][1]).astype(jnp.bfloat16)
        packed[g][q, pl.ds(1, side - 1), a] = out[1:]
        for b in range(1, side):
            out_second(g, q, a, b).start()
        relay_slab(g, q, a, 0)[...] = out[0]

    def pack_own(q, carry):
        for g in range(3):
            pack(g, q, 0)
        return carry

    if far:
        with jax.named_scope('gather_far'):
            for g in range(3):
                for d in range(2):
                    gather_near(g, d, 0).wait_recv()
                    gather_far(g, d).start()
    with jax.named_scope('pack_own'):
        lax.fori_loop(0, chunks, pack_own, 0)
    parts[...] = jnp.zeros_like(parts)
    with jax.named_scope('gather_wait'):
        for g in range(3):
            gather_plans_all(g).wait_recv()
            for d in range(len(near)):
                if not far:
                    gather_near(g, d, 0).wait_recv()
                gather_near(g, d, 1).wait_recv()
            if far:
                gather_far(g, 0).wait_recv()
                gather_far(g, 1).wait_recv()

    def outward(i, carry):
        @pl.when(i < chunks)
        def _():
            for g in range(3):
                def source(a, c):
                    pack(g, i, a)
                    return c
                with jax.named_scope('pack'):
                    lax.fori_loop(1, side, source, 0)

        @pl.when(i > 0)
        def _():
            forward(i - 1)
        return carry

    def forward(q):
        for g in range(3):
            with jax.named_scope('s1_wait'):
                out_second_all(g, q).wait_recv()
            for e in range(1, ends):
                out_third(g, q, e).start()
            rows[rows_at(g, q, 0)] = relay[g][q, :, :, 0]
            with jax.named_scope('s1_send_wait'):
                out_second_all(g, q).wait_send()
            for b in range(1, side):
                tell(free2_sem.at[g, q], ORDERS[g][1], b)

    lax.fori_loop(0, chunks + 1, outward, 0)
    for copy in weights:
        copy.wait()

    def experts(q, carry):
        with jax.named_scope('s2_wait'):
            for g in range(3):
                third_all(g, q, s2_sem, r2_sem).wait_recv()
        for g in range(3):
            with jax.named_scope('s2_send_wait'):
                third_all(g, q, s2_sem, r2_sem).wait_send()
            for e in range(1, ends):
                tell(free3_sem.at[g, q], ORDERS[g][2], e // 2, e % 2)

        def block(z, c):
            shape = rows.shape[2:]
            u = rows[q, z].astype(jnp.float32).reshape(packed_rows, shape[-1]).astype(jnp.bfloat16)
            gate_pre = jnp.dot(u, w_one[...], preferred_element_type=jnp.float32)
            up_pre = jnp.dot(u, w_three[...], preferred_element_type=jnp.float32)
            hidden = (jax.nn.silu(gate_pre) * up_pre).astype(jnp.bfloat16)
            out = jnp.dot(hidden, w_two[...], preferred_element_type=jnp.float32)
            rows[q, z] = out.reshape(shape).astype(jnp.bfloat16)
            return c
        with jax.named_scope('mlp'):
            lax.fori_loop(0, side, block, 0)
        for g in range(3):
            with jax.named_scope('free3'):
                pl.semaphore_wait(free3_sem.at[g, q], ends - 1)
            for e in range(1, ends):
                home_third(g, q, e).start()
            relay[g][q, :, :, 0] = rows[rows_at(g, q, 0)]
        return carry

    lax.fori_loop(0, chunks, experts, 0)

    def backward(q):
        for g in range(3):
            with jax.named_scope('r1_wait'):
                third_all(g, q, b1_sem, c1_sem).wait_recv()
            pl.semaphore_wait(free2_sem.at[g, q], side - 1)
            for b in range(1, side):
                home_second(g, q, b).start()
            packed[g][q, 0] = relay_from(g, q, 0)[...]

    def combine(q):
        for g in (1, 2, 0):
            with jax.named_scope('r2_wait'):
                home_second_all(g, q).wait_recv()
            width = groups[g][1]

            def source(i, c):
                a = (i + side // 2) % side
                gates = plans[g][a, pl.ds(plane, plane), :]
                used = taken(g, q, a)
                o = packed[g][q, :, a].astype(jnp.float32).reshape(packed_rows, width).astype(jnp.bfloat16)
                total = None
                for _ in range(3):
                    part = gates.astype(jnp.bfloat16).astype(jnp.float32)
                    gates = gates - part
                    mix = jnp.where(used, jnp.broadcast_to(part[:, None, :], used.shape), 0.0).reshape(packed_rows, num_tokens).astype(jnp.bfloat16)
                    term = lax.dot_general(mix, o, (((0,), (0,)), ((), ())), preferred_element_type=jnp.float32)
                    total = term if total is None else total + term
                parts[a, :, columns(g)] += total

                last = q == chunks - 1
                if far:
                    @pl.when(jnp.logical_and(last, a == 2))
                    def _():
                        home_mid(g, 0).start()
                        home_mid(g, 1).start()
                for d in range(len(near)):
                    @pl.when(jnp.logical_and(last, a == near[d]))
                    def _():
                        home_near(g, d, 0).start()
                return c
            with jax.named_scope('combine'):
                lax.fori_loop(0, side, source, 0)

    def homeward(i, carry):
        @pl.when(i < chunks)
        def _():
            backward(i)

        @pl.when(i > 0)
        def _():
            combine(i - 1)
        return carry

    lax.fori_loop(0, chunks + 1, homeward, 0)
    own = pltpu.make_async_copy(parts.at[0], y_own, out_sem)
    own.start()
    for g in (1, 2, 0):
        for d in range(len(near)):
            if far:
                with jax.named_scope('mid_wait'):
                    home_mid(g, d).wait_recv()
                parts[near[d], half(d), columns(g)] += mids[d, :, columns(g)]
            home_near(g, d, 1).start()

    for g in range(3):
        def drain(q, c):
            third_all(g, q, b1_sem, c1_sem).wait_send()
            home_second_all(g, q).wait_send()
            return c
        lax.fori_loop(0, chunks, drain, 0)
        gather_plans_all(g).wait_send()
        for d in range(len(near)):
            gather_near(g, d, 0).wait_send()
            gather_near(g, d, 1).wait_send()
            if far:
                gather_far(g, d).wait_send()
                home_mid(g, d).wait_send()
    for g in (1, 2, 0):
        for d in range(len(near)):
            for i in range(2):
                with jax.named_scope('r3_wait'):
                    home_near(g, d, i).wait_recv()
                    home_near(g, d, i).wait_send()
    own.wait()


def solution(mesh):
    group_size = mesh.shape['ep']
    side = torus_side(group_size)
    row_spec = P(('dp', 'ep'), None)
    expert_spec = P('ep', None, None)

    def device_step(tokens, routes, w_router, w_one, w_three, w_two):
        num_tokens, d_model = tokens.shape
        top_k = routes.shape[1]
        num_experts = w_router.shape[1]
        d_expert = w_one.shape[2]
        capacity = slot_capacity(num_tokens, top_k, num_experts)
        chunks = capacity // SLOTS
        groups = column_groups(d_model)
        plane = 2 * side * side
        hbm = pl.BlockSpec(memory_space=pl.ANY)
        vmem = pl.BlockSpec(memory_space=pltpu.VMEM)
        dma = pltpu.SemaphoreType.DMA
        slab = [[pltpu.VMEM((chunks, side, side, 2 * side, SLOTS, width), jnp.bfloat16) for _, width in groups] for _ in range(2)]
        pair = [dma((3, chunks)), dma((3, chunks))]
        y_own, y_peers = pl.pallas_call(
            functools.partial(moe_kernel, side, chunks, groups),
            out_shape=(jax.ShapeDtypeStruct((num_tokens, d_model), jnp.float32),
                       jax.ShapeDtypeStruct((2 if side > 2 else 1, num_tokens, d_model), jnp.float32)),
            in_specs=[hbm, vmem, vmem, hbm, hbm, hbm],
            out_specs=(hbm, hbm),
            scratch_shapes=[
                [pltpu.VMEM((side, num_tokens, width), jnp.bfloat16) for _, width in groups],
                [pltpu.VMEM((side, 2 * plane, num_tokens), jnp.float32) for _ in groups],
                [pltpu.VMEM((side, 2 * plane, num_tokens), jnp.float32) for _ in groups],
                slab[0], slab[1],
                pltpu.VMEM((chunks, side, side, side, 2, SLOTS, d_model), jnp.bfloat16),
                pltpu.VMEM((d_model, d_expert), jnp.bfloat16),
                pltpu.VMEM((d_model, d_expert), jnp.bfloat16),
                pltpu.VMEM((d_expert, d_model), jnp.bfloat16),
                pltpu.VMEM((side, num_tokens, d_model), jnp.float32),
                pltpu.VMEM((2, num_tokens // 2, d_model), jnp.float32),
                dma((3,)), dma((3,)), dma((3, 6)), dma((3, 6)), dma((3,)), dma((3,)),
                *pair, *pair, *pair, *pair, dma((3, 6)), dma((3, 6)), dma,
                pltpu.SemaphoreType.REGULAR((3, chunks)), pltpu.SemaphoreType.REGULAR((3, chunks)),
            ],
            compiler_params=pltpu.CompilerParams(collective_id=0, has_side_effects=True, vmem_limit_bytes=67043328),
            name='moe',
        )(tokens, routes.T, w_router, w_one[0], w_three[0], w_two[0])
        total = y_own
        for i in range(y_peers.shape[0]):
            total = total + y_peers[i]
        return total.astype(jnp.bfloat16)

    return jax.shard_map(device_step, mesh=mesh, in_specs=(row_spec, row_spec, P(None, None), expert_spec, expert_spec, expert_spec), out_specs=row_spec, check_vma=False)
```

```python
import functools

import jax
import jax.numpy as jnp
from jax import lax
from jax.experimental import pallas as pl
from jax.experimental.pallas import tpu as pltpu
from jax.sharding import PartitionSpec as P

MESH = pl.DeviceIdType.MESH
Z, Y, X = 0, 1, 2
ORDERS = ((Z, Y, X), (X, Z, Y), (Y, X, Z))
SLOTS = 8


def slot_capacity(num_tokens, top_k, num_experts):
    return 8 * ((3 * num_tokens * top_k + 16 * num_experts - 1) // (16 * num_experts))


def torus_side(group_size):
    side = 1
    while 2 * side ** 3 < group_size:
        side += 1
    return side


def column_groups(d_model):
    lanes = d_model // 128
    count = 6 if lanes >= 6 else 3
    widths = [128 * (lanes // count + (1 if i < lanes % count else 0)) for i in range(count)]
    starts = [sum(widths[:i]) for i in range(count)]
    return list(zip(starts, widths))


def moved(me, side, axis, steps, core_steps=0):
    digits = [me // (2 * side * side), (me // (2 * side)) % side, (me // 2) % side]
    digits[axis] = (digits[axis] + steps + side) % side
    return ((digits[Z] * side + digits[Y]) * side + digits[X]) * 2 + (me + core_steps) % 2


def plane_experts(me, side, order, num_tokens):
    bits = side.bit_length() - 1
    position = lax.broadcasted_iota(jnp.int32, (2 * side * side, num_tokens), 0)
    digits = [me // (2 * side * side), (me // (2 * side)) % side, (me // 2) % side]
    for place, axis in enumerate(order[1:]):
        steps = jnp.right_shift(position, 1 + (1 - place) * bits)
        digits[axis] = jnp.bitwise_and(digits[axis] + steps, side - 1)
    core = jnp.bitwise_and(me + position, 1)
    return ((digits[Z] * side + digits[Y]) * side + digits[X]) * 2 + core


def each(first, end, act):
    def step(i, carry):
        act(i)
        return carry
    lax.fori_loop(first, end, step, 0)


def moe_kernel(side, chunks, groups, tokens_hbm, routes_ref, w_router, w_one_hbm, w_three_hbm, w_two_hbm, y_own, y_peers,
               toks, infos, own_info, plans, packed, relay, rows, w_one, w_three, w_two, parts, mids,
               load_sem, w_sem, s0_sem, r0_sem, sp_sem, rp_sem, s1_sem, r1_sem, s2_sem, r2_sem, b1_sem, c1_sem, b2_sem, c2_sem, s3_sem, r3_sem, out_sem, free2_sem, free3_sem):
    me = lax.axis_index('ep')
    dp = lax.axis_index('dp')
    num_tokens = tokens_hbm.shape[0]
    plane = 2 * side * side
    ends = 2 * side
    count = len(groups)
    arrival = (1, 4, 0, 2, 3, 5) if count == 6 else (1, 0, 2)
    near = (1, side - 1) if side > 2 else (1,)
    far = side > 2
    packed_rows = plane * SLOTS
    top_k = routes_ref.shape[0]
    orders = [ORDERS[g % 3] for g in range(count)]

    def remote(src, dst, s_sem, r_sem, axis, steps, core_steps=0):
        return pltpu.make_async_remote_copy(
            src_ref=src, dst_ref=dst, send_sem=s_sem, recv_sem=r_sem,
            device_id=(dp, moved(me, side, axis, steps, core_steps)), device_id_type=MESH)

    def columns(g):
        return pl.ds(*groups[g])

    def relay_from(g, q, b):
        return relay[g].at[q, b] if g % 3 == 1 else relay[g].at[q, :, b]

    def relay_others(g, q):
        return relay[g].at[q, pl.ds(1, side - 1)] if g % 3 == 1 else relay[g].at[q, :, pl.ds(1, side - 1)]

    def rows_at(g, q, e):
        c, core = e // 2, e % 2
        third = orders[g][2]
        where = {Z: (q, c, slice(None), slice(None), core), Y: (q, slice(None), c, slice(None), core),
                 X: (q, slice(None), slice(None), c, core)}[third]
        return where + (slice(None), columns(g))

    def half(i):
        return pl.ds(i * (num_tokens // 2), num_tokens // 2)

    def gather_near(g, d, i):
        part = half(i if d == 0 else 1 - i)
        return remote(tokens_hbm.at[part, columns(g)], toks[g].at[near[d], part],
                      s0_sem.at[g, 2 * d + i], r0_sem.at[g, 2 * d + i], orders[g][0], near[d])

    def gather_far(g, d):
        return remote(toks[g].at[near[d], half(d)], toks[g].at[2, half(d)],
                      s0_sem.at[g, 4 + d], r0_sem.at[g, 4 + d], orders[g][0], near[d])

    def gather_info(o, a):
        return remote(own_info, infos.at[o, a], sp_sem.at[o], rp_sem.at[o], ORDERS[o][0], a)

    def gather_info_all(o):
        others = infos.at[o, pl.ds(1, side - 1)]
        return remote(others, others, sp_sem.at[o], rp_sem.at[o], ORDERS[o][0], 1)

    def relay_slab(g, q, a, b):
        return relay[g].at[q, b, a] if g % 3 == 1 else relay[g].at[q, a, b]

    def out_second(g, q, a, b):
        return remote(packed[g].at[q, b, a], relay_slab(g, q, a, b), s1_sem.at[g, q], r1_sem.at[g, q], orders[g][1], b)

    def out_second_all(g, q):
        return remote(packed[g].at[q, pl.ds(1, side - 1)], relay_others(g, q), s1_sem.at[g, q], r1_sem.at[g, q], orders[g][1], 1)

    def out_third(g, q, e):
        return remote(relay[g].at[q, :, :, e], rows.at[rows_at(g, q, e)], s2_sem.at[g, q], r2_sem.at[g, q], orders[g][2], e // 2, e % 2)

    def third_all(g, q, s_sem, r_sem):
        some = relay[g].at[q, :, :, pl.ds(1, ends - 1)]
        return remote(some, some, s_sem.at[g, q], r_sem.at[g, q], orders[g][2], 1)

    def home_third(g, q, e):
        return remote(rows.at[rows_at(g, q, e)], relay[g].at[q, :, :, e], b1_sem.at[g, q], c1_sem.at[g, q], orders[g][2], -(e // 2), e % 2)

    def home_second(g, q, b):
        return remote(relay_from(g, q, b), packed[g].at[q, b], b2_sem.at[g, q], c2_sem.at[g, q], orders[g][1], -b)

    def home_second_all(g, q):
        return remote(relay_others(g, q), packed[g].at[q, pl.ds(1, side - 1)], b2_sem.at[g, q], c2_sem.at[g, q], orders[g][1], 1)

    def home_mid(g, d):
        return remote(parts.at[2, half(d), columns(g)], mids.at[d, :, columns(g)],
                      s3_sem.at[g, d], r3_sem.at[g, d], orders[g][0], -near[d])

    def home_near(g, d, i):
        part = half(1 - d if i == 0 else d)
        return remote(parts.at[near[d], part, columns(g)], y_peers.at[d, part, columns(g)],
                      s3_sem.at[g, 2 + 2 * d + i], r3_sem.at[g, 2 + 2 * d + i], orders[g][0], -near[d])

    def tell(sem, axis, steps, core_steps=0):
        pl.semaphore_signal(sem, inc=1, device_id=(dp, moved(me, side, axis, steps, core_steps)), device_id_type=MESH)

    loads = [pltpu.make_async_copy(tokens_hbm.at[:, columns(g)], toks[g].at[0], load_sem.at[g]) for g in range(count)]
    weights = [pltpu.make_async_copy(src, dst, w_sem.at[i]) for i, (src, dst) in enumerate(
        [(w_one_hbm, w_one), (w_three_hbm, w_three), (w_two_hbm, w_two)])]
    for copy in loads:
        copy.start()

    barrier = pltpu.get_barrier_semaphore()
    tell(barrier, X, 0, 1)
    for axis in (Z, Y, X):
        for steps in range(1, side):
            for core_steps in range(2):
                tell(barrier, axis, steps, core_steps)
    with jax.named_scope('barrier'):
        pl.semaphore_wait(barrier, 1 + 3 * (side - 1) * 2)

    for i in range(2):
        for g in range(count):
            for d in range(len(near)):
                gather_near(g, d, i).start()
    with jax.named_scope('own_wait'):
        for copy in loads:
            copy.wait()

    num_experts = 2 * side ** 3
    logits = sum(jnp.dot(toks[g][0], w_router[columns(g), :], preferred_element_type=jnp.float32) for g in range(count)).T
    ids = lax.broadcasted_iota(jnp.int32, (num_experts, num_tokens), 0)
    picks = [routes_ref[k:k + 1, :] for k in range(top_k)]
    scores = [jnp.sum(jnp.where(pick == ids, logits, 0.0), axis=0, keepdims=True) for pick in picks]
    peak = functools.reduce(jnp.maximum, scores)
    scores = [jnp.exp(score - peak) for score in scores]
    norm = sum(scores)
    for k in range(top_k):
        own_info[k:k + 1, :] = picks[k].astype(jnp.float32)
        own_info[top_k + k:top_k + k + 1, :] = scores[k] / norm
    for o in range(3):
        for a in range(1, side):
            gather_info(o, a).start()
    before = (lax.broadcasted_iota(jnp.int32, (num_tokens, num_tokens), 0)
              < lax.broadcasted_iota(jnp.int32, (num_tokens, num_tokens), 1))
    before = jnp.where(before, 1.0, 0.0).astype(jnp.bfloat16)
    expert_at = [plane_experts(me, side, order, num_tokens).astype(jnp.float32) for order in ORDERS]

    def make_plan(o, a, info):
        mask = jnp.zeros((plane, num_tokens), jnp.float32)
        gate = jnp.zeros((plane, num_tokens), jnp.float32)
        for k in range(top_k):
            hit = info[k:k + 1] == expert_at[o]
            mask = jnp.where(hit, 1.0, mask)
            gate = jnp.where(hit, info[top_k + k:top_k + k + 1], gate)
        slot = jnp.dot(mask.astype(jnp.bfloat16), before, preferred_element_type=jnp.float32)
        plans[o][a, pl.ds(0, plane), :] = jnp.where(mask > 0.0, slot, -1.0)
        plans[o][a, pl.ds(plane, plane), :] = gate

    for o in range(3):
        make_plan(o, 0, own_info[...])
    for copy in weights:
        copy.start()

    def taken(g, q, a):
        slots = plans[g % 3][a, pl.ds(0, plane), :]
        ids = lax.broadcasted_iota(jnp.int32, (plane, SLOTS, num_tokens), 1) + q * SLOTS
        return jnp.broadcast_to(slots[:, None, :], (plane, SLOTS, num_tokens)) == ids.astype(jnp.float32)

    def pack(g, q, a):
        select = jnp.where(taken(g, q, a), 1.0, 0.0).reshape(packed_rows, num_tokens).astype(jnp.bfloat16)
        out = jnp.dot(select, toks[g][a], preferred_element_type=jnp.float32)
        out = out.reshape(side, ends, SLOTS, groups[g][1]).astype(jnp.bfloat16)
        packed[g][q, pl.ds(1, side - 1), a] = out[1:]
        each(1, side, lambda b: out_second(g, q, a, b).start())
        relay_slab(g, q, a, 0)[...] = out[0]

    def pack_own(q, carry):
        for g in range(count):
            pack(g, q, 0)
        return carry

    if far:
        with jax.named_scope('gather_far'):
            for g in range(count):
                for d in range(2):
                    gather_near(g, d, 0).wait_recv()
                    gather_far(g, d).start()
    with jax.named_scope('pack_own'):
        lax.fori_loop(0, chunks, pack_own, 0)
    parts[...] = jnp.zeros_like(parts)
    with jax.named_scope('gather_wait'):
        for o in range(3):
            gather_info_all(o).wait_recv()
            for a in range(1, side):
                make_plan(o, a, infos[o, a])
        for g in range(count):
            for d in range(len(near)):
                if not far:
                    gather_near(g, d, 0).wait_recv()
                gather_near(g, d, 1).wait_recv()
            if far:
                gather_far(g, 0).wait_recv()
                gather_far(g, 1).wait_recv()

    def outward(i, carry):
        @pl.when(i < chunks)
        def _():
            for g in range(count):
                def source(a, c):
                    pack(g, i, a)
                    return c
                with jax.named_scope('pack'):
                    lax.fori_loop(1, side, source, 0)

        @pl.when(i > 0)
        def _():
            forward(i - 1)
        return carry

    def forward(q):
        for g in range(count):
            with jax.named_scope('s1_wait'):
                out_second_all(g, q).wait_recv()
            each(1, ends, lambda e: out_third(g, q, e).start())
            rows[rows_at(g, q, 0)] = relay[g][q, :, :, 0]
            with jax.named_scope('s1_send_wait'):
                out_second_all(g, q).wait_send()
            each(1, side, lambda b: tell(free2_sem.at[g, q], orders[g][1], b))

    lax.fori_loop(0, chunks + 1, outward, 0)
    for copy in weights:
        copy.wait()

    def experts(q, carry):
        with jax.named_scope('s2_wait'):
            for g in range(count):
                third_all(g, q, s2_sem, r2_sem).wait_recv()
        for g in range(count):
            with jax.named_scope('s2_send_wait'):
                third_all(g, q, s2_sem, r2_sem).wait_send()
            each(1, ends, lambda e: tell(free3_sem.at[g, q], orders[g][2], e // 2, e % 2))

        def block(z, c):
            shape = rows.shape[2:]
            u = rows[q, z].astype(jnp.float32).reshape(packed_rows, shape[-1]).astype(jnp.bfloat16)
            gate_pre = jnp.dot(u, w_one[...], preferred_element_type=jnp.float32)
            up_pre = jnp.dot(u, w_three[...], preferred_element_type=jnp.float32)
            hidden = (jax.nn.silu(gate_pre) * up_pre).astype(jnp.bfloat16)
            out = jnp.dot(hidden, w_two[...], preferred_element_type=jnp.float32)
            rows[q, z] = out.reshape(shape).astype(jnp.bfloat16)
            return c
        with jax.named_scope('mlp'):
            lax.fori_loop(0, side, block, 0)
        for g in range(count):
            with jax.named_scope('free3'):
                pl.semaphore_wait(free3_sem.at[g, q], ends - 1)
            each(1, ends, lambda e: home_third(g, q, e).start())
            relay[g][q, :, :, 0] = rows[rows_at(g, q, 0)]
        return carry

    lax.fori_loop(0, chunks, experts, 0)

    def backward(q):
        for g in range(count):
            with jax.named_scope('r1_wait'):
                third_all(g, q, b1_sem, c1_sem).wait_recv()
            pl.semaphore_wait(free2_sem.at[g, q], side - 1)
            each(1, side, lambda b: home_second(g, q, b).start())
            packed[g][q, 0] = relay_from(g, q, 0)[...]

    def combine(q):
        for g in arrival:
            with jax.named_scope('r2_wait'):
                home_second_all(g, q).wait_recv()
            width = groups[g][1]

            def source(i, c):
                a = (i + side // 2) % side
                gates = plans[g % 3][a, pl.ds(plane, plane), :]
                used = taken(g, q, a)
                o = packed[g][q, :, a].astype(jnp.float32).reshape(packed_rows, width).astype(jnp.bfloat16)
                total = None
                for _ in range(3):
                    part = gates.astype(jnp.bfloat16).astype(jnp.float32)
                    gates = gates - part
                    mix = jnp.where(used, jnp.broadcast_to(part[:, None, :], used.shape), 0.0).reshape(packed_rows, num_tokens).astype(jnp.bfloat16)
                    term = lax.dot_general(mix, o, (((0,), (0,)), ((), ())), preferred_element_type=jnp.float32)
                    total = term if total is None else total + term
                parts[a, :, columns(g)] += total

                last = q == chunks - 1
                if far:
                    @pl.when(jnp.logical_and(last, a == 2))
                    def _():
                        home_mid(g, 0).start()
                        home_mid(g, 1).start()
                for d in range(len(near)):
                    @pl.when(jnp.logical_and(last, a == near[d]))
                    def _():
                        home_near(g, d, 0).start()
                return c
            with jax.named_scope('combine'):
                lax.fori_loop(0, side, source, 0)

    def send_home(q, carry):
        backward(q)
        return carry

    def sum_up(q, carry):
        combine(q)
        return carry

    lax.fori_loop(0, chunks, send_home, 0)
    lax.fori_loop(0, chunks, sum_up, 0)
    own = pltpu.make_async_copy(parts.at[0], y_own, out_sem)
    own.start()
    for g in arrival:
        for d in range(len(near)):
            if far:
                with jax.named_scope('mid_wait'):
                    home_mid(g, d).wait_recv()
                parts[near[d], half(d), columns(g)] += mids[d, :, columns(g)]
            home_near(g, d, 1).start()

    for g in range(count):
        def drain(q, c):
            third_all(g, q, b1_sem, c1_sem).wait_send()
            home_second_all(g, q).wait_send()
            return c
        lax.fori_loop(0, chunks, drain, 0)
        for d in range(len(near)):
            gather_near(g, d, 0).wait_send()
            gather_near(g, d, 1).wait_send()
            if far:
                gather_far(g, d).wait_send()
                home_mid(g, d).wait_send()
    for o in range(3):
        gather_info_all(o).wait_send()
    for g in arrival:
        for d in range(len(near)):
            for i in range(2):
                with jax.named_scope('r3_wait'):
                    home_near(g, d, i).wait_recv()
                    home_near(g, d, i).wait_send()
    own.wait()


def solution(mesh):
    group_size = mesh.shape['ep']
    side = torus_side(group_size)
    row_spec = P(('dp', 'ep'), None)
    expert_spec = P('ep', None, None)

    def device_step(tokens, routes, w_router, w_one, w_three, w_two):
        num_tokens, d_model = tokens.shape
        top_k = routes.shape[1]
        num_experts = w_router.shape[1]
        d_expert = w_one.shape[2]
        capacity = slot_capacity(num_tokens, top_k, num_experts)
        chunks = capacity // SLOTS
        groups = column_groups(d_model)
        count = len(groups)
        plane = 2 * side * side
        hbm = pl.BlockSpec(memory_space=pl.ANY)
        vmem = pl.BlockSpec(memory_space=pltpu.VMEM)
        dma = pltpu.SemaphoreType.DMA
        slab = [[pltpu.VMEM((chunks, side, side, 2 * side, SLOTS, width), jnp.bfloat16) for _, width in groups] for _ in range(2)]
        pair = [dma((count, chunks)), dma((count, chunks))]
        y_own, y_peers = pl.pallas_call(
            functools.partial(moe_kernel, side, chunks, groups),
            out_shape=(jax.ShapeDtypeStruct((num_tokens, d_model), jnp.float32),
                       jax.ShapeDtypeStruct((2 if side > 2 else 1, num_tokens, d_model), jnp.float32)),
            in_specs=[hbm, vmem, vmem, hbm, hbm, hbm],
            out_specs=(hbm, hbm),
            scratch_shapes=[
                [pltpu.VMEM((side, num_tokens, width), jnp.bfloat16) for _, width in groups],
                pltpu.VMEM((3, side, 2 * top_k, num_tokens), jnp.float32),
                pltpu.VMEM((2 * top_k, num_tokens), jnp.float32),
                [pltpu.VMEM((side, 2 * plane, num_tokens), jnp.float32) for _ in ORDERS],
                slab[0], slab[1],
                pltpu.VMEM((chunks, side, side, side, 2, SLOTS, d_model), jnp.bfloat16),
                pltpu.VMEM((d_model, d_expert), jnp.bfloat16),
                pltpu.VMEM((d_model, d_expert), jnp.bfloat16),
                pltpu.VMEM((d_expert, d_model), jnp.bfloat16),
                pltpu.VMEM((side, num_tokens, d_model), jnp.float32),
                pltpu.VMEM((2, num_tokens // 2, d_model), jnp.float32),
                dma((count,)), dma((3,)), dma((count, 6)), dma((count, 6)), dma((3,)), dma((3,)),
                *pair, *pair, *pair, *pair, dma((count, 6)), dma((count, 6)), dma,
                pltpu.SemaphoreType.REGULAR((count, chunks)), pltpu.SemaphoreType.REGULAR((count, chunks)),
            ],
            compiler_params=pltpu.CompilerParams(collective_id=0, has_side_effects=True, vmem_limit_bytes=67043328),
            name='moe',
        )(tokens, routes.T, w_router, w_one[0], w_three[0], w_two[0])
        total = y_own
        for i in range(y_peers.shape[0]):
            total = total + y_peers[i]
        return total.astype(jnp.bfloat16)

    return jax.shard_map(device_step, mesh=mesh, in_specs=(row_spec, row_spec, P(None, None), expert_spec, expert_spec, expert_spec), out_specs=row_spec, check_vma=False)
```

```python
import functools

import jax
import jax.numpy as jnp
from jax import lax
from jax.experimental import pallas as pl
from jax.experimental.pallas import tpu as pltpu
from jax.sharding import PartitionSpec as P

MESH = pl.DeviceIdType.MESH
Z, Y, X = 0, 1, 2
ORDERS = ((Z, Y, X), (X, Z, Y), (Y, X, Z))
SLOTS = 8


def slot_capacity(num_tokens, top_k, num_experts):
    return 8 * ((3 * num_tokens * top_k + 16 * num_experts - 1) // (16 * num_experts))


def torus_side(group_size):
    side = 1
    while 2 * side ** 3 < group_size:
        side += 1
    return side


def column_groups(d_model):
    lanes = d_model // 128
    count = 6 if lanes >= 6 else 3
    widths = [128 * (lanes // count + (1 if i < lanes % count else 0)) for i in range(count)]
    starts = [sum(widths[:i]) for i in range(count)]
    return list(zip(starts, widths))


def moved(me, side, axis, steps, core_steps=0):
    digits = [me // (2 * side * side), (me // (2 * side)) % side, (me // 2) % side]
    digits[axis] = (digits[axis] + steps + side) % side
    return ((digits[Z] * side + digits[Y]) * side + digits[X]) * 2 + (me + core_steps) % 2


def plane_experts(me, side, order, num_tokens):
    bits = side.bit_length() - 1
    position = lax.broadcasted_iota(jnp.int32, (2 * side * side, num_tokens), 0)
    digits = [me // (2 * side * side), (me // (2 * side)) % side, (me // 2) % side]
    for place, axis in enumerate(order[1:]):
        steps = jnp.right_shift(position, 1 + (1 - place) * bits)
        digits[axis] = jnp.bitwise_and(digits[axis] + steps, side - 1)
    core = jnp.bitwise_and(me + position, 1)
    return ((digits[Z] * side + digits[Y]) * side + digits[X]) * 2 + core


def each(first, end, act):
    def step(i, carry):
        act(i)
        return carry
    lax.fori_loop(first, end, step, 0)


def moe_kernel(side, chunks, groups, tokens_hbm, routes_ref, w_router_hbm, w_one_hbm, w_three_hbm, w_two_hbm, y_own, y_peers,
               toks, infos, own_info, plans, packed, relay, rows, w_router, w_one, w_three, w_two, parts, mids,
               load_sem, w_sem, s0_sem, r0_sem, sp_sem, rp_sem, s1_sem, r1_sem, s2_sem, r2_sem, b1_sem, c1_sem, b2_sem, c2_sem, s3_sem, r3_sem, out_sem, free2_sem, free3_sem):
    me = lax.axis_index('ep')
    dp = lax.axis_index('dp')
    num_tokens = tokens_hbm.shape[0]
    plane = 2 * side * side
    ends = 2 * side
    count = len(groups)
    arrival = (0, 2, 1, 4, 3, 5) if count == 6 else (1, 0, 2)
    near = (1, side - 1) if side > 2 else (1,)
    far = side > 2
    packed_rows = plane * SLOTS
    top_k = routes_ref.shape[0]
    orders = [ORDERS[g % 3] for g in range(count)]

    def remote(src, dst, s_sem, r_sem, axis, steps, core_steps=0):
        return pltpu.make_async_remote_copy(
            src_ref=src, dst_ref=dst, send_sem=s_sem, recv_sem=r_sem,
            device_id=(dp, moved(me, side, axis, steps, core_steps)), device_id_type=MESH)

    def columns(g):
        return pl.ds(*groups[g])

    def relay_from(g, q, b):
        return relay[g].at[q, b] if g % 3 == 1 else relay[g].at[q, :, b]

    def relay_others(g, q):
        return relay[g].at[q, pl.ds(1, side - 1)] if g % 3 == 1 else relay[g].at[q, :, pl.ds(1, side - 1)]

    def rows_at(g, q, e):
        c, core = e // 2, e % 2
        third = orders[g][2]
        where = {Z: (q, c, slice(None), slice(None), core), Y: (q, slice(None), c, slice(None), core),
                 X: (q, slice(None), slice(None), c, core)}[third]
        return where + (slice(None), columns(g))

    def half(i):
        return pl.ds(i * (num_tokens // 2), num_tokens // 2)

    def gather_near(g, d, i):
        part = half(i if d == 0 else 1 - i)
        return remote(tokens_hbm.at[part, columns(g)], toks[g].at[near[d], part],
                      s0_sem.at[g, 2 * d + i], r0_sem.at[g, 2 * d + i], orders[g][0], near[d])

    def gather_far(g, d):
        return remote(toks[g].at[near[d], half(d)], toks[g].at[2, half(d)],
                      s0_sem.at[g, 4 + d], r0_sem.at[g, 4 + d], orders[g][0], near[d])

    def gather_info(o, a):
        return remote(own_info, infos.at[o, a], sp_sem.at[o], rp_sem.at[o], ORDERS[o][0], a)

    def gather_info_all(o):
        others = infos.at[o, pl.ds(1, side - 1)]
        return remote(others, others, sp_sem.at[o], rp_sem.at[o], ORDERS[o][0], 1)

    def relay_slab(g, q, a, b):
        return relay[g].at[q, b, a] if g % 3 == 1 else relay[g].at[q, a, b]

    def out_second(g, q, a, b):
        return remote(packed[g].at[q, b, a], relay_slab(g, q, a, b), s1_sem.at[g, q], r1_sem.at[g, q], orders[g][1], b)

    def out_second_all(g, q):
        return remote(packed[g].at[q, pl.ds(1, side - 1)], relay_others(g, q), s1_sem.at[g, q], r1_sem.at[g, q], orders[g][1], 1)

    def out_third(g, q, e):
        return remote(relay[g].at[q, :, :, e], rows.at[rows_at(g, q, e)], s2_sem.at[g, q], r2_sem.at[g, q], orders[g][2], e // 2, e % 2)

    def third_all(g, q, s_sem, r_sem):
        some = relay[g].at[q, :, :, pl.ds(1, ends - 1)]
        return remote(some, some, s_sem.at[g, q], r_sem.at[g, q], orders[g][2], 1)

    def home_third(g, q, e):
        return remote(rows.at[rows_at(g, q, e)], relay[g].at[q, :, :, e], b1_sem.at[g, q], c1_sem.at[g, q], orders[g][2], -(e // 2), e % 2)

    def home_second(g, q, b):
        return remote(relay_from(g, q, b), packed[g].at[q, b], b2_sem.at[g, q], c2_sem.at[g, q], orders[g][1], -b)

    def home_second_all(g, q):
        return remote(relay_others(g, q), packed[g].at[q, pl.ds(1, side - 1)], b2_sem.at[g, q], c2_sem.at[g, q], orders[g][1], 1)

    def home_mid(g, d):
        return remote(parts.at[2, half(d), columns(g)], mids.at[d, :, columns(g)],
                      s3_sem.at[g, d], r3_sem.at[g, d], orders[g][0], -near[d])

    def home_near(g, d, i):
        part = half(1 - d if i == 0 else d)
        return remote(parts.at[near[d], part, columns(g)], y_peers.at[d, part, columns(g)],
                      s3_sem.at[g, 2 + 2 * d + i], r3_sem.at[g, 2 + 2 * d + i], orders[g][0], -near[d])

    def tell(sem, axis, steps, core_steps=0):
        pl.semaphore_signal(sem, inc=1, device_id=(dp, moved(me, side, axis, steps, core_steps)), device_id_type=MESH)

    loads = [pltpu.make_async_copy(tokens_hbm.at[:, columns(g)], toks[g].at[0], load_sem.at[g]) for g in range(count)]
    loads.append(pltpu.make_async_copy(w_router_hbm, w_router, load_sem.at[count]))
    weights = [pltpu.make_async_copy(src, dst, w_sem.at[i]) for i, (src, dst) in enumerate(
        [(w_one_hbm, w_one), (w_three_hbm, w_three), (w_two_hbm, w_two)])]
    for copy in loads:
        copy.start()

    barrier = pltpu.get_barrier_semaphore()
    tell(barrier, X, 0, 1)
    for axis in (Z, Y, X):
        for steps in range(1, side):
            for core_steps in range(2):
                tell(barrier, axis, steps, core_steps)
    with jax.named_scope('barrier'):
        pl.semaphore_wait(barrier, 1 + 3 * (side - 1) * 2)

    for i in range(2):
        for g in range(count):
            for d in range(len(near)):
                gather_near(g, d, i).start()
    with jax.named_scope('own_wait'):
        for copy in loads:
            copy.wait()

    num_experts = 2 * side ** 3
    logits = sum(jnp.dot(toks[g][0], w_router[columns(g), :], preferred_element_type=jnp.float32) for g in range(count)).T
    ids = lax.broadcasted_iota(jnp.int32, (num_experts, num_tokens), 0)
    picks = [routes_ref[k:k + 1, :] for k in range(top_k)]
    scores = [jnp.sum(jnp.where(pick == ids, logits, 0.0), axis=0, keepdims=True) for pick in picks]
    peak = functools.reduce(jnp.maximum, scores)
    scores = [jnp.exp(score - peak) for score in scores]
    norm = sum(scores)
    for k in range(top_k):
        own_info[k:k + 1, :] = picks[k].astype(jnp.float32)
        own_info[top_k + k:top_k + k + 1, :] = scores[k] / norm
    for o in range(3):
        for a in range(1, side):
            gather_info(o, a).start()
    before = (lax.broadcasted_iota(jnp.int32, (num_tokens, num_tokens), 0)
              < lax.broadcasted_iota(jnp.int32, (num_tokens, num_tokens), 1))
    before = jnp.where(before, 1.0, 0.0).astype(jnp.bfloat16)
    expert_at = [plane_experts(me, side, order, num_tokens).astype(jnp.float32) for order in ORDERS]

    def make_plan(o, a, info):
        mask = jnp.zeros((plane, num_tokens), jnp.float32)
        gate = jnp.zeros((plane, num_tokens), jnp.float32)
        for k in range(top_k):
            hit = info[k:k + 1] == expert_at[o]
            mask = jnp.where(hit, 1.0, mask)
            gate = jnp.where(hit, info[top_k + k:top_k + k + 1], gate)
        slot = jnp.dot(mask.astype(jnp.bfloat16), before, preferred_element_type=jnp.float32)
        plans[o][a, pl.ds(0, plane), :] = jnp.where(mask > 0.0, slot, -1.0)
        plans[o][a, pl.ds(plane, plane), :] = gate

    for o in range(3):
        make_plan(o, 0, own_info[...])
    for copy in weights:
        copy.start()

    def taken(g, q, a):
        slots = plans[g % 3][a, pl.ds(0, plane), :]
        ids = lax.broadcasted_iota(jnp.int32, (plane, SLOTS, num_tokens), 1) + q * SLOTS
        return jnp.broadcast_to(slots[:, None, :], (plane, SLOTS, num_tokens)) == ids.astype(jnp.float32)

    def pack(g, q, a):
        select = jnp.where(taken(g, q, a), 1.0, 0.0).reshape(packed_rows, num_tokens).astype(jnp.bfloat16)
        out = jnp.dot(select, toks[g][a], preferred_element_type=jnp.float32)
        out = out.reshape(side, ends, SLOTS, groups[g][1]).astype(jnp.bfloat16)
        packed[g][q, pl.ds(1, side - 1), a] = out[1:]
        each(1, side, lambda b: out_second(g, q, a, b).start())
        relay_slab(g, q, a, 0)[...] = out[0]

    def pack_own(q, carry):
        for g in range(count):
            pack(g, q, 0)
        return carry

    if far:
        with jax.named_scope('gather_far'):
            for g in range(count):
                for d in range(2):
                    gather_near(g, d, 0).wait_recv()
                    gather_far(g, d).start()
    with jax.named_scope('pack_own'):
        lax.fori_loop(0, chunks, pack_own, 0)
    parts[...] = jnp.zeros_like(parts)
    with jax.named_scope('gather_wait'):
        for o in range(3):
            gather_info_all(o).wait_recv()
            for a in range(1, side):
                make_plan(o, a, infos[o, a])
        for g in range(count):
            for d in range(len(near)):
                if not far:
                    gather_near(g, d, 0).wait_recv()
                gather_near(g, d, 1).wait_recv()
            if far:
                gather_far(g, 0).wait_recv()
                gather_far(g, 1).wait_recv()

    def outward(i, carry):
        @pl.when(i < chunks)
        def _():
            for g in range(count):
                def source(a, c):
                    pack(g, i, a)
                    return c
                with jax.named_scope('pack'):
                    lax.fori_loop(1, side, source, 0)

        @pl.when(i > 0)
        def _():
            forward(i - 1)
        return carry

    def forward(q):
        for g in range(count):
            with jax.named_scope('s1_wait'):
                out_second_all(g, q).wait_recv()
            each(1, ends, lambda e: out_third(g, q, e).start())
            rows[rows_at(g, q, 0)] = relay[g][q, :, :, 0]
            with jax.named_scope('s1_send_wait'):
                out_second_all(g, q).wait_send()
            each(1, side, lambda b: tell(free2_sem.at[g, q], orders[g][1], b))

    lax.fori_loop(0, chunks + 1, outward, 0)
    for copy in weights:
        copy.wait()

    def experts(q, carry):
        with jax.named_scope('s2_wait'):
            for g in range(count):
                third_all(g, q, s2_sem, r2_sem).wait_recv()
        for g in range(count):
            with jax.named_scope('s2_send_wait'):
                third_all(g, q, s2_sem, r2_sem).wait_send()
            each(1, ends, lambda e: tell(free3_sem.at[g, q], orders[g][2], e // 2, e % 2))

        def block(z, c):
            shape = rows.shape[2:]
            u = rows[q, z].astype(jnp.float32).reshape(packed_rows, shape[-1]).astype(jnp.bfloat16)
            gate_pre = jnp.dot(u, w_one[...], preferred_element_type=jnp.float32)
            up_pre = jnp.dot(u, w_three[...], preferred_element_type=jnp.float32)
            hidden = (jax.nn.silu(gate_pre) * up_pre).astype(jnp.bfloat16)
            out = jnp.dot(hidden, w_two[...], preferred_element_type=jnp.float32)
            rows[q, z] = out.reshape(shape).astype(jnp.bfloat16)
            return c
        with jax.named_scope('mlp'):
            lax.fori_loop(0, side, block, 0)
        for g in range(count):
            with jax.named_scope('free3'):
                pl.semaphore_wait(free3_sem.at[g, q], ends - 1)
            each(1, ends, lambda e: home_third(g, q, e).start())
            relay[g][q, :, :, 0] = rows[rows_at(g, q, 0)]
        return carry

    lax.fori_loop(0, chunks, experts, 0)

    def backward(q):
        for g in range(count):
            with jax.named_scope('r1_wait'):
                third_all(g, q, b1_sem, c1_sem).wait_recv()
            pl.semaphore_wait(free2_sem.at[g, q], side - 1)
            each(1, side, lambda b: home_second(g, q, b).start())
            packed[g][q, 0] = relay_from(g, q, 0)[...]

    def combine(q):
        for g in arrival:
            with jax.named_scope('r2_wait'):
                home_second_all(g, q).wait_recv()
            width = groups[g][1]

            def source(i, c):
                a = (i + side // 2) % side
                gates = plans[g % 3][a, pl.ds(plane, plane), :]
                used = taken(g, q, a)
                o = packed[g][q, :, a].astype(jnp.float32).reshape(packed_rows, width).astype(jnp.bfloat16)
                total = None
                for _ in range(3):
                    part = gates.astype(jnp.bfloat16).astype(jnp.float32)
                    gates = gates - part
                    mix = jnp.where(used, jnp.broadcast_to(part[:, None, :], used.shape), 0.0).reshape(packed_rows, num_tokens).astype(jnp.bfloat16)
                    term = lax.dot_general(mix, o, (((0,), (0,)), ((), ())), preferred_element_type=jnp.float32)
                    total = term if total is None else total + term
                parts[a, :, columns(g)] += total

                last = q == chunks - 1
                if far:
                    @pl.when(jnp.logical_and(last, a == 2))
                    def _():
                        home_mid(g, 0).start()
                        home_mid(g, 1).start()
                for d in range(len(near)):
                    @pl.when(jnp.logical_and(last, a == near[d]))
                    def _():
                        home_near(g, d, 0).start()
                return c
            with jax.named_scope('combine'):
                lax.fori_loop(0, side, source, 0)

    def send_home(q, carry):
        backward(q)
        return carry

    def sum_up(q, carry):
        combine(q)
        return carry

    lax.fori_loop(0, chunks, send_home, 0)
    lax.fori_loop(0, chunks, sum_up, 0)
    own = pltpu.make_async_copy(parts.at[0], y_own, out_sem)
    own.start()
    for g in arrival:
        for d in range(len(near)):
            if far:
                with jax.named_scope('mid_wait'):
                    home_mid(g, d).wait_recv()
                parts[near[d], half(d), columns(g)] += mids[d, :, columns(g)]
            home_near(g, d, 1).start()

    for g in range(count):
        def drain(q, c):
            third_all(g, q, b1_sem, c1_sem).wait_send()
            home_second_all(g, q).wait_send()
            return c
        lax.fori_loop(0, chunks, drain, 0)
        for d in range(len(near)):
            gather_near(g, d, 0).wait_send()
            gather_near(g, d, 1).wait_send()
            if far:
                gather_far(g, d).wait_send()
                home_mid(g, d).wait_send()
    for o in range(3):
        gather_info_all(o).wait_send()
    for g in arrival:
        for d in range(len(near)):
            for i in range(2):
                with jax.named_scope('r3_wait'):
                    home_near(g, d, i).wait_recv()
                    home_near(g, d, i).wait_send()
    own.wait()


def sum_kernel(own_ref, peers_ref, y_ref):
    total = own_ref[...]
    for i in range(peers_ref.shape[0]):
        total = total + peers_ref[i]
    y_ref[...] = total.astype(y_ref.dtype)


def solution(mesh):
    group_size = mesh.shape['ep']
    side = torus_side(group_size)
    row_spec = P(('dp', 'ep'), None)
    expert_spec = P('ep', None, None)

    def device_step(tokens, routes, w_router, w_one, w_three, w_two):
        num_tokens, d_model = tokens.shape
        top_k = routes.shape[1]
        num_experts = w_router.shape[1]
        d_expert = w_one.shape[2]
        capacity = slot_capacity(num_tokens, top_k, num_experts)
        chunks = capacity // SLOTS
        groups = column_groups(d_model)
        count = len(groups)
        plane = 2 * side * side
        hbm = pl.BlockSpec(memory_space=pl.ANY)
        vmem = pl.BlockSpec(memory_space=pltpu.VMEM)
        dma = pltpu.SemaphoreType.DMA
        slab = [[pltpu.VMEM((chunks, side, side, 2 * side, SLOTS, width), jnp.bfloat16) for _, width in groups] for _ in range(2)]
        pair = [dma((count, chunks)), dma((count, chunks))]
        y_own, y_peers = pl.pallas_call(
            functools.partial(moe_kernel, side, chunks, groups),
            out_shape=(jax.ShapeDtypeStruct((num_tokens, d_model), jnp.float32),
                       jax.ShapeDtypeStruct((2 if side > 2 else 1, num_tokens, d_model), jnp.float32)),
            in_specs=[hbm, vmem, hbm, hbm, hbm, hbm],
            out_specs=(hbm, hbm),
            scratch_shapes=[
                [pltpu.VMEM((side, num_tokens, width), jnp.bfloat16) for _, width in groups],
                pltpu.VMEM((3, side, 2 * top_k, num_tokens), jnp.float32),
                pltpu.VMEM((2 * top_k, num_tokens), jnp.float32),
                [pltpu.VMEM((side, 2 * plane, num_tokens), jnp.float32) for _ in ORDERS],
                slab[0], slab[1],
                pltpu.VMEM((chunks, side, side, side, 2, SLOTS, d_model), jnp.bfloat16),
                pltpu.VMEM((d_model, num_experts), jnp.bfloat16),
                pltpu.VMEM((d_model, d_expert), jnp.bfloat16),
                pltpu.VMEM((d_model, d_expert), jnp.bfloat16),
                pltpu.VMEM((d_expert, d_model), jnp.bfloat16),
                pltpu.VMEM((side, num_tokens, d_model), jnp.float32),
                pltpu.VMEM((2, num_tokens // 2, d_model), jnp.float32),
                dma((count + 1,)), dma((3,)), dma((count, 6)), dma((count, 6)), dma((3,)), dma((3,)),
                *pair, *pair, *pair, *pair, dma((count, 6)), dma((count, 6)), dma,
                pltpu.SemaphoreType.REGULAR((count, chunks)), pltpu.SemaphoreType.REGULAR((count, chunks)),
            ],
            compiler_params=pltpu.CompilerParams(collective_id=0, has_side_effects=True, vmem_limit_bytes=67043328),
            name='moe',
        )(tokens, routes.T, w_router, w_one[0], w_three[0], w_two[0])
        peers = y_peers.shape[0]
        block = num_tokens // 8
        return pl.pallas_call(
            sum_kernel,
            grid=(8,),
            out_shape=jax.ShapeDtypeStruct((num_tokens, d_model), jnp.bfloat16),
            in_specs=[pl.BlockSpec((block, d_model), lambda i: (i, 0)), pl.BlockSpec((peers, block, d_model), lambda i: (0, i, 0))],
            out_specs=pl.BlockSpec((block, d_model), lambda i: (i, 0)),
            name='final_sum',
        )(y_own, y_peers)

    return jax.shard_map(device_step, mesh=mesh, in_specs=(row_spec, row_spec, P(None, None), expert_spec, expert_spec, expert_spec), out_specs=row_spec, check_vma=False)
```

```python
import functools

import jax
import jax.numpy as jnp
from jax import lax
from jax.experimental import pallas as pl
from jax.experimental.pallas import tpu as pltpu
from jax.sharding import PartitionSpec as P

MESH = pl.DeviceIdType.MESH
Z, Y, X = 0, 1, 2
ORDERS = ((Z, Y, X), (X, Z, Y), (Y, X, Z))
SLOTS = 8


def slot_capacity(num_tokens, top_k, num_experts):
    return 8 * ((3 * num_tokens * top_k + 16 * num_experts - 1) // (16 * num_experts))


def torus_side(group_size):
    side = 1
    while 2 * side ** 3 < group_size:
        side += 1
    return side


def column_groups(d_model):
    lanes = d_model // 128
    count = 6 if lanes >= 6 else 3
    widths = [128 * (lanes // count + (1 if i < lanes % count else 0)) for i in range(count)]
    starts = [sum(widths[:i]) for i in range(count)]
    return list(zip(starts, widths))


def moved(me, side, axis, steps, core_steps=0):
    digits = [me // (2 * side * side), (me // (2 * side)) % side, (me // 2) % side]
    digits[axis] = (digits[axis] + steps + side) % side
    return ((digits[Z] * side + digits[Y]) * side + digits[X]) * 2 + (me + core_steps) % 2


def plane_experts(me, side, order, num_tokens):
    bits = side.bit_length() - 1
    position = lax.broadcasted_iota(jnp.int32, (2 * side * side, num_tokens), 0)
    digits = [me // (2 * side * side), (me // (2 * side)) % side, (me // 2) % side]
    for place, axis in enumerate(order[1:]):
        steps = jnp.right_shift(position, 1 + (1 - place) * bits)
        digits[axis] = jnp.bitwise_and(digits[axis] + steps, side - 1)
    core = jnp.bitwise_and(me + position, 1)
    return ((digits[Z] * side + digits[Y]) * side + digits[X]) * 2 + core


def each(first, end, act):
    def step(i, carry):
        act(i)
        return carry
    lax.fori_loop(first, end, step, 0)


def moe_kernel(side, chunks, groups, tokens_hbm, routes_ref, w_router_hbm, w_one_hbm, w_three_hbm, w_two_hbm, y_own, y_peers,
               toks, infos, own_info, plans, packed, relay, rows, w_router, w_one, w_three, w_two, parts, mids,
               load_sem, w_sem, s0_sem, r0_sem, sp_sem, rp_sem, s1_sem, r1_sem, s2_sem, r2_sem, b1_sem, c1_sem, b2_sem, c2_sem, s3_sem, r3_sem, out_sem, free2_sem, free3_sem):
    me = lax.axis_index('ep')
    dp = lax.axis_index('dp')
    num_tokens = tokens_hbm.shape[0]
    plane = 2 * side * side
    ends = 2 * side
    count = len(groups)
    arrival = (0, 1, 4, 2, 3, 5) if count == 6 else (1, 0, 2)
    near = (1, side - 1) if side > 2 else (1,)
    far = side > 2
    packed_rows = plane * SLOTS
    top_k = routes_ref.shape[0]
    orders = [ORDERS[g % 3] for g in range(count)]

    def remote(src, dst, s_sem, r_sem, axis, steps, core_steps=0):
        return pltpu.make_async_remote_copy(
            src_ref=src, dst_ref=dst, send_sem=s_sem, recv_sem=r_sem,
            device_id=(dp, moved(me, side, axis, steps, core_steps)), device_id_type=MESH)

    def columns(g):
        return pl.ds(*groups[g])

    def relay_from(g, q, b):
        return relay[g].at[q, b] if g % 3 == 1 else relay[g].at[q, :, b]

    def relay_others(g, q):
        return relay[g].at[q, pl.ds(1, side - 1)] if g % 3 == 1 else relay[g].at[q, :, pl.ds(1, side - 1)]

    def rows_at(g, q, e):
        c, core = e // 2, e % 2
        third = orders[g][2]
        where = {Z: (q, c, slice(None), slice(None), core), Y: (q, slice(None), c, slice(None), core),
                 X: (q, slice(None), slice(None), c, core)}[third]
        return where + (slice(None), columns(g))

    def half(i):
        return pl.ds(i * (num_tokens // 2), num_tokens // 2)

    def gather_near(g, d, i):
        part = half(i if d == 0 else 1 - i)
        return remote(tokens_hbm.at[part, columns(g)], toks[g].at[near[d], part],
                      s0_sem.at[g, 2 * d + i], r0_sem.at[g, 2 * d + i], orders[g][0], near[d])

    def gather_far(g, d):
        return remote(toks[g].at[near[d], half(d)], toks[g].at[2, half(d)],
                      s0_sem.at[g, 4 + d], r0_sem.at[g, 4 + d], orders[g][0], near[d])

    def gather_info(o, a):
        return remote(own_info, infos.at[o, a], sp_sem.at[o], rp_sem.at[o], ORDERS[o][0], a)

    def gather_info_all(o):
        others = infos.at[o, pl.ds(1, side - 1)]
        return remote(others, others, sp_sem.at[o], rp_sem.at[o], ORDERS[o][0], 1)

    def relay_slab(g, q, a, b):
        return relay[g].at[q, b, a] if g % 3 == 1 else relay[g].at[q, a, b]

    def out_second(g, q, a, b):
        return remote(packed[g].at[q, b, a], relay_slab(g, q, a, b), s1_sem.at[g, q], r1_sem.at[g, q], orders[g][1], b)

    def out_second_all(g, q):
        return remote(packed[g].at[q, pl.ds(1, side - 1)], relay_others(g, q), s1_sem.at[g, q], r1_sem.at[g, q], orders[g][1], 1)

    def out_third(g, q, e):
        return remote(relay[g].at[q, :, :, e], rows.at[rows_at(g, q, e)], s2_sem.at[g, q], r2_sem.at[g, q], orders[g][2], e // 2, e % 2)

    def third_all(g, q, s_sem, r_sem):
        some = relay[g].at[q, :, :, pl.ds(1, ends - 1)]
        return remote(some, some, s_sem.at[g, q], r_sem.at[g, q], orders[g][2], 1)

    def home_third(g, q, e):
        return remote(rows.at[rows_at(g, q, e)], relay[g].at[q, :, :, e], b1_sem.at[g, q], c1_sem.at[g, q], orders[g][2], -(e // 2), e % 2)

    def home_second(g, q, b):
        return remote(relay_from(g, q, b), packed[g].at[q, b], b2_sem.at[g, q], c2_sem.at[g, q], orders[g][1], -b)

    def home_second_all(g, q):
        return remote(relay_others(g, q), packed[g].at[q, pl.ds(1, side - 1)], b2_sem.at[g, q], c2_sem.at[g, q], orders[g][1], 1)

    def home_mid(g, d):
        return remote(parts.at[2, half(d), columns(g)], mids.at[d, :, columns(g)],
                      s3_sem.at[g, d], r3_sem.at[g, d], orders[g][0], -near[d])

    def home_near(g, d, i):
        part = half(1 - d if i == 0 else d)
        return remote(parts.at[near[d], part, columns(g)], y_peers.at[d, part, columns(g)],
                      s3_sem.at[g, 2 + 2 * d + i], r3_sem.at[g, 2 + 2 * d + i], orders[g][0], -near[d])

    def tell(sem, axis, steps, core_steps=0):
        pl.semaphore_signal(sem, inc=1, device_id=(dp, moved(me, side, axis, steps, core_steps)), device_id_type=MESH)

    loads = [pltpu.make_async_copy(tokens_hbm.at[:, columns(g)], toks[g].at[0], load_sem.at[g]) for g in range(count)]
    loads.append(pltpu.make_async_copy(w_router_hbm, w_router, load_sem.at[count]))
    weights = [pltpu.make_async_copy(src, dst, w_sem.at[i]) for i, (src, dst) in enumerate(
        [(w_one_hbm, w_one), (w_three_hbm, w_three), (w_two_hbm, w_two)])]
    for copy in loads:
        copy.start()

    barrier = pltpu.get_barrier_semaphore()
    tell(barrier, X, 0, 1)
    for axis in (Z, Y, X):
        for steps in range(1, side):
            for core_steps in range(2):
                tell(barrier, axis, steps, core_steps)
    with jax.named_scope('barrier'):
        pl.semaphore_wait(barrier, 1 + 3 * (side - 1) * 2)

    for i in range(2):
        for g in range(count):
            for d in range(len(near)):
                gather_near(g, d, i).start()
    with jax.named_scope('own_wait'):
        for copy in loads:
            copy.wait()

    num_experts = 2 * side ** 3
    logits = sum(jnp.dot(toks[g][0], w_router[columns(g), :], preferred_element_type=jnp.float32) for g in range(count)).T
    ids = lax.broadcasted_iota(jnp.int32, (num_experts, num_tokens), 0)
    picks = [routes_ref[k:k + 1, :] for k in range(top_k)]
    scores = [jnp.sum(jnp.where(pick == ids, logits, 0.0), axis=0, keepdims=True) for pick in picks]
    peak = functools.reduce(jnp.maximum, scores)
    scores = [jnp.exp(score - peak) for score in scores]
    norm = sum(scores)
    for k in range(top_k):
        own_info[k:k + 1, :] = picks[k].astype(jnp.float32)
        own_info[top_k + k:top_k + k + 1, :] = scores[k] / norm
    for o in range(3):
        for a in range(1, side):
            gather_info(o, a).start()
    before = (lax.broadcasted_iota(jnp.int32, (num_tokens, num_tokens), 0)
              < lax.broadcasted_iota(jnp.int32, (num_tokens, num_tokens), 1))
    before = jnp.where(before, 1.0, 0.0).astype(jnp.bfloat16)
    expert_at = [plane_experts(me, side, order, num_tokens).astype(jnp.float32) for order in ORDERS]

    def make_plan(o, a, info):
        mask = jnp.zeros((plane, num_tokens), jnp.float32)
        gate = jnp.zeros((plane, num_tokens), jnp.float32)
        for k in range(top_k):
            hit = info[k:k + 1] == expert_at[o]
            mask = jnp.where(hit, 1.0, mask)
            gate = jnp.where(hit, info[top_k + k:top_k + k + 1], gate)
        slot = jnp.dot(mask.astype(jnp.bfloat16), before, preferred_element_type=jnp.float32)
        plans[o][a, pl.ds(0, plane), :] = jnp.where(mask > 0.0, slot, -1.0)
        plans[o][a, pl.ds(plane, plane), :] = gate

    for o in range(3):
        make_plan(o, 0, own_info[...])
    for copy in weights:
        copy.start()

    def taken(g, q, a):
        slots = plans[g % 3][a, pl.ds(0, plane), :]
        ids = lax.broadcasted_iota(jnp.int32, (plane, SLOTS, num_tokens), 1) + q * SLOTS
        return jnp.broadcast_to(slots[:, None, :], (plane, SLOTS, num_tokens)) == ids.astype(jnp.float32)

    def pack(g, q, a):
        select = jnp.where(taken(g, q, a), 1.0, 0.0).reshape(packed_rows, num_tokens).astype(jnp.bfloat16)
        out = jnp.dot(select, toks[g][a], preferred_element_type=jnp.float32)
        out = out.reshape(side, ends, SLOTS, groups[g][1]).astype(jnp.bfloat16)
        packed[g][q, pl.ds(1, side - 1), a] = out[1:]
        each(1, side, lambda b: out_second(g, q, a, b).start())
        relay_slab(g, q, a, 0)[...] = out[0]

    def pack_own(q, carry):
        for g in range(count):
            pack(g, q, 0)
        return carry

    if far:
        with jax.named_scope('gather_far'):
            for g in range(count):
                for d in range(2):
                    gather_near(g, d, 0).wait_recv()
                    gather_far(g, d).start()
    with jax.named_scope('pack_own'):
        lax.fori_loop(0, chunks, pack_own, 0)
    parts[...] = jnp.zeros_like(parts)
    with jax.named_scope('gather_wait'):
        for o in range(3):
            gather_info_all(o).wait_recv()
            for a in range(1, side):
                make_plan(o, a, infos[o, a])
        for g in range(count):
            for d in range(len(near)):
                if not far:
                    gather_near(g, d, 0).wait_recv()
                gather_near(g, d, 1).wait_recv()
            if far:
                gather_far(g, 0).wait_recv()
                gather_far(g, 1).wait_recv()

    def outward(i, carry):
        @pl.when(i < chunks)
        def _():
            for g in range(count):
                def source(a, c):
                    pack(g, i, a)
                    return c
                with jax.named_scope('pack'):
                    lax.fori_loop(1, side, source, 0)

        @pl.when(i > 0)
        def _():
            forward(i - 1)
        return carry

    def forward(q):
        for g in range(count):
            with jax.named_scope('s1_wait'):
                out_second_all(g, q).wait_recv()
            each(1, ends, lambda e: out_third(g, q, e).start())
            rows[rows_at(g, q, 0)] = relay[g][q, :, :, 0]
            with jax.named_scope('s1_send_wait'):
                out_second_all(g, q).wait_send()
            each(1, side, lambda b: tell(free2_sem.at[g, q], orders[g][1], b))

    lax.fori_loop(0, chunks + 1, outward, 0)
    for copy in weights:
        copy.wait()

    def experts(q, carry):
        with jax.named_scope('s2_wait'):
            for g in range(count):
                third_all(g, q, s2_sem, r2_sem).wait_recv()
        for g in range(count):
            with jax.named_scope('s2_send_wait'):
                third_all(g, q, s2_sem, r2_sem).wait_send()
            each(1, ends, lambda e: tell(free3_sem.at[g, q], orders[g][2], e // 2, e % 2))

        def block(z, c):
            shape = rows.shape[2:]
            u = rows[q, z].astype(jnp.float32).reshape(packed_rows, shape[-1]).astype(jnp.bfloat16)
            gate_pre = jnp.dot(u, w_one[...], preferred_element_type=jnp.float32)
            up_pre = jnp.dot(u, w_three[...], preferred_element_type=jnp.float32)
            hidden = (jax.nn.silu(gate_pre) * up_pre).astype(jnp.bfloat16)
            out = jnp.dot(hidden, w_two[...], preferred_element_type=jnp.float32)
            rows[q, z] = out.reshape(shape).astype(jnp.bfloat16)
            return c
        with jax.named_scope('mlp'):
            lax.fori_loop(0, side, block, 0)
        for g in range(count):
            with jax.named_scope('free3'):
                pl.semaphore_wait(free3_sem.at[g, q], ends - 1)
            each(1, ends, lambda e: home_third(g, q, e).start())
            relay[g][q, :, :, 0] = rows[rows_at(g, q, 0)]
        return carry

    lax.fori_loop(0, chunks, experts, 0)

    def backward(q):
        for g in range(count):
            with jax.named_scope('r1_wait'):
                third_all(g, q, b1_sem, c1_sem).wait_recv()
            pl.semaphore_wait(free2_sem.at[g, q], side - 1)
            each(1, side, lambda b: home_second(g, q, b).start())
            packed[g][q, 0] = relay_from(g, q, 0)[...]

    def combine(q):
        for g in arrival:
            with jax.named_scope('r2_wait'):
                home_second_all(g, q).wait_recv()
            width = groups[g][1]

            def source(i, c):
                a = (i + side // 2) % side
                gates = plans[g % 3][a, pl.ds(plane, plane), :]
                used = taken(g, q, a)
                o = packed[g][q, :, a].astype(jnp.float32).reshape(packed_rows, width).astype(jnp.bfloat16)
                total = None
                for _ in range(3):
                    part = gates.astype(jnp.bfloat16).astype(jnp.float32)
                    gates = gates - part
                    mix = jnp.where(used, jnp.broadcast_to(part[:, None, :], used.shape), 0.0).reshape(packed_rows, num_tokens).astype(jnp.bfloat16)
                    term = lax.dot_general(mix, o, (((0,), (0,)), ((), ())), preferred_element_type=jnp.float32)
                    total = term if total is None else total + term
                parts[a, :, columns(g)] += total

                last = q == chunks - 1
                if far:
                    @pl.when(jnp.logical_and(last, a == 2))
                    def _():
                        home_mid(g, 0).start()
                        home_mid(g, 1).start()
                for d in range(len(near)):
                    @pl.when(jnp.logical_and(last, a == near[d]))
                    def _():
                        home_near(g, d, 0).start()
                return c
            with jax.named_scope('combine'):
                lax.fori_loop(0, side, source, 0)

    def send_home(q, carry):
        backward(q)
        return carry

    def sum_up(q, carry):
        combine(q)
        return carry

    lax.fori_loop(0, chunks, send_home, 0)
    lax.fori_loop(0, chunks, sum_up, 0)
    own = pltpu.make_async_copy(parts.at[0], y_own, out_sem)
    own.start()
    for g in arrival:
        for d in range(len(near)):
            if far:
                with jax.named_scope('mid_wait'):
                    home_mid(g, d).wait_recv()
                parts[near[d], half(d), columns(g)] += mids[d, :, columns(g)]
            home_near(g, d, 1).start()

    for g in range(count):
        def drain(q, c):
            third_all(g, q, b1_sem, c1_sem).wait_send()
            home_second_all(g, q).wait_send()
            return c
        lax.fori_loop(0, chunks, drain, 0)
        for d in range(len(near)):
            gather_near(g, d, 0).wait_send()
            gather_near(g, d, 1).wait_send()
            if far:
                gather_far(g, d).wait_send()
                home_mid(g, d).wait_send()
    for o in range(3):
        gather_info_all(o).wait_send()
    for g in arrival:
        for d in range(len(near)):
            for i in range(2):
                with jax.named_scope('r3_wait'):
                    home_near(g, d, i).wait_recv()
                    home_near(g, d, i).wait_send()
    own.wait()


def solution(mesh):
    group_size = mesh.shape['ep']
    side = torus_side(group_size)
    row_spec = P(('dp', 'ep'), None)
    expert_spec = P('ep', None, None)

    def device_step(tokens, routes, w_router, w_one, w_three, w_two):
        num_tokens, d_model = tokens.shape
        top_k = routes.shape[1]
        num_experts = w_router.shape[1]
        d_expert = w_one.shape[2]
        capacity = slot_capacity(num_tokens, top_k, num_experts)
        chunks = capacity // SLOTS
        groups = column_groups(d_model)
        count = len(groups)
        plane = 2 * side * side
        hbm = pl.BlockSpec(memory_space=pl.ANY)
        vmem = pl.BlockSpec(memory_space=pltpu.VMEM)
        dma = pltpu.SemaphoreType.DMA
        slab = [[pltpu.VMEM((chunks, side, side, 2 * side, SLOTS, width), jnp.bfloat16) for _, width in groups] for _ in range(2)]
        pair = [dma((count, chunks)), dma((count, chunks))]
        y_own, y_peers = pl.pallas_call(
            functools.partial(moe_kernel, side, chunks, groups),
            out_shape=(jax.ShapeDtypeStruct((num_tokens, d_model), jnp.float32),
                       jax.ShapeDtypeStruct((2 if side > 2 else 1, num_tokens, d_model), jnp.float32)),
            in_specs=[hbm, vmem, hbm, hbm, hbm, hbm],
            out_specs=(hbm, hbm),
            scratch_shapes=[
                [pltpu.VMEM((side, num_tokens, width), jnp.bfloat16) for _, width in groups],
                pltpu.VMEM((3, side, 2 * top_k, num_tokens), jnp.float32),
                pltpu.VMEM((2 * top_k, num_tokens), jnp.float32),
                [pltpu.VMEM((side, 2 * plane, num_tokens), jnp.float32) for _ in ORDERS],
                slab[0], slab[1],
                pltpu.VMEM((chunks, side, side, side, 2, SLOTS, d_model), jnp.bfloat16),
                pltpu.VMEM((d_model, num_experts), jnp.bfloat16),
                pltpu.VMEM((d_model, d_expert), jnp.bfloat16),
                pltpu.VMEM((d_model, d_expert), jnp.bfloat16),
                pltpu.VMEM((d_expert, d_model), jnp.bfloat16),
                pltpu.VMEM((side, num_tokens, d_model), jnp.float32),
                pltpu.VMEM((2, num_tokens // 2, d_model), jnp.float32),
                dma((count + 1,)), dma((3,)), dma((count, 6)), dma((count, 6)), dma((3,)), dma((3,)),
                *pair, *pair, *pair, *pair, dma((count, 6)), dma((count, 6)), dma,
                pltpu.SemaphoreType.REGULAR((count, chunks)), pltpu.SemaphoreType.REGULAR((count, chunks)),
            ],
            compiler_params=pltpu.CompilerParams(collective_id=0, has_side_effects=True, vmem_limit_bytes=67043328),
            name='moe',
        )(tokens, routes.T, w_router, w_one[0], w_three[0], w_two[0])
        total = y_own
        for i in range(y_peers.shape[0]):
            total = total + y_peers[i]
        return total.astype(jnp.bfloat16)

    return jax.shard_map(device_step, mesh=mesh, in_specs=(row_spec, row_spec, P(None, None), expert_spec, expert_spec, expert_spec), out_specs=row_spec, check_vma=False)
```

```python
import functools

import jax
import jax.numpy as jnp
from jax import lax
from jax.experimental import pallas as pl
from jax.experimental.pallas import tpu as pltpu
from jax.sharding import PartitionSpec as P

MESH = pl.DeviceIdType.MESH
Z, Y, X = 0, 1, 2
ORDERS = ((Z, Y, X), (X, Z, Y), (Y, X, Z))
SLOTS = 8


def slot_capacity(num_tokens, top_k, num_experts):
    return 8 * ((3 * num_tokens * top_k + 16 * num_experts - 1) // (16 * num_experts))


def torus_side(group_size):
    side = 1
    while 2 * side ** 3 < group_size:
        side += 1
    return side


def column_groups(d_model):
    lanes = d_model // 128
    count = 6 if lanes >= 6 else 3
    widths = [128 * (lanes // count + (1 if i < lanes % count else 0)) for i in range(count)]
    starts = [sum(widths[:i]) for i in range(count)]
    return list(zip(starts, widths))


def moved(me, side, axis, steps, core_steps=0):
    digits = [me // (2 * side * side), (me // (2 * side)) % side, (me // 2) % side]
    digits[axis] = (digits[axis] + steps + side) % side
    return ((digits[Z] * side + digits[Y]) * side + digits[X]) * 2 + (me + core_steps) % 2


def plane_experts(me, side, order, num_tokens):
    bits = side.bit_length() - 1
    position = lax.broadcasted_iota(jnp.int32, (2 * side * side, num_tokens), 0)
    digits = [me // (2 * side * side), (me // (2 * side)) % side, (me // 2) % side]
    for place, axis in enumerate(order[1:]):
        steps = jnp.right_shift(position, 1 + (1 - place) * bits)
        digits[axis] = jnp.bitwise_and(digits[axis] + steps, side - 1)
    core = jnp.bitwise_and(me + position, 1)
    return ((digits[Z] * side + digits[Y]) * side + digits[X]) * 2 + core


def each(first, end, act):
    def step(i, carry):
        act(i)
        return carry
    lax.fori_loop(first, end, step, 0)


def moe_kernel(side, chunks, groups, tokens_hbm, routes_ref, w_router_hbm, w_one_hbm, w_three_hbm, w_two_hbm, y_own, y_peers,
               toks, infos, own_info, plans, packed, relay, rows, w_router, w_one, w_three, w_two, parts, mids,
               load_sem, w_sem, s0_sem, r0_sem, sp_sem, rp_sem, s1_sem, r1_sem, s2_sem, r2_sem, b1_sem, c1_sem, b2_sem, c2_sem, s3_sem, r3_sem, out_sem, free2_sem, free3_sem):
    me = lax.axis_index('ep')
    dp = lax.axis_index('dp')
    num_tokens = tokens_hbm.shape[0]
    plane = 2 * side * side
    ends = 2 * side
    count = len(groups)
    arrival = (0, 1, 4, 2, 3, 5) if count == 6 else (1, 0, 2)
    near = (1, side - 1) if side > 2 else (1,)
    far = side > 2
    packed_rows = plane * SLOTS
    top_k = routes_ref.shape[0]
    orders = [ORDERS[g % 3] for g in range(count)]

    def remote(src, dst, s_sem, r_sem, axis, steps, core_steps=0):
        return pltpu.make_async_remote_copy(
            src_ref=src, dst_ref=dst, send_sem=s_sem, recv_sem=r_sem,
            device_id=(dp, moved(me, side, axis, steps, core_steps)), device_id_type=MESH)

    def columns(g):
        return pl.ds(*groups[g])

    def relay_from(g, q, b):
        return relay[g].at[q, b] if g % 3 == 1 else relay[g].at[q, :, b]

    def relay_others(g, q):
        return relay[g].at[q, pl.ds(1, side - 1)] if g % 3 == 1 else relay[g].at[q, :, pl.ds(1, side - 1)]

    def rows_at(g, q, e):
        c, core = e // 2, e % 2
        third = orders[g][2]
        where = {Z: (q, c, slice(None), slice(None), core), Y: (q, slice(None), c, slice(None), core),
                 X: (q, slice(None), slice(None), c, core)}[third]
        return where + (slice(None), columns(g))

    def half(i):
        return pl.ds(i * (num_tokens // 2), num_tokens // 2)

    def gather_near(g, d, i):
        part = half(i if d == 0 else 1 - i)
        return remote(tokens_hbm.at[part, columns(g)], toks[g].at[near[d], part],
                      s0_sem.at[g, 2 * d + i], r0_sem.at[g, 2 * d + i], orders[g][0], near[d])

    def gather_far(g, d):
        return remote(toks[g].at[near[d], half(d)], toks[g].at[2, half(d)],
                      s0_sem.at[g, 4 + d], r0_sem.at[g, 4 + d], orders[g][0], near[d])

    def gather_info(o, a):
        return remote(own_info, infos.at[o, a], sp_sem.at[o], rp_sem.at[o], ORDERS[o][0], a)

    def gather_info_all(o):
        others = infos.at[o, pl.ds(1, side - 1)]
        return remote(others, others, sp_sem.at[o], rp_sem.at[o], ORDERS[o][0], 1)

    def relay_slab(g, q, a, b):
        return relay[g].at[q, b, a] if g % 3 == 1 else relay[g].at[q, a, b]

    def out_second(g, q, a, b):
        return remote(packed[g].at[q, b, a], relay_slab(g, q, a, b), s1_sem.at[g, q], r1_sem.at[g, q], orders[g][1], b)

    def out_second_all(g, q):
        return remote(packed[g].at[q, pl.ds(1, side - 1)], relay_others(g, q), s1_sem.at[g, q], r1_sem.at[g, q], orders[g][1], 1)

    def out_third(g, q, e):
        return remote(relay[g].at[q, :, :, e], rows.at[rows_at(g, q, e)], s2_sem.at[g, q], r2_sem.at[g, q], orders[g][2], e // 2, e % 2)

    def third_all(g, q, s_sem, r_sem):
        some = relay[g].at[q, :, :, pl.ds(1, ends - 1)]
        return remote(some, some, s_sem.at[g, q], r_sem.at[g, q], orders[g][2], 1)

    def home_third(g, q, e):
        return remote(rows.at[rows_at(g, q, e)], relay[g].at[q, :, :, e], b1_sem.at[g, q], c1_sem.at[g, q], orders[g][2], -(e // 2), e % 2)

    def home_second(g, q, b):
        return remote(relay_from(g, q, b), packed[g].at[q, b], b2_sem.at[g, q], c2_sem.at[g, q], orders[g][1], -b)

    def home_second_all(g, q):
        return remote(relay_others(g, q), packed[g].at[q, pl.ds(1, side - 1)], b2_sem.at[g, q], c2_sem.at[g, q], orders[g][1], 1)

    def home_mid(g, d):
        return remote(parts.at[2, half(d), columns(g)], mids.at[d, :, columns(g)],
                      s3_sem.at[g, d], r3_sem.at[g, d], orders[g][0], -near[d])

    def home_near(g, d, i):
        part = half(1 - d if i == 0 else d)
        return remote(parts.at[near[d], part, columns(g)], y_peers.at[d, part, columns(g)],
                      s3_sem.at[g, 2 + 2 * d + i], r3_sem.at[g, 2 + 2 * d + i], orders[g][0], -near[d])

    def tell(sem, axis, steps, core_steps=0):
        pl.semaphore_signal(sem, inc=1, device_id=(dp, moved(me, side, axis, steps, core_steps)), device_id_type=MESH)

    loads = [pltpu.make_async_copy(tokens_hbm.at[:, columns(g)], toks[g].at[0], load_sem.at[g]) for g in range(count)]
    loads.append(pltpu.make_async_copy(w_router_hbm, w_router, load_sem.at[count]))
    weights = [pltpu.make_async_copy(src, dst, w_sem.at[i]) for i, (src, dst) in enumerate(
        [(w_one_hbm, w_one), (w_three_hbm, w_three), (w_two_hbm, w_two)])]
    for copy in loads:
        copy.start()

    barrier = pltpu.get_barrier_semaphore()
    tell(barrier, X, 0, 1)
    for axis in (Z, Y, X):
        for steps in range(1, side):
            for core_steps in range(2):
                tell(barrier, axis, steps, core_steps)
    with jax.named_scope('barrier'):
        pl.semaphore_wait(barrier, 1 + 3 * (side - 1) * 2)

    for i in range(2):
        for g in range(count):
            for d in range(len(near)):
                gather_near(g, d, i).start()
    with jax.named_scope('own_wait'):
        for copy in loads:
            copy.wait()

    num_experts = 2 * side ** 3
    logits = sum(jnp.dot(toks[g][0], w_router[columns(g), :], preferred_element_type=jnp.float32) for g in range(count)).T
    ids = lax.broadcasted_iota(jnp.int32, (num_experts, num_tokens), 0)
    picks = [routes_ref[k:k + 1, :] for k in range(top_k)]
    scores = [jnp.sum(jnp.where(pick == ids, logits, 0.0), axis=0, keepdims=True) for pick in picks]
    peak = functools.reduce(jnp.maximum, scores)
    scores = [jnp.exp(score - peak) for score in scores]
    norm = sum(scores)
    for k in range(top_k):
        own_info[k:k + 1, :] = picks[k].astype(jnp.float32)
        own_info[top_k + k:top_k + k + 1, :] = scores[k] / norm
    for o in range(3):
        for a in range(1, side):
            gather_info(o, a).start()
    before = (lax.broadcasted_iota(jnp.int32, (num_tokens, num_tokens), 0)
              < lax.broadcasted_iota(jnp.int32, (num_tokens, num_tokens), 1))
    before = jnp.where(before, 1.0, 0.0).astype(jnp.bfloat16)
    expert_at = [plane_experts(me, side, order, num_tokens).astype(jnp.float32) for order in ORDERS]

    def make_plan(o, a, info):
        mask = jnp.zeros((plane, num_tokens), jnp.float32)
        gate = jnp.zeros((plane, num_tokens), jnp.float32)
        for k in range(top_k):
            hit = info[k:k + 1] == expert_at[o]
            mask = jnp.where(hit, 1.0, mask)
            gate = jnp.where(hit, info[top_k + k:top_k + k + 1], gate)
        slot = jnp.dot(mask.astype(jnp.bfloat16), before, preferred_element_type=jnp.float32)
        plans[o][a, pl.ds(0, plane), :] = jnp.where(mask > 0.0, slot, -1.0)
        plans[o][a, pl.ds(plane, plane), :] = gate

    for o in range(3):
        make_plan(o, 0, own_info[...])
    for copy in weights:
        copy.start()

    def taken(g, q, a):
        slots = plans[g % 3][a, pl.ds(0, plane), :]
        ids = lax.broadcasted_iota(jnp.int32, (plane, SLOTS, num_tokens), 1) + q * SLOTS
        return jnp.broadcast_to(slots[:, None, :], (plane, SLOTS, num_tokens)) == ids.astype(jnp.float32)

    def pack(g, q, a):
        select = jnp.where(taken(g, q, a), 1.0, 0.0).reshape(packed_rows, num_tokens).astype(jnp.bfloat16)
        out = jnp.dot(select, toks[g][a], preferred_element_type=jnp.float32)
        out = out.reshape(side, ends, SLOTS, groups[g][1]).astype(jnp.bfloat16)
        packed[g][q, pl.ds(1, side - 1), a] = out[1:]
        each(1, side, lambda b: out_second(g, q, a, b).start())
        relay_slab(g, q, a, 0)[...] = out[0]

    def pack_own(q, carry):
        for g in range(count):
            pack(g, q, 0)
        return carry

    if far:
        with jax.named_scope('gather_far'):
            for g in range(count):
                for d in range(2):
                    gather_near(g, d, 0).wait_recv()
                    gather_far(g, d).start()
    with jax.named_scope('pack_own'):
        lax.fori_loop(0, chunks, pack_own, 0)
    parts[...] = jnp.zeros_like(parts)
    with jax.named_scope('gather_wait'):
        for o in range(3):
            gather_info_all(o).wait_recv()
            for a in range(1, side):
                make_plan(o, a, infos[o, a])
        for g in range(count):
            for d in range(len(near)):
                if not far:
                    gather_near(g, d, 0).wait_recv()
                gather_near(g, d, 1).wait_recv()
            if far:
                gather_far(g, 0).wait_recv()
                gather_far(g, 1).wait_recv()

    def outward(i, carry):
        @pl.when(i < chunks)
        def _():
            for g in range(count):
                def source(a, c):
                    pack(g, i, a)
                    return c
                with jax.named_scope('pack'):
                    lax.fori_loop(1, side, source, 0)

        @pl.when(i > 0)
        def _():
            forward(i - 1)
        return carry

    def forward(q):
        for g in range(count):
            with jax.named_scope('s1_wait'):
                out_second_all(g, q).wait_recv()
            each(1, ends, lambda e: out_third(g, q, e).start())
            rows[rows_at(g, q, 0)] = relay[g][q, :, :, 0]
            with jax.named_scope('s1_send_wait'):
                out_second_all(g, q).wait_send()
            each(1, side, lambda b: tell(free2_sem.at[g, q], orders[g][1], b))

    lax.fori_loop(0, chunks + 1, outward, 0)
    for copy in weights:
        copy.wait()

    def experts(q, carry):
        with jax.named_scope('s2_wait'):
            for g in range(count):
                third_all(g, q, s2_sem, r2_sem).wait_recv()
        for g in range(count):
            with jax.named_scope('s2_send_wait'):
                third_all(g, q, s2_sem, r2_sem).wait_send()
            each(1, ends, lambda e: tell(free3_sem.at[g, q], orders[g][2], e // 2, e % 2))

        def block(z, c):
            shape = rows.shape[2:]
            u = rows[q, z].astype(jnp.float32).reshape(packed_rows, shape[-1]).astype(jnp.bfloat16)
            gate_pre = jnp.dot(u, w_one[...], preferred_element_type=jnp.float32)
            up_pre = jnp.dot(u, w_three[...], preferred_element_type=jnp.float32)
            hidden = (jax.nn.silu(gate_pre) * up_pre).astype(jnp.bfloat16)
            out = jnp.dot(hidden, w_two[...], preferred_element_type=jnp.float32)
            rows[q, z] = out.reshape(shape).astype(jnp.bfloat16)
            return c
        with jax.named_scope('mlp'):
            lax.fori_loop(0, side, block, 0)
        for g in range(count):
            with jax.named_scope('free3'):
                pl.semaphore_wait(free3_sem.at[g, q], ends - 1)
            each(1, ends, lambda e: home_third(g, q, e).start())
            relay[g][q, :, :, 0] = rows[rows_at(g, q, 0)]
        return carry

    lax.fori_loop(0, chunks, experts, 0)

    def backward(q):
        for g in range(count):
            with jax.named_scope('r1_wait'):
                third_all(g, q, b1_sem, c1_sem).wait_recv()
            pl.semaphore_wait(free2_sem.at[g, q], side - 1)
            each(1, side, lambda b: home_second(g, q, b).start())
            packed[g][q, 0] = relay_from(g, q, 0)[...]

    ahead = w_one.shape[1] >= 3 * packed_rows and w_one.shape[0] >= 2 * side * num_tokens

    def gate_rows(o, a):
        return pl.ds(pl.multiple_of(((o % 2) * side + a) * num_tokens, num_tokens), num_tokens)

    def gate_parts(g, q, a):
        gates = plans[g % 3][a, pl.ds(plane, plane), :]
        used = taken(g, q, a)
        for _ in range(3):
            part = gates.astype(jnp.bfloat16).astype(jnp.float32)
            gates = gates - part
            yield jnp.where(used, jnp.broadcast_to(part[:, None, :], used.shape), 0.0).reshape(packed_rows, num_tokens)

    def build_gates(q):
        for o in range(3):
            def build(a):
                for i, mix in enumerate(gate_parts(o, q, a)):
                    home = w_one if o < 2 else w_three
                    home[gate_rows(o, a), i * packed_rows:(i + 1) * packed_rows] = mix.T.astype(jnp.bfloat16)
            each(0, side, build)

    def combine(q):
        last = q == chunks - 1
        if ahead:
            with jax.named_scope('gates_ahead'):
                build_gates(q)
        for g in arrival:
            with jax.named_scope('r2_wait'):
                home_second_all(g, q).wait_recv()
            width = groups[g][1]

            def source(i, c):
                a = (i + side // 2) % side
                o = packed[g][q, :, a].astype(jnp.float32).reshape(packed_rows, width).astype(jnp.bfloat16)
                if ahead:
                    mixes = w_one if g % 3 < 2 else w_three
                    terms = [jnp.dot(mixes[gate_rows(g % 3, a), i * packed_rows:(i + 1) * packed_rows], o, preferred_element_type=jnp.float32)
                             for i in range(3)]
                else:
                    terms = [lax.dot_general(mix.astype(jnp.bfloat16), o, (((0,), (0,)), ((), ())), preferred_element_type=jnp.float32)
                             for mix in gate_parts(g, q, a)]
                parts[a, :, columns(g)] += terms[0] + terms[1] + terms[2]

                if far:
                    @pl.when(jnp.logical_and(last, a == 2))
                    def _():
                        home_mid(g, 0).start()
                        home_mid(g, 1).start()
                for d in range(len(near)):
                    @pl.when(jnp.logical_and(last, a == near[d]))
                    def _():
                        home_near(g, d, 0).start()
                return c
            with jax.named_scope('combine'):
                lax.fori_loop(0, side, source, 0)

    def send_home(q, carry):
        backward(q)
        return carry

    def sum_up(q, carry):
        combine(q)
        return carry

    lax.fori_loop(0, chunks, send_home, 0)
    lax.fori_loop(0, chunks, sum_up, 0)
    own = pltpu.make_async_copy(parts.at[0], y_own, out_sem)
    own.start()
    for g in arrival:
        for d in range(len(near)):
            if far:
                with jax.named_scope('mid_wait'):
                    home_mid(g, d).wait_recv()
                parts[near[d], half(d), columns(g)] += mids[d, :, columns(g)]
            home_near(g, d, 1).start()

    for g in range(count):
        def drain(q, c):
            third_all(g, q, b1_sem, c1_sem).wait_send()
            home_second_all(g, q).wait_send()
            return c
        lax.fori_loop(0, chunks, drain, 0)
        for d in range(len(near)):
            gather_near(g, d, 0).wait_send()
            gather_near(g, d, 1).wait_send()
            if far:
                gather_far(g, d).wait_send()
                home_mid(g, d).wait_send()
    for o in range(3):
        gather_info_all(o).wait_send()
    for g in arrival:
        for d in range(len(near)):
            for i in range(2):
                with jax.named_scope('r3_wait'):
                    home_near(g, d, i).wait_recv()
                    home_near(g, d, i).wait_send()
    own.wait()


def solution(mesh):
    group_size = mesh.shape['ep']
    side = torus_side(group_size)
    row_spec = P(('dp', 'ep'), None)
    expert_spec = P('ep', None, None)

    def device_step(tokens, routes, w_router, w_one, w_three, w_two):
        num_tokens, d_model = tokens.shape
        top_k = routes.shape[1]
        num_experts = w_router.shape[1]
        d_expert = w_one.shape[2]
        capacity = slot_capacity(num_tokens, top_k, num_experts)
        chunks = capacity // SLOTS
        groups = column_groups(d_model)
        count = len(groups)
        plane = 2 * side * side
        hbm = pl.BlockSpec(memory_space=pl.ANY)
        vmem = pl.BlockSpec(memory_space=pltpu.VMEM)
        dma = pltpu.SemaphoreType.DMA
        slab = [[pltpu.VMEM((chunks, side, side, 2 * side, SLOTS, width), jnp.bfloat16) for _, width in groups] for _ in range(2)]
        pair = [dma((count, chunks)), dma((count, chunks))]
        y_own, y_peers = pl.pallas_call(
            functools.partial(moe_kernel, side, chunks, groups),
            out_shape=(jax.ShapeDtypeStruct((num_tokens, d_model), jnp.float32),
                       jax.ShapeDtypeStruct((2 if side > 2 else 1, num_tokens, d_model), jnp.float32)),
            in_specs=[hbm, vmem, hbm, hbm, hbm, hbm],
            out_specs=(hbm, hbm),
            scratch_shapes=[
                [pltpu.VMEM((side, num_tokens, width), jnp.bfloat16) for _, width in groups],
                pltpu.VMEM((3, side, 2 * top_k, num_tokens), jnp.float32),
                pltpu.VMEM((2 * top_k, num_tokens), jnp.float32),
                [pltpu.VMEM((side, 2 * plane, num_tokens), jnp.float32) for _ in ORDERS],
                slab[0], slab[1],
                pltpu.VMEM((chunks, side, side, side, 2, SLOTS, d_model), jnp.bfloat16),
                pltpu.VMEM((d_model, num_experts), jnp.bfloat16),
                pltpu.VMEM((d_model, d_expert), jnp.bfloat16),
                pltpu.VMEM((d_model, d_expert), jnp.bfloat16),
                pltpu.VMEM((d_expert, d_model), jnp.bfloat16),
                pltpu.VMEM((side, num_tokens, d_model), jnp.float32),
                pltpu.VMEM((2, num_tokens // 2, d_model), jnp.float32),
                dma((count + 1,)), dma((3,)), dma((count, 6)), dma((count, 6)), dma((3,)), dma((3,)),
                *pair, *pair, *pair, *pair, dma((count, 6)), dma((count, 6)), dma,
                pltpu.SemaphoreType.REGULAR((count, chunks)), pltpu.SemaphoreType.REGULAR((count, chunks)),
            ],
            compiler_params=pltpu.CompilerParams(collective_id=0, has_side_effects=True, vmem_limit_bytes=67043328),
            name='moe',
        )(tokens, routes.T, w_router, w_one[0], w_three[0], w_two[0])
        total = y_own
        for i in range(y_peers.shape[0]):
            total = total + y_peers[i]
        return total.astype(jnp.bfloat16)

    return jax.shard_map(device_step, mesh=mesh, in_specs=(row_spec, row_spec, P(None, None), expert_spec, expert_spec, expert_spec), out_specs=row_spec, check_vma=False)
```

```python
import functools

import jax
import jax.numpy as jnp
from jax import lax
from jax.experimental import pallas as pl
from jax.experimental.pallas import tpu as pltpu
from jax.sharding import PartitionSpec as P

MESH = pl.DeviceIdType.MESH
Z, Y, X = 0, 1, 2
ORDERS = ((Z, Y, X), (X, Z, Y), (Y, X, Z))
SLOTS = 8


def slot_capacity(num_tokens, top_k, num_experts):
    return 8 * ((3 * num_tokens * top_k + 16 * num_experts - 1) // (16 * num_experts))


def torus_side(group_size):
    side = 1
    while 2 * side ** 3 < group_size:
        side += 1
    return side


def column_groups(d_model):
    lanes = d_model // 128
    count = 6 if lanes >= 6 else 3
    widths = [128 * (lanes // count + (1 if i < lanes % count else 0)) for i in range(count)]
    starts = [sum(widths[:i]) for i in range(count)]
    return list(zip(starts, widths))


def moved(me, side, axis, steps, core_steps=0):
    digits = [me // (2 * side * side), (me // (2 * side)) % side, (me // 2) % side]
    digits[axis] = (digits[axis] + steps + side) % side
    return ((digits[Z] * side + digits[Y]) * side + digits[X]) * 2 + (me + core_steps) % 2


def plane_experts(me, side, order, num_tokens):
    bits = side.bit_length() - 1
    position = lax.broadcasted_iota(jnp.int32, (2 * side * side, num_tokens), 0)
    digits = [me // (2 * side * side), (me // (2 * side)) % side, (me // 2) % side]
    for place, axis in enumerate(order[1:]):
        steps = jnp.right_shift(position, 1 + (1 - place) * bits)
        digits[axis] = jnp.bitwise_and(digits[axis] + steps, side - 1)
    core = jnp.bitwise_and(me + position, 1)
    return ((digits[Z] * side + digits[Y]) * side + digits[X]) * 2 + core


def each(first, end, act):
    def step(i, carry):
        act(i)
        return carry
    lax.fori_loop(first, end, step, 0)


def moe_kernel(side, chunks, groups, tokens_hbm, routes_ref, w_router_hbm, w_one_hbm, w_three_hbm, w_two_hbm, y_own, y_peers,
               toks, infos, own_info, plans, packed, relay, rows, w_router, w_one, w_three, w_two, parts, mids,
               load_sem, w_sem, s0_sem, r0_sem, sp_sem, rp_sem, s1_sem, r1_sem, s2_sem, r2_sem, b1_sem, c1_sem, b2_sem, c2_sem, s3_sem, r3_sem, out_sem, free2_sem, free3_sem):
    me = lax.axis_index('ep')
    dp = lax.axis_index('dp')
    num_tokens = tokens_hbm.shape[0]
    plane = 2 * side * side
    ends = 2 * side
    count = len(groups)
    arrival = (0, 1, 4, 2, 3, 5) if count == 6 else (1, 0, 2)
    near = (1, side - 1) if side > 2 else (1,)
    far = side > 2
    packed_rows = plane * SLOTS
    top_k = routes_ref.shape[0]
    orders = [ORDERS[g % 3] for g in range(count)]

    def remote(src, dst, s_sem, r_sem, axis, steps, core_steps=0):
        return pltpu.make_async_remote_copy(
            src_ref=src, dst_ref=dst, send_sem=s_sem, recv_sem=r_sem,
            device_id=(dp, moved(me, side, axis, steps, core_steps)), device_id_type=MESH)

    def columns(g):
        return pl.ds(*groups[g])

    def relay_from(g, q, b):
        return relay[g].at[q, b] if g % 3 == 1 else relay[g].at[q, :, b]

    def relay_others(g, q):
        return relay[g].at[q, pl.ds(1, side - 1)] if g % 3 == 1 else relay[g].at[q, :, pl.ds(1, side - 1)]

    def rows_at(g, q, e):
        c, core = e // 2, e % 2
        third = orders[g][2]
        where = {Z: (q, c, slice(None), slice(None), core), Y: (q, slice(None), c, slice(None), core),
                 X: (q, slice(None), slice(None), c, core)}[third]
        return where + (slice(None), columns(g))

    def half(i):
        return pl.ds(i * (num_tokens // 2), num_tokens // 2)

    def gather_near(g, d, i):
        part = half(i if d == 0 else 1 - i)
        return remote(toks[g].at[0, part], toks[g].at[near[d], part],
                      s0_sem.at[g, 2 * d + i], r0_sem.at[g, 2 * d + i], orders[g][0], near[d])

    def gather_far(g, d):
        return remote(toks[g].at[near[d], half(d)], toks[g].at[2, half(d)],
                      s0_sem.at[g, 4 + d], r0_sem.at[g, 4 + d], orders[g][0], near[d])

    def gather_info(o, a):
        return remote(own_info, infos.at[o, a], sp_sem.at[o], rp_sem.at[o], ORDERS[o][0], a)

    def gather_info_all(o):
        others = infos.at[o, pl.ds(1, side - 1)]
        return remote(others, others, sp_sem.at[o], rp_sem.at[o], ORDERS[o][0], 1)

    def relay_slab(g, q, a, b):
        return relay[g].at[q, b, a] if g % 3 == 1 else relay[g].at[q, a, b]

    def out_second(g, q, a, b):
        return remote(packed[g].at[q, b, a], relay_slab(g, q, a, b), s1_sem.at[g, q], r1_sem.at[g, q], orders[g][1], b)

    def out_second_all(g, q):
        return remote(packed[g].at[q, pl.ds(1, side - 1)], relay_others(g, q), s1_sem.at[g, q], r1_sem.at[g, q], orders[g][1], 1)

    def out_third(g, q, e):
        return remote(relay[g].at[q, :, :, e], rows.at[rows_at(g, q, e)], s2_sem.at[g, q], r2_sem.at[g, q], orders[g][2], e // 2, e % 2)

    def third_all(g, q, s_sem, r_sem):
        some = relay[g].at[q, :, :, pl.ds(1, ends - 1)]
        return remote(some, some, s_sem.at[g, q], r_sem.at[g, q], orders[g][2], 1)

    def home_third(g, q, e):
        return remote(rows.at[rows_at(g, q, e)], relay[g].at[q, :, :, e], b1_sem.at[g, q], c1_sem.at[g, q], orders[g][2], -(e // 2), e % 2)

    def home_second(g, q, b):
        return remote(relay_from(g, q, b), packed[g].at[q, b], b2_sem.at[g, q], c2_sem.at[g, q], orders[g][1], -b)

    def home_second_all(g, q):
        return remote(relay_others(g, q), packed[g].at[q, pl.ds(1, side - 1)], b2_sem.at[g, q], c2_sem.at[g, q], orders[g][1], 1)

    def home_mid(g, d):
        return remote(parts.at[2, half(d), columns(g)], mids.at[d, :, columns(g)],
                      s3_sem.at[g, d], r3_sem.at[g, d], orders[g][0], -near[d])

    def home_near(g, d, i):
        part = half(1 - d if i == 0 else d)
        return remote(parts.at[near[d], part, columns(g)], y_peers.at[d, part, columns(g)],
                      s3_sem.at[g, 2 + 2 * d + i], r3_sem.at[g, 2 + 2 * d + i], orders[g][0], -near[d])

    def tell(sem, axis, steps, core_steps=0):
        pl.semaphore_signal(sem, inc=1, device_id=(dp, moved(me, side, axis, steps, core_steps)), device_id_type=MESH)

    loads = [pltpu.make_async_copy(tokens_hbm.at[:, columns(g)], toks[g].at[0], load_sem.at[g]) for g in range(count)]
    loads.append(pltpu.make_async_copy(w_router_hbm, w_router, load_sem.at[count]))
    weights = [pltpu.make_async_copy(src, dst, w_sem.at[i]) for i, (src, dst) in enumerate(
        [(w_one_hbm, w_one), (w_three_hbm, w_three), (w_two_hbm, w_two)])]
    barrier = pltpu.get_barrier_semaphore()
    tell(barrier, X, 0, 1)
    for axis in (Z, Y, X):
        for steps in range(1, side):
            for core_steps in range(2):
                tell(barrier, axis, steps, core_steps)
    for copy in loads:
        copy.start()
    with jax.named_scope('own_wait'):
        for copy in loads:
            copy.wait()
    with jax.named_scope('barrier'):
        pl.semaphore_wait(barrier, 1 + 3 * (side - 1) * 2)

    for i in range(2):
        for g in range(count):
            for d in range(len(near)):
                gather_near(g, d, i).start()

    num_experts = 2 * side ** 3
    logits = sum(jnp.dot(toks[g][0], w_router[columns(g), :], preferred_element_type=jnp.float32) for g in range(count)).T
    ids = lax.broadcasted_iota(jnp.int32, (num_experts, num_tokens), 0)
    picks = [routes_ref[k:k + 1, :] for k in range(top_k)]
    scores = [jnp.sum(jnp.where(pick == ids, logits, 0.0), axis=0, keepdims=True) for pick in picks]
    peak = functools.reduce(jnp.maximum, scores)
    scores = [jnp.exp(score - peak) for score in scores]
    norm = sum(scores)
    for k in range(top_k):
        own_info[k:k + 1, :] = picks[k].astype(jnp.float32)
        own_info[top_k + k:top_k + k + 1, :] = scores[k] / norm
    for o in range(3):
        for a in range(1, side):
            gather_info(o, a).start()
    before = (lax.broadcasted_iota(jnp.int32, (num_tokens, num_tokens), 0)
              < lax.broadcasted_iota(jnp.int32, (num_tokens, num_tokens), 1))
    before = jnp.where(before, 1.0, 0.0).astype(jnp.bfloat16)
    expert_at = [plane_experts(me, side, order, num_tokens).astype(jnp.float32) for order in ORDERS]

    def make_plan(o, a, info):
        mask = jnp.zeros((plane, num_tokens), jnp.float32)
        gate = jnp.zeros((plane, num_tokens), jnp.float32)
        for k in range(top_k):
            hit = info[k:k + 1] == expert_at[o]
            mask = jnp.where(hit, 1.0, mask)
            gate = jnp.where(hit, info[top_k + k:top_k + k + 1], gate)
        slot = jnp.dot(mask.astype(jnp.bfloat16), before, preferred_element_type=jnp.float32)
        plans[o][a, pl.ds(0, plane), :] = jnp.where(mask > 0.0, slot, -1.0)
        plans[o][a, pl.ds(plane, plane), :] = gate

    for o in range(3):
        make_plan(o, 0, own_info[...])
    for copy in weights:
        copy.start()

    def taken(g, q, a):
        slots = plans[g % 3][a, pl.ds(0, plane), :]
        ids = lax.broadcasted_iota(jnp.int32, (plane, SLOTS, num_tokens), 1) + q * SLOTS
        return jnp.broadcast_to(slots[:, None, :], (plane, SLOTS, num_tokens)) == ids.astype(jnp.float32)

    def pack(g, q, a):
        select = jnp.where(taken(g, q, a), 1.0, 0.0).reshape(packed_rows, num_tokens).astype(jnp.bfloat16)
        out = jnp.dot(select, toks[g][a], preferred_element_type=jnp.float32)
        out = out.reshape(side, ends, SLOTS, groups[g][1]).astype(jnp.bfloat16)
        packed[g][q, pl.ds(1, side - 1), a] = out[1:]
        each(1, side, lambda b: out_second(g, q, a, b).start())
        relay_slab(g, q, a, 0)[...] = out[0]

    def pack_own(q, carry):
        for g in range(count):
            pack(g, q, 0)
        return carry

    if far:
        with jax.named_scope('gather_far'):
            for g in range(count):
                for d in range(2):
                    gather_near(g, d, 0).wait_recv()
                    gather_far(g, d).start()
    with jax.named_scope('pack_own'):
        lax.fori_loop(0, chunks, pack_own, 0)
    parts[...] = jnp.zeros_like(parts)
    with jax.named_scope('gather_wait'):
        for o in range(3):
            gather_info_all(o).wait_recv()
            for a in range(1, side):
                make_plan(o, a, infos[o, a])
        for g in range(count):
            for d in range(len(near)):
                if not far:
                    gather_near(g, d, 0).wait_recv()
                gather_near(g, d, 1).wait_recv()
            if far:
                gather_far(g, 0).wait_recv()
                gather_far(g, 1).wait_recv()

    def outward(i, carry):
        @pl.when(i < chunks)
        def _():
            for g in range(count):
                def source(a, c):
                    pack(g, i, a)
                    return c
                with jax.named_scope('pack'):
                    lax.fori_loop(1, side, source, 0)

        @pl.when(i > 0)
        def _():
            forward(i - 1)
        return carry

    def forward(q):
        for g in range(count):
            with jax.named_scope('s1_wait'):
                out_second_all(g, q).wait_recv()
            each(1, ends, lambda e: out_third(g, q, e).start())
            rows[rows_at(g, q, 0)] = relay[g][q, :, :, 0]
            with jax.named_scope('s1_send_wait'):
                out_second_all(g, q).wait_send()
            each(1, side, lambda b: tell(free2_sem.at[g, q], orders[g][1], b))

    lax.fori_loop(0, chunks + 1, outward, 0)
    for copy in weights:
        copy.wait()

    def experts(q, carry):
        with jax.named_scope('s2_wait'):
            for g in range(count):
                third_all(g, q, s2_sem, r2_sem).wait_recv()
        for g in range(count):
            with jax.named_scope('s2_send_wait'):
                third_all(g, q, s2_sem, r2_sem).wait_send()
            each(1, ends, lambda e: tell(free3_sem.at[g, q], orders[g][2], e // 2, e % 2))

        def block(z, c):
            shape = rows.shape[2:]
            u = rows[q, z].astype(jnp.float32).reshape(packed_rows, shape[-1]).astype(jnp.bfloat16)
            gate_pre = jnp.dot(u, w_one[...], preferred_element_type=jnp.float32)
            up_pre = jnp.dot(u, w_three[...], preferred_element_type=jnp.float32)
            hidden = (jax.nn.silu(gate_pre) * up_pre).astype(jnp.bfloat16)
            out = jnp.dot(hidden, w_two[...], preferred_element_type=jnp.float32)
            rows[q, z] = out.reshape(shape).astype(jnp.bfloat16)
            return c
        with jax.named_scope('mlp'):
            lax.fori_loop(0, side, block, 0)
        for g in range(count):
            with jax.named_scope('free3'):
                pl.semaphore_wait(free3_sem.at[g, q], ends - 1)
            each(1, ends, lambda e: home_third(g, q, e).start())
            relay[g][q, :, :, 0] = rows[rows_at(g, q, 0)]
        return carry

    lax.fori_loop(0, chunks, experts, 0)

    def backward(q):
        for g in range(count):
            with jax.named_scope('r1_wait'):
                third_all(g, q, b1_sem, c1_sem).wait_recv()
            pl.semaphore_wait(free2_sem.at[g, q], side - 1)
            each(1, side, lambda b: home_second(g, q, b).start())
            packed[g][q, 0] = relay_from(g, q, 0)[...]

    ahead = w_one.shape[1] >= 3 * packed_rows and w_one.shape[0] >= 2 * side * num_tokens

    def gate_rows(o, a):
        return pl.ds(pl.multiple_of(((o % 2) * side + a) * num_tokens, num_tokens), num_tokens)

    def gate_parts(g, q, a):
        gates = plans[g % 3][a, pl.ds(plane, plane), :]
        used = taken(g, q, a)
        for _ in range(3):
            part = gates.astype(jnp.bfloat16).astype(jnp.float32)
            gates = gates - part
            yield jnp.where(used, jnp.broadcast_to(part[:, None, :], used.shape), 0.0).reshape(packed_rows, num_tokens)

    def build_gates(q):
        for o in range(3):
            def build(a):
                for i, mix in enumerate(gate_parts(o, q, a)):
                    home = w_one if o < 2 else w_three
                    home[gate_rows(o, a), i * packed_rows:(i + 1) * packed_rows] = mix.T.astype(jnp.bfloat16)
            each(0, side, build)

    def combine(q):
        last = q == chunks - 1
        if ahead:
            with jax.named_scope('gates_ahead'):
                build_gates(q)
        for g in arrival:
            with jax.named_scope('r2_wait'):
                home_second_all(g, q).wait_recv()
            width = groups[g][1]

            def source(i, c):
                a = (i + side // 2) % side
                o = packed[g][q, :, a].astype(jnp.float32).reshape(packed_rows, width).astype(jnp.bfloat16)
                if ahead:
                    mixes = w_one if g % 3 < 2 else w_three
                    terms = [jnp.dot(mixes[gate_rows(g % 3, a), i * packed_rows:(i + 1) * packed_rows], o, preferred_element_type=jnp.float32)
                             for i in range(3)]
                else:
                    terms = [lax.dot_general(mix.astype(jnp.bfloat16), o, (((0,), (0,)), ((), ())), preferred_element_type=jnp.float32)
                             for mix in gate_parts(g, q, a)]
                parts[a, :, columns(g)] += terms[0] + terms[1] + terms[2]

                if far:
                    @pl.when(jnp.logical_and(last, a == 2))
                    def _():
                        home_mid(g, 0).start()
                        home_mid(g, 1).start()
                for d in range(len(near)):
                    @pl.when(jnp.logical_and(last, a == near[d]))
                    def _():
                        home_near(g, d, 0).start()
                return c
            with jax.named_scope('combine'):
                lax.fori_loop(0, side, source, 0)

    def send_home(q, carry):
        backward(q)
        return carry

    def sum_up(q, carry):
        combine(q)
        return carry

    lax.fori_loop(0, chunks, send_home, 0)
    lax.fori_loop(0, chunks, sum_up, 0)
    own = pltpu.make_async_copy(parts.at[0], y_own, out_sem)
    own.start()
    for g in arrival:
        for d in range(len(near)):
            if far:
                with jax.named_scope('mid_wait'):
                    home_mid(g, d).wait_recv()
                parts[near[d], half(d), columns(g)] += mids[d, :, columns(g)]
            home_near(g, d, 1).start()

    for g in range(count):
        def drain(q, c):
            third_all(g, q, b1_sem, c1_sem).wait_send()
            home_second_all(g, q).wait_send()
            return c
        lax.fori_loop(0, chunks, drain, 0)
        for d in range(len(near)):
            gather_near(g, d, 0).wait_send()
            gather_near(g, d, 1).wait_send()
            if far:
                gather_far(g, d).wait_send()
                home_mid(g, d).wait_send()
    for o in range(3):
        gather_info_all(o).wait_send()
    for g in arrival:
        for d in range(len(near)):
            for i in range(2):
                with jax.named_scope('r3_wait'):
                    home_near(g, d, i).wait_recv()
                    home_near(g, d, i).wait_send()
    own.wait()


def solution(mesh):
    group_size = mesh.shape['ep']
    side = torus_side(group_size)
    row_spec = P(('dp', 'ep'), None)
    expert_spec = P('ep', None, None)

    def device_step(tokens, routes, w_router, w_one, w_three, w_two):
        num_tokens, d_model = tokens.shape
        top_k = routes.shape[1]
        num_experts = w_router.shape[1]
        d_expert = w_one.shape[2]
        capacity = slot_capacity(num_tokens, top_k, num_experts)
        chunks = capacity // SLOTS
        groups = column_groups(d_model)
        count = len(groups)
        plane = 2 * side * side
        hbm = pl.BlockSpec(memory_space=pl.ANY)
        vmem = pl.BlockSpec(memory_space=pltpu.VMEM)
        dma = pltpu.SemaphoreType.DMA
        slab = [[pltpu.VMEM((chunks, side, side, 2 * side, SLOTS, width), jnp.bfloat16) for _, width in groups] for _ in range(2)]
        pair = [dma((count, chunks)), dma((count, chunks))]
        y_own, y_peers = pl.pallas_call(
            functools.partial(moe_kernel, side, chunks, groups),
            out_shape=(jax.ShapeDtypeStruct((num_tokens, d_model), jnp.float32),
                       jax.ShapeDtypeStruct((2 if side > 2 else 1, num_tokens, d_model), jnp.float32)),
            in_specs=[hbm, vmem, hbm, hbm, hbm, hbm],
            out_specs=(hbm, hbm),
            scratch_shapes=[
                [pltpu.VMEM((side, num_tokens, width), jnp.bfloat16) for _, width in groups],
                pltpu.VMEM((3, side, 2 * top_k, num_tokens), jnp.float32),
                pltpu.VMEM((2 * top_k, num_tokens), jnp.float32),
                [pltpu.VMEM((side, 2 * plane, num_tokens), jnp.float32) for _ in ORDERS],
                slab[0], slab[1],
                pltpu.VMEM((chunks, side, side, side, 2, SLOTS, d_model), jnp.bfloat16),
                pltpu.VMEM((d_model, num_experts), jnp.bfloat16),
                pltpu.VMEM((d_model, d_expert), jnp.bfloat16),
                pltpu.VMEM((d_model, d_expert), jnp.bfloat16),
                pltpu.VMEM((d_expert, d_model), jnp.bfloat16),
                pltpu.VMEM((side, num_tokens, d_model), jnp.float32),
                pltpu.VMEM((2, num_tokens // 2, d_model), jnp.float32),
                dma((count + 1,)), dma((3,)), dma((count, 6)), dma((count, 6)), dma((3,)), dma((3,)),
                *pair, *pair, *pair, *pair, dma((count, 6)), dma((count, 6)), dma,
                pltpu.SemaphoreType.REGULAR((count, chunks)), pltpu.SemaphoreType.REGULAR((count, chunks)),
            ],
            compiler_params=pltpu.CompilerParams(collective_id=0, has_side_effects=True, vmem_limit_bytes=67043328),
            name='moe',
        )(tokens, routes.T, w_router, w_one[0], w_three[0], w_two[0])
        total = y_own
        for i in range(y_peers.shape[0]):
            total = total + y_peers[i]
        return total.astype(jnp.bfloat16)

    return jax.shard_map(device_step, mesh=mesh, in_specs=(row_spec, row_spec, P(None, None), expert_spec, expert_spec, expert_spec), out_specs=row_spec, check_vma=False)
```

```python
import functools

import jax
import jax.numpy as jnp
from jax import lax
from jax.experimental import pallas as pl
from jax.experimental.pallas import tpu as pltpu
from jax.sharding import PartitionSpec as P

MESH = pl.DeviceIdType.MESH
Z, Y, X = 0, 1, 2
ORDERS = ((Z, Y, X), (X, Z, Y), (Y, X, Z))
SLOTS = 8


def slot_capacity(num_tokens, top_k, num_experts):
    return 8 * ((3 * num_tokens * top_k + 16 * num_experts - 1) // (16 * num_experts))


def torus_side(group_size):
    side = 1
    while 2 * side ** 3 < group_size:
        side += 1
    return side


def column_groups(d_model):
    lanes = d_model // 128
    count = 6 if lanes >= 6 else 3
    widths = [128 * (lanes // count + (1 if i < lanes % count else 0)) for i in range(count)]
    starts = [sum(widths[:i]) for i in range(count)]
    return list(zip(starts, widths))


def moved(me, side, axis, steps, core_steps=0):
    digits = [me // (2 * side * side), (me // (2 * side)) % side, (me // 2) % side]
    digits[axis] = (digits[axis] + steps + side) % side
    return ((digits[Z] * side + digits[Y]) * side + digits[X]) * 2 + (me + core_steps) % 2


def plane_experts(me, side, order, num_tokens):
    bits = side.bit_length() - 1
    position = lax.broadcasted_iota(jnp.int32, (2 * side * side, num_tokens), 0)
    digits = [me // (2 * side * side), (me // (2 * side)) % side, (me // 2) % side]
    for place, axis in enumerate(order[1:]):
        steps = jnp.right_shift(position, 1 + (1 - place) * bits)
        digits[axis] = jnp.bitwise_and(digits[axis] + steps, side - 1)
    core = jnp.bitwise_and(me + position, 1)
    return ((digits[Z] * side + digits[Y]) * side + digits[X]) * 2 + core


def each(first, end, act):
    def step(i, carry):
        act(i)
        return carry
    lax.fori_loop(first, end, step, 0)


def moe_kernel(side, chunks, groups, tokens_hbm, routes_ref, w_router_hbm, w_one_hbm, w_three_hbm, w_two_hbm, y_own, y_peers,
               toks, infos, own_info, plans, packed, relay, rows, w_router, w_one, w_three, w_two, parts, mids,
               load_sem, w_sem, s0_sem, r0_sem, sp_sem, rp_sem, s1_sem, r1_sem, s2_sem, r2_sem, b1_sem, c1_sem, b2_sem, c2_sem, s3_sem, r3_sem, out_sem, free2_sem, free3_sem):
    me = lax.axis_index('ep')
    dp = lax.axis_index('dp')
    num_tokens = tokens_hbm.shape[0]
    plane = 2 * side * side
    ends = 2 * side
    count = len(groups)
    arrival = (0, 1, 4, 2, 3, 5) if count == 6 else (1, 0, 2)
    near = (1, side - 1) if side > 2 else (1,)
    far = side > 2
    packed_rows = plane * SLOTS
    top_k = routes_ref.shape[0]
    orders = [ORDERS[g % 3] for g in range(count)]

    def remote(src, dst, s_sem, r_sem, axis, steps, core_steps=0):
        return pltpu.make_async_remote_copy(
            src_ref=src, dst_ref=dst, send_sem=s_sem, recv_sem=r_sem,
            device_id=(dp, moved(me, side, axis, steps, core_steps)), device_id_type=MESH)

    def columns(g):
        return pl.ds(*groups[g])

    def relay_from(g, q, b):
        return relay[g].at[q, b] if g % 3 == 1 else relay[g].at[q, :, b]

    def relay_others(g, q):
        return relay[g].at[q, pl.ds(1, side - 1)] if g % 3 == 1 else relay[g].at[q, :, pl.ds(1, side - 1)]

    def rows_at(g, q, e):
        c, core = e // 2, e % 2
        third = orders[g][2]
        where = {Z: (q, c, slice(None), slice(None), core), Y: (q, slice(None), c, slice(None), core),
                 X: (q, slice(None), slice(None), c, core)}[third]
        return where + (slice(None), columns(g))

    def half(i):
        return pl.ds(i * (num_tokens // 2), num_tokens // 2)

    def gather_near(g, d, i):
        part = half(i if d == 0 else 1 - i)
        return remote(toks[g].at[0, part], toks[g].at[near[d], part],
                      s0_sem.at[g, 2 * d + i], r0_sem.at[g, 2 * d + i], orders[g][0], near[d])

    def gather_far(g, d):
        return remote(toks[g].at[near[d], half(d)], toks[g].at[2, half(d)],
                      s0_sem.at[g, 4 + d], r0_sem.at[g, 4 + d], orders[g][0], near[d])

    def gather_info(o, a):
        return remote(own_info, infos.at[o, a], sp_sem.at[o], rp_sem.at[o], ORDERS[o][0], a)

    def gather_info_all(o):
        others = infos.at[o, pl.ds(1, side - 1)]
        return remote(others, others, sp_sem.at[o], rp_sem.at[o], ORDERS[o][0], 1)

    def relay_slab(g, q, a, b):
        return relay[g].at[q, b, a] if g % 3 == 1 else relay[g].at[q, a, b]

    def out_second(g, q, a, b):
        return remote(packed[g].at[q, b, a], relay_slab(g, q, a, b), s1_sem.at[g, q], r1_sem.at[g, q], orders[g][1], b)

    def out_second_all(g, q):
        return remote(packed[g].at[q, pl.ds(1, side - 1)], relay_others(g, q), s1_sem.at[g, q], r1_sem.at[g, q], orders[g][1], 1)

    def out_third(g, q, e):
        return remote(relay[g].at[q, :, :, e], rows.at[rows_at(g, q, e)], s2_sem.at[g, q], r2_sem.at[g, q], orders[g][2], e // 2, e % 2)

    def third_all(g, q, s_sem, r_sem):
        some = relay[g].at[q, :, :, pl.ds(1, ends - 1)]
        return remote(some, some, s_sem.at[g, q], r_sem.at[g, q], orders[g][2], 1)

    def home_third(g, q, e):
        return remote(rows.at[rows_at(g, q, e)], relay[g].at[q, :, :, e], b1_sem.at[g, q], c1_sem.at[g, q], orders[g][2], -(e // 2), e % 2)

    def home_second(g, q, b):
        return remote(relay_from(g, q, b), packed[g].at[q, b], b2_sem.at[g, q], c2_sem.at[g, q], orders[g][1], -b)

    def home_second_all(g, q):
        return remote(relay_others(g, q), packed[g].at[q, pl.ds(1, side - 1)], b2_sem.at[g, q], c2_sem.at[g, q], orders[g][1], 1)

    def home_mid(g, d):
        return remote(parts.at[2, half(d), columns(g)], mids.at[d, :, columns(g)],
                      s3_sem.at[g, d], r3_sem.at[g, d], orders[g][0], -near[d])

    def home_near(g, d, i):
        part = half(1 - d if i == 0 else d)
        return remote(parts.at[near[d], part, columns(g)], y_peers.at[d, part, columns(g)],
                      s3_sem.at[g, 2 + 2 * d + i], r3_sem.at[g, 2 + 2 * d + i], orders[g][0], -near[d])

    def tell(sem, axis, steps, core_steps=0):
        pl.semaphore_signal(sem, inc=1, device_id=(dp, moved(me, side, axis, steps, core_steps)), device_id_type=MESH)

    loads = [pltpu.make_async_copy(tokens_hbm.at[:, columns(g)], toks[g].at[0], load_sem.at[g]) for g in range(count)]
    loads.append(pltpu.make_async_copy(w_router_hbm, w_router, load_sem.at[count]))
    weights = [pltpu.make_async_copy(src, dst, w_sem.at[i]) for i, (src, dst) in enumerate(
        [(w_one_hbm, w_one), (w_three_hbm, w_three), (w_two_hbm, w_two)])]
    barrier = pltpu.get_barrier_semaphore()
    tell(barrier, X, 0, 1)
    for axis in (Z, Y, X):
        for steps in range(1, side):
            for core_steps in range(2):
                tell(barrier, axis, steps, core_steps)
    for copy in loads:
        copy.start()
    with jax.named_scope('own_wait'):
        for copy in loads:
            copy.wait()
    with jax.named_scope('barrier'):
        pl.semaphore_wait(barrier, 1 + 3 * (side - 1) * 2)

    for i in range(2):
        for g in range(count):
            for d in range(len(near)):
                gather_near(g, d, i).start()

    num_experts = 2 * side ** 3
    logits = sum(jnp.dot(toks[g][0], w_router[columns(g), :], preferred_element_type=jnp.float32) for g in range(count)).T
    ids = lax.broadcasted_iota(jnp.int32, (num_experts, num_tokens), 0)
    picks = [routes_ref[k:k + 1, :] for k in range(top_k)]
    scores = [jnp.sum(jnp.where(pick == ids, logits, 0.0), axis=0, keepdims=True) for pick in picks]
    peak = functools.reduce(jnp.maximum, scores)
    scores = [jnp.exp(score - peak) for score in scores]
    norm = sum(scores)
    for k in range(top_k):
        own_info[k:k + 1, :] = picks[k].astype(jnp.float32)
        own_info[top_k + k:top_k + k + 1, :] = scores[k] / norm
    for o in range(3):
        for a in range(1, side):
            gather_info(o, a).start()
    before = (lax.broadcasted_iota(jnp.int32, (num_tokens, num_tokens), 0)
              < lax.broadcasted_iota(jnp.int32, (num_tokens, num_tokens), 1))
    before = jnp.where(before, 1.0, 0.0).astype(jnp.bfloat16)
    expert_at = [plane_experts(me, side, order, num_tokens).astype(jnp.float32) for order in ORDERS]

    def make_plan(o, a, info):
        mask = jnp.zeros((plane, num_tokens), jnp.float32)
        gate = jnp.zeros((plane, num_tokens), jnp.float32)
        for k in range(top_k):
            hit = info[k:k + 1] == expert_at[o]
            mask = jnp.where(hit, 1.0, mask)
            gate = jnp.where(hit, info[top_k + k:top_k + k + 1], gate)
        slot = jnp.dot(mask.astype(jnp.bfloat16), before, preferred_element_type=jnp.float32)
        plans[o][a, pl.ds(0, plane), :] = jnp.where(mask > 0.0, slot, -1.0)
        plans[o][a, pl.ds(plane, plane), :] = gate

    for o in range(3):
        make_plan(o, 0, own_info[...])
    for copy in weights:
        copy.start()

    def taken(g, q, a):
        slots = plans[g % 3][a, pl.ds(0, plane), :]
        ids = lax.broadcasted_iota(jnp.int32, (plane, SLOTS, num_tokens), 1) + q * SLOTS
        return jnp.broadcast_to(slots[:, None, :], (plane, SLOTS, num_tokens)) == ids.astype(jnp.float32)

    def pack(g, q, a):
        select = jnp.where(taken(g, q, a), 1.0, 0.0).reshape(packed_rows, num_tokens).astype(jnp.bfloat16)
        out = jnp.dot(select, toks[g][a], preferred_element_type=jnp.float32)
        out = out.reshape(side, ends, SLOTS, groups[g][1]).astype(jnp.bfloat16)
        packed[g][q, pl.ds(1, side - 1), a] = out[1:]
        each(1, side, lambda b: out_second(g, q, a, b).start())
        relay_slab(g, q, a, 0)[...] = out[0]

    def pack_own(q, carry):
        for g in range(count):
            pack(g, q, 0)
        return carry

    if far:
        with jax.named_scope('gather_far'):
            for g in range(count):
                for d in range(2):
                    gather_near(g, d, 0).wait_recv()
                    gather_far(g, d).start()
    with jax.named_scope('pack_own'):
        lax.fori_loop(0, chunks, pack_own, 0)
    parts[...] = jnp.zeros_like(parts)
    with jax.named_scope('gather_wait'):
        for o in range(3):
            gather_info_all(o).wait_recv()
            for a in range(1, side):
                make_plan(o, a, infos[o, a])
        for g in range(count):
            for d in range(len(near)):
                if not far:
                    gather_near(g, d, 0).wait_recv()
                gather_near(g, d, 1).wait_recv()
            if far:
                gather_far(g, 0).wait_recv()
                gather_far(g, 1).wait_recv()

    def outward(i, carry):
        @pl.when(i < chunks)
        def _():
            for g in range(count):
                def source(a, c):
                    pack(g, i, a)
                    return c
                with jax.named_scope('pack'):
                    lax.fori_loop(1, side, source, 0)

        @pl.when(i > 0)
        def _():
            forward(i - 1)
        return carry

    def forward(q):
        for g in range(count):
            with jax.named_scope('s1_wait'):
                out_second_all(g, q).wait_recv()
            each(1, ends, lambda e: out_third(g, q, e).start())
            rows[rows_at(g, q, 0)] = relay[g][q, :, :, 0]
            with jax.named_scope('s1_send_wait'):
                out_second_all(g, q).wait_send()
            each(1, side, lambda b: tell(free2_sem.at[g, q], orders[g][1], b))

    lax.fori_loop(0, chunks + 1, outward, 0)
    for copy in weights:
        copy.wait()

    def experts(q, carry):
        with jax.named_scope('s2_wait'):
            for g in range(count):
                third_all(g, q, s2_sem, r2_sem).wait_recv()
        for g in range(count):
            with jax.named_scope('s2_send_wait'):
                third_all(g, q, s2_sem, r2_sem).wait_send()
            each(1, ends, lambda e: tell(free3_sem.at[g, q], orders[g][2], e // 2, e % 2))

        def block(z, c):
            shape = rows.shape[2:]
            u = rows[q, z].astype(jnp.float32).reshape(packed_rows, shape[-1]).astype(jnp.bfloat16)
            gate_pre = jnp.dot(u, w_one[...], preferred_element_type=jnp.float32)
            up_pre = jnp.dot(u, w_three[...], preferred_element_type=jnp.float32)
            hidden = (jax.nn.silu(gate_pre) * up_pre).astype(jnp.bfloat16)
            out = jnp.dot(hidden, w_two[...], preferred_element_type=jnp.float32)
            rows[q, z] = out.reshape(shape).astype(jnp.bfloat16)
            return c
        with jax.named_scope('mlp'):
            lax.fori_loop(0, side, block, 0)
        for g in range(count):
            with jax.named_scope('free3'):
                pl.semaphore_wait(free3_sem.at[g, q], ends - 1)
            each(1, ends, lambda e: home_third(g, q, e).start())
            relay[g][q, :, :, 0] = rows[rows_at(g, q, 0)]
        return carry

    lax.fori_loop(0, chunks, experts, 0)

    def backward(q):
        for g in range(count):
            with jax.named_scope('r1_wait'):
                third_all(g, q, b1_sem, c1_sem).wait_recv()
            pl.semaphore_wait(free2_sem.at[g, q], side - 1)
            each(1, side, lambda b: home_second(g, q, b).start())
            packed[g][q, 0] = relay_from(g, q, 0)[...]

    ahead = w_one.shape[1] >= 3 * packed_rows and w_one.shape[0] >= 2 * side * num_tokens

    def gate_rows(o, a):
        return pl.ds(pl.multiple_of(((o % 2) * side + a) * num_tokens, num_tokens), num_tokens)

    def gate_parts(g, q, a):
        gates = plans[g % 3][a, pl.ds(plane, plane), :]
        used = taken(g, q, a)
        for _ in range(3):
            part = gates.astype(jnp.bfloat16).astype(jnp.float32)
            gates = gates - part
            yield jnp.where(used, jnp.broadcast_to(part[:, None, :], used.shape), 0.0).reshape(packed_rows, num_tokens)

    def build_gates(q):
        for o in range(3):
            def build(a):
                for i, mix in enumerate(gate_parts(o, q, a)):
                    home = w_one if o < 2 else w_three
                    home[gate_rows(o, a), i * packed_rows:(i + 1) * packed_rows] = mix.T.astype(jnp.bfloat16)
            each(0, side, build)

    def combine(q):
        last = q == chunks - 1
        if ahead:
            with jax.named_scope('gates_ahead'):
                build_gates(q)
        for g in arrival:
            with jax.named_scope('r2_wait'):
                home_second_all(g, q).wait_recv()
            width = groups[g][1]

            def source(i, c):
                a = (i + side // 2) % side
                o = packed[g][q, :, a].astype(jnp.float32).reshape(packed_rows, width).astype(jnp.bfloat16)
                if ahead:
                    mixes = w_one if g % 3 < 2 else w_three
                    terms = [jnp.dot(mixes[gate_rows(g % 3, a), i * packed_rows:(i + 1) * packed_rows], o, preferred_element_type=jnp.float32)
                             for i in range(3)]
                else:
                    terms = [lax.dot_general(mix.astype(jnp.bfloat16), o, (((0,), (0,)), ((), ())), preferred_element_type=jnp.float32)
                             for mix in gate_parts(g, q, a)]
                parts[a, :, columns(g)] += terms[0] + terms[1] + terms[2]

                if far:
                    @pl.when(jnp.logical_and(last, a == 2))
                    def _():
                        home_mid(g, 0).start()
                        home_mid(g, 1).start()
                for d in range(len(near)):
                    @pl.when(jnp.logical_and(last, a == near[d]))
                    def _():
                        home_near(g, d, 0).start()
                return c
            with jax.named_scope('combine'):
                lax.fori_loop(0, side, source, 0)

    def send_home(q, carry):
        backward(q)
        return carry

    def sum_up(q, carry):
        combine(q)
        return carry

    lax.fori_loop(0, chunks, send_home, 0)
    lax.fori_loop(0, chunks, sum_up, 0)
    own = pltpu.make_async_copy(parts.at[0], y_own, out_sem)
    own.start()
    for g in ((0, 1, 2, 3, 5, 4) if count == 6 else arrival):
        for d in range(len(near)):
            if far:
                with jax.named_scope('mid_wait'):
                    home_mid(g, d).wait_recv()
                parts[near[d], half(d), columns(g)] += mids[d, :, columns(g)]
            home_near(g, d, 1).start()

    for g in range(count):
        def drain(q, c):
            third_all(g, q, b1_sem, c1_sem).wait_send()
            home_second_all(g, q).wait_send()
            return c
        lax.fori_loop(0, chunks, drain, 0)
        for d in range(len(near)):
            gather_near(g, d, 0).wait_send()
            gather_near(g, d, 1).wait_send()
            if far:
                gather_far(g, d).wait_send()
                home_mid(g, d).wait_send()
    for o in range(3):
        gather_info_all(o).wait_send()
    for g in arrival:
        for d in range(len(near)):
            for i in range(2):
                with jax.named_scope('r3_wait'):
                    home_near(g, d, i).wait_recv()
                    home_near(g, d, i).wait_send()
    own.wait()


def solution(mesh):
    group_size = mesh.shape['ep']
    side = torus_side(group_size)
    row_spec = P(('dp', 'ep'), None)
    expert_spec = P('ep', None, None)

    def device_step(tokens, routes, w_router, w_one, w_three, w_two):
        num_tokens, d_model = tokens.shape
        top_k = routes.shape[1]
        num_experts = w_router.shape[1]
        d_expert = w_one.shape[2]
        capacity = slot_capacity(num_tokens, top_k, num_experts)
        chunks = capacity // SLOTS
        groups = column_groups(d_model)
        count = len(groups)
        plane = 2 * side * side
        hbm = pl.BlockSpec(memory_space=pl.ANY)
        vmem = pl.BlockSpec(memory_space=pltpu.VMEM)
        dma = pltpu.SemaphoreType.DMA
        slab = [[pltpu.VMEM((chunks, side, side, 2 * side, SLOTS, width), jnp.bfloat16) for _, width in groups] for _ in range(2)]
        pair = [dma((count, chunks)), dma((count, chunks))]
        y_own, y_peers = pl.pallas_call(
            functools.partial(moe_kernel, side, chunks, groups),
            out_shape=(jax.ShapeDtypeStruct((num_tokens, d_model), jnp.float32),
                       jax.ShapeDtypeStruct((2 if side > 2 else 1, num_tokens, d_model), jnp.float32)),
            in_specs=[hbm, vmem, hbm, hbm, hbm, hbm],
            out_specs=(hbm, hbm),
            scratch_shapes=[
                [pltpu.VMEM((side, num_tokens, width), jnp.bfloat16) for _, width in groups],
                pltpu.VMEM((3, side, 2 * top_k, num_tokens), jnp.float32),
                pltpu.VMEM((2 * top_k, num_tokens), jnp.float32),
                [pltpu.VMEM((side, 2 * plane, num_tokens), jnp.float32) for _ in ORDERS],
                slab[0], slab[1],
                pltpu.VMEM((chunks, side, side, side, 2, SLOTS, d_model), jnp.bfloat16),
                pltpu.VMEM((d_model, num_experts), jnp.bfloat16),
                pltpu.VMEM((d_model, d_expert), jnp.bfloat16),
                pltpu.VMEM((d_model, d_expert), jnp.bfloat16),
                pltpu.VMEM((d_expert, d_model), jnp.bfloat16),
                pltpu.VMEM((side, num_tokens, d_model), jnp.float32),
                pltpu.VMEM((2, num_tokens // 2, d_model), jnp.float32),
                dma((count + 1,)), dma((3,)), dma((count, 6)), dma((count, 6)), dma((3,)), dma((3,)),
                *pair, *pair, *pair, *pair, dma((count, 6)), dma((count, 6)), dma,
                pltpu.SemaphoreType.REGULAR((count, chunks)), pltpu.SemaphoreType.REGULAR((count, chunks)),
            ],
            compiler_params=pltpu.CompilerParams(collective_id=0, has_side_effects=True, vmem_limit_bytes=67043328),
            name='moe',
        )(tokens, routes.T, w_router, w_one[0], w_three[0], w_two[0])
        total = y_own
        for i in range(y_peers.shape[0]):
            total = total + y_peers[i]
        return total.astype(jnp.bfloat16)

    return jax.shard_map(device_step, mesh=mesh, in_specs=(row_spec, row_spec, P(None, None), expert_spec, expert_spec, expert_spec), out_specs=row_spec, check_vma=False)
```

```python
import functools

import jax
import jax.numpy as jnp
from jax import lax
from jax.experimental import pallas as pl
from jax.experimental.pallas import tpu as pltpu
from jax.sharding import PartitionSpec as P

MESH = pl.DeviceIdType.MESH
Z, Y, X = 0, 1, 2
ORDERS = ((Z, Y, X), (X, Z, Y), (Y, X, Z))
SLOTS = 8


def slot_capacity(num_tokens, top_k, num_experts):
    return 8 * ((3 * num_tokens * top_k + 16 * num_experts - 1) // (16 * num_experts))


def torus_side(group_size):
    side = 1
    while 2 * side ** 3 < group_size:
        side += 1
    return side


def column_groups(d_model):
    lanes = d_model // 128
    count = 6 if lanes >= 6 else 3
    widths = [128 * (lanes // count + (1 if i < lanes % count else 0)) for i in range(count)]
    starts = [sum(widths[:i]) for i in range(count)]
    return list(zip(starts, widths))


def moved(me, side, axis, steps, core_steps=0):
    digits = [me // (2 * side * side), (me // (2 * side)) % side, (me // 2) % side]
    digits[axis] = (digits[axis] + steps + side) % side
    return ((digits[Z] * side + digits[Y]) * side + digits[X]) * 2 + (me + core_steps) % 2


def plane_experts(me, side, order, num_tokens):
    bits = side.bit_length() - 1
    position = lax.broadcasted_iota(jnp.int32, (2 * side * side, num_tokens), 0)
    digits = [me // (2 * side * side), (me // (2 * side)) % side, (me // 2) % side]
    for place, axis in enumerate(order[1:]):
        steps = jnp.right_shift(position, 1 + (1 - place) * bits)
        digits[axis] = jnp.bitwise_and(digits[axis] + steps, side - 1)
    core = jnp.bitwise_and(me + position, 1)
    return ((digits[Z] * side + digits[Y]) * side + digits[X]) * 2 + core


def each(first, end, act):
    def step(i, carry):
        act(i)
        return carry
    lax.fori_loop(first, end, step, 0)


def moe_kernel(side, chunks, groups, tokens_hbm, routes_ref, w_router_hbm, w_one_hbm, w_three_hbm, w_two_hbm, y_own, y_peers,
               toks, infos, own_info, plans, packed, relay, rows, w_router, w_one, w_three, w_two, parts, mids,
               load_sem, w_sem, s0_sem, r0_sem, sp_sem, rp_sem, s1_sem, r1_sem, s2_sem, r2_sem, b1_sem, c1_sem, b2_sem, c2_sem, s3_sem, r3_sem, out_sem, free2_sem, free3_sem):
    me = lax.axis_index('ep')
    dp = lax.axis_index('dp')
    num_tokens = tokens_hbm.shape[0]
    plane = 2 * side * side
    ends = 2 * side
    count = len(groups)
    arrival = (0, 1, 4, 2, 3, 5) if count == 6 else (1, 0, 2)
    near = (1, side - 1) if side > 2 else (1,)
    far = side > 2
    packed_rows = plane * SLOTS
    top_k = routes_ref.shape[0]
    orders = [ORDERS[g % 3] for g in range(count)]

    def remote(src, dst, s_sem, r_sem, axis, steps, core_steps=0):
        return pltpu.make_async_remote_copy(
            src_ref=src, dst_ref=dst, send_sem=s_sem, recv_sem=r_sem,
            device_id=(dp, moved(me, side, axis, steps, core_steps)), device_id_type=MESH)

    def columns(g):
        return pl.ds(*groups[g])

    def relay_from(g, q, b):
        return relay[g].at[q, b] if g % 3 == 1 else relay[g].at[q, :, b]

    def relay_others(g, q):
        return relay[g].at[q, pl.ds(1, side - 1)] if g % 3 == 1 else relay[g].at[q, :, pl.ds(1, side - 1)]

    def rows_at(g, q, e):
        c, core = e // 2, e % 2
        third = orders[g][2]
        where = {Z: (q, c, slice(None), slice(None), core), Y: (q, slice(None), c, slice(None), core),
                 X: (q, slice(None), slice(None), c, core)}[third]
        return where + (slice(None), columns(g))

    def half(i):
        return pl.ds(i * (num_tokens // 2), num_tokens // 2)

    def gather_near(g, d, i):
        part = half(i if d == 0 else 1 - i)
        return remote(toks[g].at[0, part], toks[g].at[near[d], part],
                      s0_sem.at[g, 2 * d + i], r0_sem.at[g, 2 * d + i], orders[g][0], near[d])

    def gather_far(g, d):
        return remote(toks[g].at[near[d], half(d)], toks[g].at[2, half(d)],
                      s0_sem.at[g, 4 + d], r0_sem.at[g, 4 + d], orders[g][0], near[d])

    def gather_info(o, a):
        return remote(own_info, infos.at[o, a], sp_sem.at[o], rp_sem.at[o], ORDERS[o][0], a)

    def gather_info_all(o):
        others = infos.at[o, pl.ds(1, side - 1)]
        return remote(others, others, sp_sem.at[o], rp_sem.at[o], ORDERS[o][0], 1)

    def relay_slab(g, q, a, b):
        return relay[g].at[q, b, a] if g % 3 == 1 else relay[g].at[q, a, b]

    def out_second(g, q, a, b):
        return remote(packed[g].at[q, b, a], relay_slab(g, q, a, b), s1_sem.at[g, q], r1_sem.at[g, q], orders[g][1], b)

    def out_second_all(g, q):
        return remote(packed[g].at[q, pl.ds(1, side - 1)], relay_others(g, q), s1_sem.at[g, q], r1_sem.at[g, q], orders[g][1], 1)

    def out_third(g, q, e):
        return remote(relay[g].at[q, :, :, e], rows.at[rows_at(g, q, e)], s2_sem.at[g, q], r2_sem.at[g, q], orders[g][2], e // 2, e % 2)

    def third_all(g, q, s_sem, r_sem):
        some = relay[g].at[q, :, :, pl.ds(1, ends - 1)]
        return remote(some, some, s_sem.at[g, q], r_sem.at[g, q], orders[g][2], 1)

    def home_third(g, q, e):
        return remote(rows.at[rows_at(g, q, e)], relay[g].at[q, :, :, e], b1_sem.at[g, q], c1_sem.at[g, q], orders[g][2], -(e // 2), e % 2)

    def home_second(g, q, b):
        return remote(relay_from(g, q, b), packed[g].at[q, b], b2_sem.at[g, q], c2_sem.at[g, q], orders[g][1], -b)

    def home_second_all(g, q):
        return remote(relay_others(g, q), packed[g].at[q, pl.ds(1, side - 1)], b2_sem.at[g, q], c2_sem.at[g, q], orders[g][1], 1)

    def home_mid(g, d):
        return remote(parts.at[2, half(d), columns(g)], mids.at[d, :, columns(g)],
                      s3_sem.at[g, d], r3_sem.at[g, d], orders[g][0], -near[d])

    def home_near(g, d, i):
        part = half(1 - d if i == 0 else d)
        return remote(parts.at[near[d], part, columns(g)], y_peers.at[d, part, columns(g)],
                      s3_sem.at[g, 2 + 2 * d + i], r3_sem.at[g, 2 + 2 * d + i], orders[g][0], -near[d])

    def tell(sem, axis, steps, core_steps=0):
        pl.semaphore_signal(sem, inc=1, device_id=(dp, moved(me, side, axis, steps, core_steps)), device_id_type=MESH)

    loads = [pltpu.make_async_copy(tokens_hbm.at[:, columns(g)], toks[g].at[0], load_sem.at[g]) for g in range(count)]
    loads.append(pltpu.make_async_copy(w_router_hbm, w_router, load_sem.at[count]))
    weights = [pltpu.make_async_copy(src, dst, w_sem.at[i]) for i, (src, dst) in enumerate(
        [(w_one_hbm, w_one), (w_three_hbm, w_three), (w_two_hbm, w_two)])]
    barrier = pltpu.get_barrier_semaphore()
    tell(barrier, X, 0, 1)
    for axis in (Z, Y, X):
        for steps in range(1, side):
            for core_steps in range(2):
                tell(barrier, axis, steps, core_steps)
    for copy in loads:
        copy.start()
    with jax.named_scope('own_wait'):
        for copy in loads:
            copy.wait()
    with jax.named_scope('barrier'):
        pl.semaphore_wait(barrier, 1 + 3 * (side - 1) * 2)

    for i in range(2):
        for g in range(count):
            for d in range(len(near)):
                gather_near(g, d, i).start()

    num_experts = 2 * side ** 3
    logits = sum(jnp.dot(toks[g][0], w_router[columns(g), :], preferred_element_type=jnp.float32) for g in range(count)).T
    ids = lax.broadcasted_iota(jnp.int32, (num_experts, num_tokens), 0)
    picks = [routes_ref[k:k + 1, :] for k in range(top_k)]
    scores = [jnp.sum(jnp.where(pick == ids, logits, 0.0), axis=0, keepdims=True) for pick in picks]
    peak = functools.reduce(jnp.maximum, scores)
    scores = [jnp.exp(score - peak) for score in scores]
    norm = sum(scores)
    for k in range(top_k):
        own_info[k:k + 1, :] = picks[k].astype(jnp.float32)
        own_info[top_k + k:top_k + k + 1, :] = scores[k] / norm
    for o in range(3):
        for a in range(1, side):
            gather_info(o, a).start()
    before = (lax.broadcasted_iota(jnp.int32, (num_tokens, num_tokens), 0)
              < lax.broadcasted_iota(jnp.int32, (num_tokens, num_tokens), 1))
    before = jnp.where(before, 1.0, 0.0).astype(jnp.bfloat16)
    expert_at = [plane_experts(me, side, order, num_tokens).astype(jnp.float32) for order in ORDERS]

    def make_plan(o, a, info):
        mask = jnp.zeros((plane, num_tokens), jnp.float32)
        gate = jnp.zeros((plane, num_tokens), jnp.float32)
        for k in range(top_k):
            hit = info[k:k + 1] == expert_at[o]
            mask = jnp.where(hit, 1.0, mask)
            gate = jnp.where(hit, info[top_k + k:top_k + k + 1], gate)
        slot = jnp.dot(mask.astype(jnp.bfloat16), before, preferred_element_type=jnp.float32)
        plans[o][a, pl.ds(0, plane), :] = jnp.where(mask > 0.0, slot, -1.0)
        plans[o][a, pl.ds(plane, plane), :] = gate

    for o in range(3):
        make_plan(o, 0, own_info[...])
    for copy in weights:
        copy.start()

    def taken(g, q, a):
        slots = plans[g % 3][a, pl.ds(0, plane), :]
        ids = lax.broadcasted_iota(jnp.int32, (plane, SLOTS, num_tokens), 1) + q * SLOTS
        return jnp.broadcast_to(slots[:, None, :], (plane, SLOTS, num_tokens)) == ids.astype(jnp.float32)

    def pack(g, q, a):
        select = jnp.where(taken(g, q, a), 1.0, 0.0).reshape(packed_rows, num_tokens).astype(jnp.bfloat16)
        out = jnp.dot(select, toks[g][a], preferred_element_type=jnp.float32)
        out = out.reshape(side, ends, SLOTS, groups[g][1]).astype(jnp.bfloat16)
        packed[g][q, pl.ds(1, side - 1), a] = out[1:]
        each(1, side, lambda b: out_second(g, q, a, b % (side - 1) + 1).start())
        relay_slab(g, q, a, 0)[...] = out[0]

    def pack_own(q, carry):
        for g in range(count):
            pack(g, q, 0)
        return carry

    if far:
        with jax.named_scope('gather_far'):
            for g in range(count):
                for d in range(2):
                    gather_near(g, d, 0).wait_recv()
                    gather_far(g, d).start()
    with jax.named_scope('pack_own'):
        lax.fori_loop(0, chunks, pack_own, 0)
    parts[...] = jnp.zeros_like(parts)
    with jax.named_scope('gather_wait'):
        for o in range(3):
            gather_info_all(o).wait_recv()
            for a in range(1, side):
                make_plan(o, a, infos[o, a])
        for g in range(count):
            for d in range(len(near)):
                if not far:
                    gather_near(g, d, 0).wait_recv()
                gather_near(g, d, 1).wait_recv()
            if far:
                gather_far(g, 0).wait_recv()
                gather_far(g, 1).wait_recv()

    def outward(i, carry):
        @pl.when(i < chunks)
        def _():
            for g in range(count):
                def source(a, c):
                    pack(g, i, a)
                    return c
                with jax.named_scope('pack'):
                    lax.fori_loop(1, side, source, 0)

        @pl.when(i > 0)
        def _():
            forward(i - 1)
        return carry

    def forward(q):
        for g in range(count):
            with jax.named_scope('s1_wait'):
                out_second_all(g, q).wait_recv()
            each(1, ends, lambda e: out_third(g, q, e).start())
            rows[rows_at(g, q, 0)] = relay[g][q, :, :, 0]
            with jax.named_scope('s1_send_wait'):
                out_second_all(g, q).wait_send()
            each(1, side, lambda b: tell(free2_sem.at[g, q], orders[g][1], b))

    lax.fori_loop(0, chunks + 1, outward, 0)
    for copy in weights:
        copy.wait()

    def experts(q, carry):
        with jax.named_scope('s2_wait'):
            for g in range(count):
                third_all(g, q, s2_sem, r2_sem).wait_recv()
        for g in range(count):
            with jax.named_scope('s2_send_wait'):
                third_all(g, q, s2_sem, r2_sem).wait_send()
            each(1, ends, lambda e: tell(free3_sem.at[g, q], orders[g][2], e // 2, e % 2))

        def block(z, c):
            shape = rows.shape[2:]
            u = rows[q, z].astype(jnp.float32).reshape(packed_rows, shape[-1]).astype(jnp.bfloat16)
            gate_pre = jnp.dot(u, w_one[...], preferred_element_type=jnp.float32)
            up_pre = jnp.dot(u, w_three[...], preferred_element_type=jnp.float32)
            hidden = (jax.nn.silu(gate_pre) * up_pre).astype(jnp.bfloat16)
            out = jnp.dot(hidden, w_two[...], preferred_element_type=jnp.float32)
            rows[q, z] = out.reshape(shape).astype(jnp.bfloat16)
            return c
        with jax.named_scope('mlp'):
            lax.fori_loop(0, side, block, 0)
        for g in range(count):
            with jax.named_scope('free3'):
                pl.semaphore_wait(free3_sem.at[g, q], ends - 1)
            each(1, ends, lambda e: home_third(g, q, e).start())
            relay[g][q, :, :, 0] = rows[rows_at(g, q, 0)]
        return carry

    lax.fori_loop(0, chunks, experts, 0)

    def backward(q):
        for g in range(count):
            with jax.named_scope('r1_wait'):
                third_all(g, q, b1_sem, c1_sem).wait_recv()
            pl.semaphore_wait(free2_sem.at[g, q], side - 1)
            each(1, side, lambda b: home_second(g, q, b % (side - 1) + 1).start())
            packed[g][q, 0] = relay_from(g, q, 0)[...]

    ahead = w_one.shape[1] >= 3 * packed_rows and w_one.shape[0] >= 2 * side * num_tokens

    def gate_rows(o, a):
        return pl.ds(pl.multiple_of(((o % 2) * side + a) * num_tokens, num_tokens), num_tokens)

    def gate_parts(g, q, a):
        gates = plans[g % 3][a, pl.ds(plane, plane), :]
        used = taken(g, q, a)
        for _ in range(3):
            part = gates.astype(jnp.bfloat16).astype(jnp.float32)
            gates = gates - part
            yield jnp.where(used, jnp.broadcast_to(part[:, None, :], used.shape), 0.0).reshape(packed_rows, num_tokens)

    def build_gates(q):
        for o in range(3):
            def build(a):
                for i, mix in enumerate(gate_parts(o, q, a)):
                    home = w_one if o < 2 else w_three
                    home[gate_rows(o, a), i * packed_rows:(i + 1) * packed_rows] = mix.T.astype(jnp.bfloat16)
            each(0, side, build)

    def combine(q):
        last = q == chunks - 1
        if ahead:
            with jax.named_scope('gates_ahead'):
                build_gates(q)
        for g in arrival:
            with jax.named_scope('r2_wait'):
                home_second_all(g, q).wait_recv()
            width = groups[g][1]

            def source(i, c):
                a = (i + side // 2) % side
                o = packed[g][q, :, a].astype(jnp.float32).reshape(packed_rows, width).astype(jnp.bfloat16)
                if ahead:
                    mixes = w_one if g % 3 < 2 else w_three
                    terms = [jnp.dot(mixes[gate_rows(g % 3, a), i * packed_rows:(i + 1) * packed_rows], o, preferred_element_type=jnp.float32)
                             for i in range(3)]
                else:
                    terms = [lax.dot_general(mix.astype(jnp.bfloat16), o, (((0,), (0,)), ((), ())), preferred_element_type=jnp.float32)
                             for mix in gate_parts(g, q, a)]
                parts[a, :, columns(g)] += terms[0] + terms[1] + terms[2]

                if far:
                    @pl.when(jnp.logical_and(last, a == 2))
                    def _():
                        home_mid(g, 0).start()
                        home_mid(g, 1).start()
                for d in range(len(near)):
                    @pl.when(jnp.logical_and(last, a == near[d]))
                    def _():
                        home_near(g, d, 0).start()
                return c
            with jax.named_scope('combine'):
                lax.fori_loop(0, side, source, 0)

    def send_home(q, carry):
        backward(q)
        return carry

    def sum_up(q, carry):
        combine(q)
        return carry

    lax.fori_loop(0, chunks, send_home, 0)
    lax.fori_loop(0, chunks, sum_up, 0)
    own = pltpu.make_async_copy(parts.at[0], y_own, out_sem)
    own.start()
    for g in ((0, 1, 2, 3, 5, 4) if count == 6 else arrival):
        for d in range(len(near)):
            if far:
                with jax.named_scope('mid_wait'):
                    home_mid(g, d).wait_recv()
                parts[near[d], half(d), columns(g)] += mids[d, :, columns(g)]
            home_near(g, d, 1).start()

    for g in range(count):
        def drain(q, c):
            third_all(g, q, b1_sem, c1_sem).wait_send()
            home_second_all(g, q).wait_send()
            return c
        lax.fori_loop(0, chunks, drain, 0)
        for d in range(len(near)):
            gather_near(g, d, 0).wait_send()
            gather_near(g, d, 1).wait_send()
            if far:
                gather_far(g, d).wait_send()
                home_mid(g, d).wait_send()
    for o in range(3):
        gather_info_all(o).wait_send()
    for g in arrival:
        for d in range(len(near)):
            for i in range(2):
                with jax.named_scope('r3_wait'):
                    home_near(g, d, i).wait_recv()
                    home_near(g, d, i).wait_send()
    own.wait()


def solution(mesh):
    group_size = mesh.shape['ep']
    side = torus_side(group_size)
    row_spec = P(('dp', 'ep'), None)
    expert_spec = P('ep', None, None)

    def device_step(tokens, routes, w_router, w_one, w_three, w_two):
        num_tokens, d_model = tokens.shape
        top_k = routes.shape[1]
        num_experts = w_router.shape[1]
        d_expert = w_one.shape[2]
        capacity = slot_capacity(num_tokens, top_k, num_experts)
        chunks = capacity // SLOTS
        groups = column_groups(d_model)
        count = len(groups)
        plane = 2 * side * side
        hbm = pl.BlockSpec(memory_space=pl.ANY)
        vmem = pl.BlockSpec(memory_space=pltpu.VMEM)
        dma = pltpu.SemaphoreType.DMA
        slab = [[pltpu.VMEM((chunks, side, side, 2 * side, SLOTS, width), jnp.bfloat16) for _, width in groups] for _ in range(2)]
        pair = [dma((count, chunks)), dma((count, chunks))]
        y_own, y_peers = pl.pallas_call(
            functools.partial(moe_kernel, side, chunks, groups),
            out_shape=(jax.ShapeDtypeStruct((num_tokens, d_model), jnp.float32),
                       jax.ShapeDtypeStruct((2 if side > 2 else 1, num_tokens, d_model), jnp.float32)),
            in_specs=[hbm, vmem, hbm, hbm, hbm, hbm],
            out_specs=(hbm, hbm),
            scratch_shapes=[
                [pltpu.VMEM((side, num_tokens, width), jnp.bfloat16) for _, width in groups],
                pltpu.VMEM((3, side, 2 * top_k, num_tokens), jnp.float32),
                pltpu.VMEM((2 * top_k, num_tokens), jnp.float32),
                [pltpu.VMEM((side, 2 * plane, num_tokens), jnp.float32) for _ in ORDERS],
                slab[0], slab[1],
                pltpu.VMEM((chunks, side, side, side, 2, SLOTS, d_model), jnp.bfloat16),
                pltpu.VMEM((d_model, num_experts), jnp.bfloat16),
                pltpu.VMEM((d_model, d_expert), jnp.bfloat16),
                pltpu.VMEM((d_model, d_expert), jnp.bfloat16),
                pltpu.VMEM((d_expert, d_model), jnp.bfloat16),
                pltpu.VMEM((side, num_tokens, d_model), jnp.float32),
                pltpu.VMEM((2, num_tokens // 2, d_model), jnp.float32),
                dma((count + 1,)), dma((3,)), dma((count, 6)), dma((count, 6)), dma((3,)), dma((3,)),
                *pair, *pair, *pair, *pair, dma((count, 6)), dma((count, 6)), dma,
                pltpu.SemaphoreType.REGULAR((count, chunks)), pltpu.SemaphoreType.REGULAR((count, chunks)),
            ],
            compiler_params=pltpu.CompilerParams(collective_id=0, has_side_effects=True, vmem_limit_bytes=67043328),
            name='moe',
        )(tokens, routes.T, w_router, w_one[0], w_three[0], w_two[0])
        total = y_own
        for i in range(y_peers.shape[0]):
            total = total + y_peers[i]
        return total.astype(jnp.bfloat16)

    return jax.shard_map(device_step, mesh=mesh, in_specs=(row_spec, row_spec, P(None, None), expert_spec, expert_spec, expert_spec), out_specs=row_spec, check_vma=False)
```
